256 devices in a mesh: dp: 32 (over y, x, core), tensor: 8 (over z).
Axes of the slice: x: 4, y: 4, z: 8, core: 2. Of those that a mesh axis runs over, the one named last changes fastest.
Arguments:
- text: bfloat16 [32, 256, 5120], P('dp', None, 'tensor'), may hold values from -6 to 6
- prompts: bfloat16 [32, 100, 5120], P('dp', None, 'tensor'), may hold values from -6 to 6
- gain: float32 [5120], replicated, may hold values from 0.1 to 1.9
- w_query: bfloat16 [5120, 3072], P(None, 'tensor'), may hold values from -0.069877124 to 0.069877124, as said below
- w_key: bfloat16 [5120, 3072], P(None, 'tensor'), may hold values from -1.2577882 to 1.2577882, as said below
- w_value: bfloat16 [5120, 3072], P(None, 'tensor'), may hold values from -0.078125 to 0.078125
- cotangent: bfloat16 [32, 356, 3072], P('dp', None, 'tensor'), may hold values from -6 to 6
- task_of: int32 [32], replicated, may hold values from 0 to 31, as said below
- lengths: int32 [32], replicated, may hold values from 1 to 256, as said below
- slot: int32 [32], replicated, may hold values from 0 to 31, as said below
Outputs:
- attn_out: bfloat16 [32, 356, 3072], P('dp', None, 'tensor')
- prompt_grad: float32 [32, 100, 5120], P('dp', None, 'tensor')
The draws below stay inside these ranges and needn't reach their ends.
Inputs may be any that keep to these rules, and one draw needn't show every extreme that they name: `task_of`: nondecreasing along the source order. `lengths`: some example has exactly 256 text tokens; rows of an example beyond its length are padding. `slot`: a permutation of 0 to 31; position s lies on index s // 1 of dp. `w_query`: entries of order 5120 ** -0.5. `w_key`: entries of order 5120 ** -0.5 or larger.
All inputs are finite; a program needn't handle non-finite values.
Results may differ from the reference program's by a relative error of at most 0.0082.
Values may be sent and summed in bfloat16 or wider, within the bound.
A program may use at most 128 MiB of HBM per device.

```python
import math
import jax
import jax.numpy as jnp
from jax import lax

D = 5120
HEADS = 24
HD = 128
P_SIZE = 100
SEQ = 256
EX_DEV = 1
ROWS = 356
EXAMPLES = 32
TASKS = 32


def weight_base(key):
    return jax.random.truncated_normal(jax.random.fold_in(key, 11), -4.0, 4.0, (D, HEADS * HD), jnp.float32) / math.sqrt(D)


def draw_w_query(key, part):
    return weight_base(key).astype(jnp.bfloat16)


def draw_w_key(key, part):
    noise_part = jax.random.truncated_normal(jax.random.fold_in(key, 12), -4.0, 4.0, (D, HEADS * HD), jnp.float32) / math.sqrt(D)
    result = noise_part
    return result.astype(jnp.bfloat16)


def draw_task_of(key, part):
    first_key, second_key, third_key = jax.random.split(jax.random.fold_in(key, 21), 3)
    first_pick = jax.random.randint(first_key, (EXAMPLES,), 0, TASKS)
    second_pick = jax.random.randint(second_key, (EXAMPLES,), 0, TASKS)
    ranked = jnp.minimum(first_pick, second_pick)
    shuffle = jax.random.permutation(third_key, TASKS)
    return jnp.sort(shuffle[ranked]).astype(jnp.int32)


def length_base(key):
    first_key, second_key = jax.random.split(jax.random.fold_in(key, 31))
    raw_lengths = jax.random.randint(first_key, (EXAMPLES,), 1, SEQ + 1)
    longest = jax.random.randint(second_key, (), 0, EXAMPLES)
    return jnp.where(jnp.arange(EXAMPLES) == longest, SEQ, raw_lengths).astype(jnp.int32)


def draw_lengths(key, part):
    return length_base(key)


def draw_slot(key, part):
    length_all = length_base(key)
    device_count = EXAMPLES // EX_DEV
    order = jnp.argsort(-length_all, stable=True)
    ranks = jnp.arange(EXAMPLES, dtype=jnp.int32)
    rounds = ranks // device_count
    column = ranks % device_count
    device = jnp.where(rounds % 2 == 0, column, device_count - 1 - column)
    placed = (device * EX_DEV + rounds).astype(jnp.int32)
    return jnp.zeros((EXAMPLES,), jnp.int32).at[order].set(placed)


def block_scale(key, dims, shards, least, largest):
    level, own = 1.0, jax.random.fold_in(key, 6)
    for dim, shards_of in shards:
        draws = jnp.exp(jax.random.uniform(jax.random.fold_in(own, dim), (shards_of,), jnp.float32, least / len(shards), largest / len(shards)))
        level = level * jnp.repeat(draws, dims[dim] // shards_of).reshape([-1 if axis == dim else 1 for axis in range(len(dims))])
    return level


def scatter_about(stream_key, shape, width, most, cuts=(), held_as=jnp.bfloat16):
    factor_of = block_scale(stream_key, shape, cuts, -0.22, 0.18) if cuts else 1.0
    array = jax.random.normal(stream_key, shape, jnp.float32) * width * factor_of
    return jnp.minimum(jnp.maximum(array, -most), most).astype(held_as)


def setup_inputs(seed: int = 0) -> dict:
    keys = jax.random.split(jax.random.key(seed), 11)
    return {
        "text": scatter_about(keys[0], (EXAMPLES, SEQ, D), 1.0, 6.0, ((0, 32), (2, 8))),
        "prompts": scatter_about(keys[1], (TASKS, P_SIZE, D), 1.0, 6.0, ((0, 32), (2, 8))),
        "gain": jnp.clip(1.0 + 0.18 * jax.random.normal(keys[2], (D,), jnp.float32), 0.1, 1.9),
        "w_query": draw_w_query(jax.random.fold_in(keys[10], 71), 0),
        "w_key": draw_w_key(jax.random.fold_in(keys[10], 71), 0),
        "w_value": scatter_about(keys[5], (D, HEADS * HD), D ** -0.5, 0.078125, ((1, 8),)),
        "cotangent": scatter_about(keys[6], (EXAMPLES, ROWS, HEADS * HD), 1.0, 6.0, ((0, 32), (2, 8))),
        "task_of": draw_task_of(jax.random.fold_in(keys[10], 71), 0),
        "lengths": draw_lengths(jax.random.fold_in(keys[10], 71), 0),
        "slot": draw_slot(jax.random.fold_in(keys[10], 71), 0),
    }


def rope_tables(row_count):
    half_dim = HD // 2
    frequency = 10000.0 ** (-jnp.arange(half_dim, dtype=jnp.float32) / half_dim)
    angle_table = jnp.arange(row_count, dtype=jnp.float32)[:, None] * frequency[None, :]
    return (jnp.cos(angle_table), jnp.sin(angle_table))

def rotate(vectors, cosine_table, sine_table):
    half_dim = vectors.shape[-1] // 2
    first_half = vectors[..., :half_dim]
    second_half = vectors[..., half_dim:]
    cosine_b = cosine_table[:, None, :]
    sine_b = sine_table[:, None, :]
    return jnp.concatenate([first_half * cosine_b - second_half * sine_b, second_half * cosine_b + first_half * sine_b], axis=-1)

def unrotate(vectors, cosine_table, sine_table):
    half_dim = vectors.shape[-1] // 2
    first_half = vectors[..., :half_dim]
    second_half = vectors[..., half_dim:]
    cosine_b = cosine_table[:, None, :]
    sine_b = sine_table[:, None, :]
    return jnp.concatenate([first_half * cosine_b + second_half * sine_b, second_half * cosine_b - first_half * sine_b], axis=-1)

def transpose_product(grad_low, matrix):
    return lax.dot_general(grad_low, matrix, (((1,), (1,)), ((), ())), preferred_element_type=jnp.float32)

def attention_window(full_rows, gain, w_query, w_key, w_value, cotangent, valid_rows, prompt_len):
    batch_size, row_count, model_width = full_rows.shape
    head_count = w_query.shape[1] // HD
    wide_rows = full_rows.astype(jnp.float32)
    inv_rms = lax.rsqrt(lax.optimization_barrier(jnp.mean(wide_rows * wide_rows, axis=-1)) + 1e-05)
    normed = (wide_rows * inv_rms[..., None] * gain).astype(jnp.bfloat16).reshape(batch_size * row_count, model_width)
    cosine_table, sine_table = rope_tables(row_count)

    def project(matrix):
        return jnp.dot(normed, matrix, preferred_element_type=jnp.float32).reshape(batch_size, row_count, head_count, HD)
    queries = rotate(project(w_query), cosine_table, sine_table).astype(jnp.bfloat16)
    key_rows = rotate(project(w_key), cosine_table, sine_table).astype(jnp.bfloat16)
    value_rows = project(w_value).astype(jnp.bfloat16)
    score_scale = 1.0 / math.sqrt(HD)
    scores = jnp.einsum('erhd,ekhd->ehrk', queries.astype(jnp.float32), key_rows.astype(jnp.float32)) * score_scale
    rows_at = jnp.arange(row_count, dtype=jnp.int32)
    row_limit = (prompt_len + valid_rows).astype(jnp.int32)
    allowed = (rows_at[None, None, :] <= rows_at[None, :, None]) & (rows_at[None, None, :] < row_limit[:, None, None])
    allowed = allowed[:, None]
    scores = jnp.where(allowed, scores, -1e+30)
    row_peak = lax.optimization_barrier(jnp.max(scores, axis=-1, keepdims=True))
    weights = jnp.where(allowed, jnp.exp(scores - row_peak), 0.0)
    probability = weights / lax.optimization_barrier(jnp.sum(weights, axis=-1, keepdims=True))
    probs_low = probability.astype(jnp.bfloat16)
    live_rows = rows_at[None, :] < row_limit[:, None]
    mixed_rows = jnp.einsum('ehrk,ekhd->erhd', probs_low.astype(jnp.float32), value_rows.astype(jnp.float32))
    mixed_rows = jnp.where(live_rows[:, :, None, None], mixed_rows, 0.0)
    output = mixed_rows.reshape(batch_size, row_count, head_count * HD).astype(jnp.bfloat16)
    upstream = jnp.where(live_rows[:, :, None, None], cotangent.reshape(batch_size, row_count, head_count, HD), 0.0).astype(jnp.bfloat16)
    grad_prob = jnp.einsum('erhd,ekhd->ehrk', upstream.astype(jnp.float32), value_rows.astype(jnp.float32))
    row_delta = lax.optimization_barrier(jnp.sum(probability * grad_prob, axis=-1, keepdims=True))
    grad_score = (probability * (grad_prob - row_delta)).astype(jnp.bfloat16)
    grad_query = jnp.einsum('ehrk,ekhd->erhd', grad_score[:, :, :prompt_len, :].astype(jnp.float32), key_rows.astype(jnp.float32)) * score_scale
    grad_key = jnp.einsum('ehrk,erhd->ekhd', grad_score[:, :, :, :prompt_len].astype(jnp.float32), queries.astype(jnp.float32)) * score_scale
    grad_value = jnp.einsum('ehrk,erhd->ekhd', probs_low[:, :, :, :prompt_len].astype(jnp.float32), upstream.astype(jnp.float32))
    cosine_lead = cosine_table[:prompt_len]
    sine_lead = sine_table[:prompt_len]
    flat_rows = batch_size * prompt_len
    grad_query = unrotate(grad_query, cosine_lead, sine_lead).astype(jnp.bfloat16).reshape(flat_rows, head_count * HD)
    grad_key = unrotate(grad_key, cosine_lead, sine_lead).astype(jnp.bfloat16).reshape(flat_rows, head_count * HD)
    grad_value = grad_value.astype(jnp.bfloat16).reshape(flat_rows, head_count * HD)
    grad_normed = transpose_product(grad_query, w_query) + transpose_product(grad_key, w_key) + transpose_product(grad_value, w_value)
    grad_normed = grad_normed.reshape(batch_size, prompt_len, model_width) * gain
    prompt_rows = wide_rows[:, :prompt_len]
    prompt_inv = inv_rms[:, :prompt_len, None]
    grad_rows = prompt_inv * grad_normed - prompt_rows * prompt_inv ** 3 * lax.optimization_barrier(jnp.mean(grad_normed * prompt_rows, axis=-1, keepdims=True))
    return (output, grad_rows)

def reference(text, prompts, gain, w_query, w_key, w_value, cotangent, task_of, lengths, slot):
    example_count = text.shape[0]
    positions = jnp.arange(example_count, dtype=jnp.int32)

    def one_slot(task_grads, place_id):
        hit_mask = slot == place_id
        source = jnp.sum(jnp.where(hit_mask, positions, 0)).astype(jnp.int32)
        task_id = jnp.sum(jnp.where(hit_mask, task_of, 0)).astype(jnp.int32)
        length = jnp.sum(jnp.where(hit_mask, lengths, 0)).astype(jnp.int32)
        joined = jnp.concatenate([prompts[task_id], text[source]], axis=0)[None]
        output, grad_rows = attention_window(joined, gain, w_query, w_key, w_value, cotangent[place_id][None], length[None], P_SIZE)
        task_grads = task_grads.at[task_id].add(grad_rows[0])
        return (task_grads, output[0])
    prompt_grad, attn_out = lax.scan(one_slot, jnp.zeros((TASKS, P_SIZE, D), jnp.float32), positions)
    return (attn_out, prompt_grad)
```

```python
import math

import jax
import jax.numpy as jnp
import numpy as np
from jax import lax
from jax.experimental import pallas as pl
from jax.experimental.pallas import tpu as pltpu
from jax.sharding import PartitionSpec as P

HD = 128
HALF = 64
EPS = 1e-05
MESH = pl.DeviceIdType.MESH
BF = jnp.bfloat16
F32 = jnp.float32

TEXT = 256
PROMPT = 100
PROMPT_PAD = 128
PROMPT_SENT = 104
ROWS = TEXT + PROMPT
ROWS_PAD = TEXT + PROMPT_PAD
COLS = 640
TILES = COLS // 128
HEADS = 3
WIDTH = HEADS * HD
ALL = 3 * WIDTH
NZ = 8
ND = 32
G_PIECES = 20
R_PIECES = 23
TEXT_SUB = 4
SUBS = ((0, 64), (64, 64), (128, 64), (192, 64), (0, 56), (56, 48))
LAST = ((0, 1, 4), (2, 3, 5))
RS_LAST = ((0, 1, 2), (3, 4))
T_TASK, T_SLOT, T_INV, T_LAST, T_HAS, T_SAME, T_LEN = range(7)


def rope_constants():
    frequency = (np.float32(10000.0) ** (-np.arange(HALF, dtype=np.float32) / np.float32(HALF))).astype(np.float32)
    position = np.concatenate([np.arange(TEXT) + PROMPT, np.arange(PROMPT_PAD)]).astype(np.float32)
    angle = (position[:, None] * frequency[None, :]).astype(np.float32)
    cosine = np.cos(angle.astype(np.float64)).astype(np.float32)
    sine = np.sin(angle.astype(np.float64)).astype(np.float32)
    return np.concatenate([cosine, cosine], axis=1), np.concatenate([-sine, sine], axis=1)


def dot(a, b):
    return lax.dot_general(a, b, (((1,), (0,)), ((), ())), preferred_element_type=F32)


def dot_t(a, b):
    return lax.dot_general(a, b, (((1,), (1,)), ((), ())), preferred_element_type=F32)


def kernel(
    tab, text_hbm, prompts_hbm, gain, wq_hbm, wk_hbm, wv_hbm, cot_hbm, cos_hbm, sin_hbm,
    out_ref, pg_ref,
    text_all, prm_all, pr_loc, ct_loc, w_all, cos_t, sin_t, acc, nb, inv_t, inv_p, s_col,
    sst_all, ssp_all, sx_all,
    pp_src, pp_mid, pp_send, pp_dst,
    ct_src, ct_mid, ct_send, ct_dst,
    ot_src, ot_mid, ot_send, ot_dst,
    gr_src, gr_mid, gr_send, gr_dst, gr_run,
    u_ext, u_t, u_p, o_full, gcat, rs_tx, rs_rx,
    local_sem, ag_s, ag_r, rs_s, rs_r, sm_s, sm_r, a2_s, a2_r,
):
    d = lax.axis_index("dp")
    z = lax.axis_index("tensor")

    def mod8(v):
        return lax.rem(v + 16, NZ)

    loads = [
        pltpu.make_async_copy(prompts_hbm.at[0], pr_loc, local_sem.at[0]),
        pltpu.make_async_copy(text_hbm.at[0], text_all.at[z], local_sem.at[1]),
        pltpu.make_async_copy(cot_hbm.at[0], ct_loc, local_sem.at[2]),
        pltpu.make_async_copy(wq_hbm, w_all.at[:, pl.ds(0, WIDTH)], local_sem.at[3]),
        pltpu.make_async_copy(wk_hbm, w_all.at[:, pl.ds(WIDTH, WIDTH)], local_sem.at[4]),
        pltpu.make_async_copy(wv_hbm, w_all.at[:, pl.ds(2 * WIDTH, WIDTH)], local_sem.at[5]),
        pltpu.make_async_copy(cos_hbm, cos_t, local_sem.at[6]),
        pltpu.make_async_copy(sin_hbm, sin_t, local_sem.at[7]),
    ]
    for load in loads:
        load.start()

    barrier = pltpu.get_barrier_semaphore()

    def greet_dp(i, carry):
        pl.semaphore_signal(barrier, inc=1, device_id={"dp": lax.rem(d + i, ND)}, device_id_type=MESH)
        return carry

    def greet_z(i, carry):
        pl.semaphore_signal(barrier, inc=1, device_id={"tensor": lax.rem(z + i, NZ)}, device_id_type=MESH)
        return carry

    lax.fori_loop(1, NZ, greet_z, 0)
    lax.fori_loop(1, ND, greet_dp, 0)

    def remote(src, dst, s_sem, r_sem, where):
        return pltpu.make_async_remote_copy(
            src_ref=src, dst_ref=dst, send_sem=s_sem, recv_sem=r_sem, device_id=where, device_id_type=MESH
        )

    def middle(pieces):
        mine = lax.div(d * pieces + ND - 1, ND)
        there = jnp.logical_and(mine < pieces, lax.div(mine * ND, pieces) == d)
        return mine, there

    def scatter_one(src, mid, pieces, which, p):
        m = lax.div(p * ND, pieces) if not isinstance(p, int) else (p * ND) // pieces

        @pl.when(m != d)
        def _():
            remote(src.at[p], mid.at[d], a2_s.at[which, 0], a2_r.at[which, 0], {"dp": m}).start()

        @pl.when(m == d)
        def _():
            mid[d] = src[p]

    def scatter(src, mid, pieces, which):
        def body(i, carry):
            scatter_one(src, mid, pieces, which, lax.rem(d + i, pieces))
            return carry

        lax.fori_loop(0, pieces, body, 0)

    def await_middle(mid, which):
        part = mid.at[pl.ds(0, ND - 1)]
        pltpu.make_async_copy(part, part, a2_r.at[which, 0]).wait()

    def relay(value, send, dst, which, mine):
        def body(i, carry):
            e = lax.rem(d + i, ND)
            send[e] = value(e)

            @pl.when(e != d)
            def _():
                remote(send.at[e], dst.at[mine], a2_s.at[which, 1], a2_r.at[which, 1], {"dp": e}).start()

            @pl.when(e == d)
            def _():
                dst[mine] = send[e]

            return carry

        lax.fori_loop(0, ND, body, 0)

    def await_pieces(dst, sem, pieces, there):
        @pl.when(there)
        def _():
            part = dst.at[pl.ds(0, pieces - 1)]
            pltpu.make_async_copy(part, part, sem).wait()

        @pl.when(jnp.logical_not(there))
        def _():
            part = dst.at[pl.ds(0, pieces)]
            pltpu.make_async_copy(part, part, sem).wait()

    def finish_sends(src, send, pieces, which, there):
        await_pieces(src, a2_s.at[which, 0], pieces, there)

        @pl.when(there)
        def _():
            part = send.at[pl.ds(0, ND - 1)]
            pltpu.make_async_copy(part, part, a2_s.at[which, 1]).wait()

    mine_g, there_g = middle(G_PIECES)
    mine_r, there_r = middle(R_PIECES)
    PP, CT, OT, GR = range(4)

    def send_small(ref, which):
        def body(i, carry):
            remote(ref.at[z], ref.at[z], sm_s.at[which], sm_r.at[which], {"tensor": lax.rem(z + i, NZ)}).start()
            return carry

        lax.fori_loop(1, NZ, body, 0)

    def await_small(ref, sem):
        part = ref.at[pl.ds(0, NZ - 1)]
        pltpu.make_async_copy(part, part, sem).wait()

    SIGN = (1, -1)

    def ring_rows(c, j):
        first, count = SUBS[j]
        return (text_all if j < TEXT_SUB else prm_all).at[c, pl.ds(first, count), :]

    def ring_send(way, k, j):
        rows = ring_rows(mod8(z - SIGN[way] * (k - 1)), j)
        return remote(rows, rows, ag_s.at[way, k - 1, j], ag_r.at[way, k - 1, j], {"tensor": mod8(z + SIGN[way])})

    def ring_recv(way, k, j):
        rows = ring_rows(mod8(z - SIGN[way] * k), j)
        return remote(rows, rows, ag_s.at[way, k - 1, j], ag_r.at[way, k - 1, j], {"tensor": mod8(z + SIGN[way])})

    def ring_step(k, subs):
        for j in subs:
            for way in range(2):
                ring_recv(way, k, j).wait_recv()
                if j in LAST[way]:
                    ring_send(way, k + 1, j).start()
                else:

                    @pl.when(k < 3)
                    def _(way=way, j=j):
                        ring_send(way, k + 1, j).start()

    loads[0].wait()
    for c in range(TILES):
        lanes = slice(128 * c, 128 * c + 128)
        for g in range(3):
            pp_src[g * TILES + c] = pr_loc[32 * g : 32 * g + 32, lanes]
        pp_src[3 * TILES + c] = jnp.zeros((32, 128), BF)
        pp_src[3 * TILES + c, 0:4] = pr_loc[96:100, lanes]
        gr_src[3 * TILES + c] = jnp.zeros((32, 128), BF)
    loads[1].wait()
    total = jnp.zeros((TEXT, 128), F32)
    for c in range(TILES):
        x = text_all[z, :, 128 * c : 128 * c + 128].astype(F32)
        total = total + x * x
    sums = jnp.broadcast_to(jnp.sum(total, axis=1, keepdims=True), (TEXT, 128))
    sst_all[z] = sums.T[0:1]
    pl.semaphore_wait(barrier, ND - 1 + NZ - 1)

    for j in range(TEXT_SUB):
        for way in range(2):
            ring_send(way, 1, j).start()
    scatter(pp_src, pp_mid, G_PIECES, PP)
    send_small(sst_all, 0)

    loads[2].wait()
    for p in range(R_PIECES - 1):
        ct_src[p] = ct_loc[16 * p : 16 * p + 16]
    ct_src[R_PIECES - 1] = jnp.zeros((16, WIDTH), BF)
    ct_src[R_PIECES - 1, 0:4] = ct_loc[352:356]
    prm_all[:, PROMPT_SENT:, :] = jnp.zeros((NZ, PROMPT_PAD - PROMPT_SENT, COLS), BF)

    @pl.when(there_g)
    def _():
        await_middle(pp_mid, PP)
        relay(lambda e: pp_mid[tab[T_TASK, e]], pp_send, pp_dst, PP, mine_g)

    scatter(ct_src, ct_mid, R_PIECES, CT)
    acc[...] = jnp.zeros_like(acc)

    ring_step(1, range(TEXT_SUB))
    await_pieces(pp_dst, a2_r.at[PP, 1], G_PIECES, there_g)
    for g in range(4):
        for c in range(TILES):
            prm_all[z, 32 * g : 32 * g + 32, 128 * c : 128 * c + 128] = pp_dst[g * TILES + c]
    for j in range(TEXT_SUB, len(SUBS)):
        for way in range(2):
            ring_send(way, 1, j).start()
    total = jnp.zeros((PROMPT_PAD, 128), F32)
    for c in range(TILES):
        x = prm_all[z, :, 128 * c : 128 * c + 128].astype(F32)
        total = total + x * x
    sums = jnp.broadcast_to(jnp.sum(total, axis=1, keepdims=True), (PROMPT_PAD, 128))
    ssp_all[z] = sums.T[0:1]
    send_small(ssp_all, 1)

    @pl.when(there_r)
    def _():
        await_middle(ct_mid, CT)
        relay(lambda e: ct_mid[tab[T_SLOT, e]], ct_send, ct_dst, CT, mine_r)

    def inverse(ref, rows):
        squares = ref[0]
        for i in range(1, NZ):
            squares = squares + ref[i]
        inv = lax.rsqrt(squares * (1.0 / (NZ * COLS)) + EPS)
        return jnp.broadcast_to(inv, (128, rows)).T

    await_small(sst_all, sm_r.at[0])
    inv_t[...] = inverse(sst_all, TEXT)
    await_small(ssp_all, sm_r.at[1])
    inv_p[...] = inverse(ssp_all, PROMPT_PAD)

    def project(c):
        for t in range(TILES):
            lanes = slice(128 * t, 128 * t + 128)
            scale = gain[c, :, lanes]
            nb[0:TEXT, lanes] = (text_all[c, :, lanes].astype(F32) * inv_t[...] * scale).astype(BF)
            nb[TEXT:, lanes] = (prm_all[c, :, lanes].astype(F32) * inv_p[...] * scale).astype(BF)
        rows = pl.ds(pl.multiple_of(c * COLS, COLS), COLS)
        for n in range(3):
            wide = slice(WIDTH * n, WIDTH * n + WIDTH)
            acc[:, wide] += dot(nb[...], w_all[rows, wide])

    def project_each(k, count):
        def body(i, carry):
            project(mod8(z + k * (i - 1) if count == 3 else z + k * (2 * i - 1)))
            return carry

        lax.fori_loop(0, count, body, 0)

    ring_step(1, range(TEXT_SUB, len(SUBS)))
    for load in loads[3:6]:
        load.wait()
    project_each(1, 3)

    def middle_steps(k, carry):
        ring_step(k, range(len(SUBS)))
        project_each(k, 2)
        return carry

    lax.fori_loop(2, 4, middle_steps, 0)

    length = tab[T_LEN, d]
    await_pieces(ct_dst, a2_r.at[CT, 1], R_PIECES, there_r)
    for p in range(R_PIECES):
        u_ext[16 * p : 16 * p + 16] = ct_dst[p].astype(F32)
    u_ext[16 * R_PIECES :] = jnp.zeros((ROWS_PAD - 16 * R_PIECES, WIDTH), F32)
    text_row = lax.broadcasted_iota(jnp.int32, (TEXT, 128), 0)
    prompt_row = lax.broadcasted_iota(jnp.int32, (PROMPT_PAD, 128), 0)
    for h in range(HEADS):
        lanes = slice(HD * h, HD * h + HD)
        x = u_ext[:, lanes]
        shifted = pltpu.roll(x, ROWS_PAD - PROMPT, 0)
        u_t[:, lanes] = jnp.where(text_row < length, shifted[0:TEXT], 0.0).astype(BF)
        u_p[:, lanes] = jnp.where(prompt_row < PROMPT, x[0:PROMPT_PAD], 0.0).astype(BF)
    loads[6].wait()
    loads[7].wait()

    for way in range(2):
        for j in LAST[way]:
            ring_recv(way, 4, j).wait_recv()
    project(mod8(z + 4))

    score_scale = 1.0 / math.sqrt(HD)
    cos_all, sin_all = cos_t[...], sin_t[...]
    cos_p, sin_p = cos_all[TEXT:], sin_all[TEXT:]
    row_tt = lax.broadcasted_iota(jnp.int32, (TEXT, TEXT), 0)
    col_tt = lax.broadcasted_iota(jnp.int32, (TEXT, TEXT), 1)
    ok_tt = (col_tt <= row_tt) & (col_tt < length)
    ok_tp = lax.broadcasted_iota(jnp.int32, (TEXT, PROMPT_PAD), 1) < PROMPT
    row_pp = lax.broadcasted_iota(jnp.int32, (PROMPT_PAD, PROMPT_PAD), 0)
    col_pp = lax.broadcasted_iota(jnp.int32, (PROMPT_PAD, PROMPT_PAD), 1)
    ok_pp = (col_pp <= row_pp) & (col_pp < PROMPT)
    s_part = jnp.zeros((PROMPT_PAD, HD), F32)
    for h in range(HEADS):
        lanes = slice(HD * h, HD * h + HD)
        pre_q = acc[:, HD * h : HD * h + HD]
        pre_k = acc[:, WIDTH + HD * h : WIDTH + HD * h + HD]
        pre_v = acc[:, 2 * WIDTH + HD * h : 2 * WIDTH + HD * h + HD]
        q = (pre_q * cos_all + pltpu.roll(pre_q, HALF, 1) * sin_all).astype(BF)
        k = (pre_k * cos_all + pltpu.roll(pre_k, HALF, 1) * sin_all).astype(BF)
        v = pre_v.astype(BF)
        qt, qp, kt, kp, vt, vp = q[:TEXT], q[TEXT:], k[:TEXT], k[TEXT:], v[:TEXT], v[TEXT:]
        s_tt = jnp.where(ok_tt, dot_t(qt, kt) * score_scale, -1e30)
        s_tp = jnp.where(ok_tp, dot_t(qt, kp) * score_scale, -1e30)
        s_pp = jnp.where(ok_pp, dot_t(qp, kp) * score_scale, -1e30)
        peak = jnp.maximum(jnp.max(s_tt, axis=1, keepdims=True), jnp.max(s_tp, axis=1, keepdims=True))
        e_tt = jnp.where(ok_tt, jnp.exp(s_tt - peak), 0.0)
        e_tp = jnp.where(ok_tp, jnp.exp(s_tp - peak), 0.0)
        norm = 1.0 / (jnp.sum(e_tt, axis=1, keepdims=True) + jnp.sum(e_tp, axis=1, keepdims=True))
        p_tt, p_tp = e_tt * norm, e_tp * norm
        e_pp = jnp.where(ok_pp, jnp.exp(s_pp - jnp.max(s_pp, axis=1, keepdims=True)), 0.0)
        p_pp = e_pp * (1.0 / jnp.sum(e_pp, axis=1, keepdims=True))
        mixed = dot(p_tt.astype(BF), vt) + dot(p_tp.astype(BF), vp)
        o_full[0:TEXT, lanes] = jnp.where(text_row < length, mixed, 0.0)
        o_full[TEXT:, lanes] = dot(p_pp.astype(BF), vp)
        ut, up = u_t[:, lanes], u_p[:, lanes]
        d_tt, d_tp, d_pp = dot_t(ut, vt), dot_t(ut, vp), dot_t(up, vp)
        delta_t = jnp.sum(p_tt * d_tt, axis=1, keepdims=True) + jnp.sum(p_tp * d_tp, axis=1, keepdims=True)
        g_tp = p_tp * (d_tp - delta_t)
        g_pp = p_pp * (d_pp - jnp.sum(p_pp * d_pp, axis=1, keepdims=True))
        grad_q = dot(g_pp.astype(BF), kp) * score_scale
        grad_k = (dot(g_tp.T.astype(BF), qt) + dot(g_pp.T.astype(BF), qp)) * score_scale
        grad_v = (dot(p_tp.T.astype(BF), ut) + dot(p_pp.T.astype(BF), up)).astype(BF)
        grad_q = (grad_q * cos_p - pltpu.roll(grad_q, HALF, 1) * sin_p).astype(BF)
        grad_k = (grad_k * cos_p - pltpu.roll(grad_k, HALF, 1) * sin_p).astype(BF)
        gcat[:, HD * h : HD * h + HD] = grad_q
        gcat[:, WIDTH + HD * h : WIDTH + HD * h + HD] = grad_k
        gcat[:, 2 * WIDTH + HD * h : 2 * WIDTH + HD * h + HD] = grad_v
        s_part = s_part + grad_q.astype(F32) * pre_q[TEXT:] + grad_k.astype(F32) * pre_k[TEXT:]
        s_part = s_part + grad_v.astype(F32) * pre_v[TEXT:]

    def grad_block(j):
        rows = pl.ds(pl.multiple_of(j * COLS, COLS), COLS)
        return dot_t(gcat[0:PROMPT_SENT], w_all[rows, :])

    def rs_copy(way, step, t):
        return remote(
            rs_tx.at[way, step, t], rs_rx.at[way, step, t], rs_s.at[way, step, t], rs_r.at[way, step, t],
            {"tensor": mod8(z + SIGN[way])},
        )

    def rs_put(way, step, t, value):
        rs_tx[way, step, t] = value.astype(BF)
        rs_copy(way, step, t).start()

    block = grad_block(mod8(z + 4))
    for way in range(2):
        for t in RS_LAST[way]:
            rs_put(way, 0, t, block[:, 128 * t : 128 * t + 128])
    sx_all[z] = jnp.broadcast_to(jnp.sum(s_part, axis=1, keepdims=True), (PROMPT_PAD, 128)).T[0:1]
    send_small(sx_all, 2)

    for h in range(HEADS):
        lanes = slice(HD * h, HD * h + HD)
        x = o_full[:, lanes]
        head_row = lax.broadcasted_iota(jnp.int32, (ROWS_PAD, 128), 0)
        outer = jnp.where(head_row < PROMPT, jnp.concatenate([x[TEXT:], x[:TEXT]], axis=0), pltpu.roll(x, PROMPT, 0))
        outer = outer.astype(BF)
        for p in range(R_PIECES):
            ot_src[p, :, lanes] = outer[16 * p : 16 * p + 16]
    scatter(ot_src, ot_mid, R_PIECES, OT)

    for step in range(1, 4):
        blocks = (grad_block(mod8(z + 4 - step)), grad_block(mod8(z - 4 + step)))
        for t in range(TILES):
            for way in range(2):
                value = blocks[way][:, 128 * t : 128 * t + 128]
                if step > 1 or t in RS_LAST[way]:
                    rs_copy(way, step - 1, t).wait_recv()
                    value = value + rs_rx[way, step - 1, t].astype(F32)
                rs_put(way, step, t, value)
        if step == 2:

            @pl.when(there_r)
            def _():
                await_middle(ot_mid, OT)
                relay(lambda s: ot_mid[tab[T_INV, s]], ot_send, ot_dst, OT, mine_r)

    own = grad_block(z)
    await_small(sx_all, sm_r.at[2])
    total = sx_all[0]
    for i in range(1, NZ):
        total = total + sx_all[i]
    s_col[...] = jnp.broadcast_to(total * (1.0 / (NZ * COLS)), (128, PROMPT_PAD)).T
    inv = inv_p[0:PROMPT_SENT]
    second = inv * inv * s_col[0:PROMPT_SENT]
    for t in range(TILES):
        lanes = slice(128 * t, 128 * t + 128)
        value = own[:, lanes]
        for way in range(2):
            rs_copy(way, 3, t).wait_recv()
            value = value + rs_rx[way, 3, t].astype(F32)
        value = inv * (value * gain[z, :, lanes]) - prm_all[z, 0:PROMPT_SENT, lanes].astype(F32) * second
        value = value.astype(BF)
        for g in range(4):
            p = g * TILES + t
            if g < 3:
                gr_src[p] = value[32 * g : 32 * g + 32]
            else:
                gr_src[p, 0:8] = value[96:104]
            scatter_one(gr_src, gr_mid, G_PIECES, GR, p)

    @pl.when(there_g)
    def _():
        await_middle(gr_mid, GR)

        def run(e, before):
            now = gr_mid[e].astype(F32) + jnp.where(tab[T_SAME, e] > 0, before, 0.0)
            gr_run[e] = now
            return now

        lax.fori_loop(0, ND, run, jnp.zeros((32, 128), F32))
        relay(
            lambda t: jnp.where(tab[T_HAS, t] > 0, gr_run[tab[T_LAST, t]], 0.0).astype(BF),
            gr_send, gr_dst, GR, mine_g,
        )

    await_pieces(ot_dst, a2_r.at[OT, 1], R_PIECES, there_r)
    for p in range(R_PIECES - 1):
        out_ref[0, 16 * p : 16 * p + 16] = ot_dst[p]
    out_ref[0, 352:356] = ot_dst[R_PIECES - 1, 0:4]

    await_pieces(gr_dst, a2_r.at[GR, 1], G_PIECES, there_g)
    for c in range(TILES):
        lanes = slice(128 * c, 128 * c + 128)
        for g in range(3):
            pg_ref[0, 32 * g : 32 * g + 32, lanes] = gr_dst[g * TILES + c].astype(F32)
        pg_ref[0, 96:100, lanes] = gr_dst[3 * TILES + c, 0:4].astype(F32)

    finish_sends(pp_src, pp_send, G_PIECES, PP, there_g)
    finish_sends(ct_src, ct_send, R_PIECES, CT, there_r)
    finish_sends(ot_src, ot_send, R_PIECES, OT, there_r)
    finish_sends(gr_src, gr_send, G_PIECES, GR, there_g)
    await_small(sst_all, sm_s.at[0])
    await_small(ssp_all, sm_s.at[1])
    await_small(sx_all, sm_s.at[2])
    for way in range(2):
        for j in range(len(SUBS)):
            for k in range(1, 5):
                if k < 4 or j in LAST[way]:
                    ring_send(way, k, j).wait_send()
        for step in range(4):
            for t in range(TILES):
                if step > 0 or t in RS_LAST[way]:
                    rs_copy(way, step, t).wait_send()


def on_device(text, prompts, gain, w_query, w_key, w_value, cotangent, task_of, lengths, slot):
    order = jnp.arange(ND, dtype=jnp.int32)
    inverse = jnp.sum(jnp.where(slot[None, :] == order[:, None], order[None, :], 0), axis=1)
    upto = jnp.sum((task_of[None, :] <= order[:, None]).astype(jnp.int32), axis=1)
    here = jnp.sum((task_of[None, :] == order[:, None]).astype(jnp.int32), axis=1)
    same = jnp.concatenate([jnp.zeros((1,), jnp.int32), (task_of[1:] == task_of[:-1]).astype(jnp.int32)])
    table = jnp.stack([task_of, slot, inverse, jnp.maximum(upto - 1, 0), here, same, lengths, lengths])
    cosine, sine = rope_constants()
    vmem, dma = pltpu.VMEM, pltpu.SemaphoreType.DMA
    anywhere = pl.BlockSpec(memory_space=pl.ANY)
    whole = pl.BlockSpec(memory_space=pltpu.VMEM)
    g_piece, r_piece = (32, 128), (16, WIDTH)
    return pl.pallas_call(
        kernel,
        out_shape=(
            jax.ShapeDtypeStruct((1, ROWS, WIDTH), BF),
            jax.ShapeDtypeStruct((1, PROMPT, COLS), F32),
        ),
        in_specs=[pl.BlockSpec(memory_space=pltpu.SMEM), anywhere, anywhere, whole] + [anywhere] * 6,
        out_specs=(whole, whole),
        scratch_shapes=[
            vmem((NZ, TEXT, COLS), BF), vmem((NZ, PROMPT_PAD, COLS), BF), vmem((PROMPT, COLS), BF),
            vmem((ROWS, WIDTH), BF), vmem((NZ * COLS, ALL), BF),
            vmem((ROWS_PAD, HD), F32), vmem((ROWS_PAD, HD), F32),
            vmem((ROWS_PAD, ALL), F32), vmem((ROWS_PAD, COLS), BF),
            vmem((TEXT, 128), F32), vmem((PROMPT_PAD, 128), F32), vmem((PROMPT_PAD, 128), F32),
            vmem((NZ, 1, TEXT), F32), vmem((NZ, 1, PROMPT_PAD), F32), vmem((NZ, 1, PROMPT_PAD), F32),
            vmem((G_PIECES, *g_piece), BF), vmem((ND, *g_piece), BF), vmem((ND, *g_piece), BF), vmem((G_PIECES, *g_piece), BF),
            vmem((R_PIECES, *r_piece), BF), vmem((ND, *r_piece), BF), vmem((ND, *r_piece), BF), vmem((R_PIECES, *r_piece), BF),
            vmem((R_PIECES, *r_piece), BF), vmem((ND, *r_piece), BF), vmem((ND, *r_piece), BF), vmem((R_PIECES, *r_piece), BF),
            vmem((G_PIECES, *g_piece), BF), vmem((ND, *g_piece), BF), vmem((ND, *g_piece), BF), vmem((G_PIECES, *g_piece), BF),
            vmem((ND, *g_piece), F32),
            vmem((ROWS_PAD, WIDTH), F32), vmem((TEXT, WIDTH), BF), vmem((PROMPT_PAD, WIDTH), BF),
            vmem((ROWS_PAD, WIDTH), F32), vmem((PROMPT_PAD, ALL), BF),
            vmem((2, 4, TILES, PROMPT_SENT, 128), BF), vmem((2, 4, TILES, PROMPT_SENT, 128), BF),
            dma((8,)), dma((2, 4, len(SUBS))), dma((2, 4, len(SUBS))), dma((2, 4, TILES)), dma((2, 4, TILES)),
            dma((3,)), dma((3,)), dma((4, 2)), dma((4, 2)),
        ],
        compiler_params=pltpu.CompilerParams(
            collective_id=0, has_side_effects=True, vmem_limit_bytes=60 * 1024 * 1024
        ),
    )(
        table, text, prompts, gain.reshape(NZ, 1, COLS), w_query, w_key, w_value, cotangent,
        jnp.asarray(cosine), jnp.asarray(sine),
    )


def solution(mesh):
    in_specs = (
        P("dp", None, "tensor"),
        P("dp", None, "tensor"),
        P(),
        P(None, "tensor"),
        P(None, "tensor"),
        P(None, "tensor"),
        P("dp", None, "tensor"),
        P(),
        P(),
        P(),
    )
    out_specs = (P("dp", None, "tensor"), P("dp", None, "tensor"))
    return jax.shard_map(on_device, mesh=mesh, in_specs=in_specs, out_specs=out_specs, check_vma=False)
```

```python
import math

import jax
import jax.numpy as jnp
import numpy as np
from jax import lax
from jax.experimental import pallas as pl
from jax.experimental.pallas import tpu as pltpu
from jax.sharding import PartitionSpec as P

HD = 128
HALF = 64
EPS = 1e-05
MESH = pl.DeviceIdType.MESH
BF = jnp.bfloat16
F32 = jnp.float32

TEXT = 256
PROMPT = 100
PROMPT_PAD = 128
PROMPT_SENT = 104
ROWS = TEXT + PROMPT
ROWS_PAD = TEXT + PROMPT_PAD
COLS = 640
TILES = COLS // 128
HEADS = 3
WIDTH = HEADS * HD
ALL = 3 * WIDTH
NZ = 8
ND = 32
G_ROWS = 16
G_HIGH = 6
R_ROWS = 40
R_HIGH = 9
R_PIECES = HEADS * R_HIGH
TEXT_SUB = 4
SUBS = ((0, 64), (64, 64), (128, 64), (192, 64), (0, 56), (56, 48))
LAST = ((0, 1, 4), (2, 3, 5))
RS_LAST = ((0, 1, 2), (3, 4))
RS_ORDER = ((3, 4, 0, 1, 2), (0, 1, 2, 3, 4))


def rope_constants():
    frequency = (np.float32(10000.0) ** (-np.arange(HALF, dtype=np.float32) / np.float32(HALF))).astype(np.float32)
    position = np.concatenate([np.arange(TEXT) + PROMPT, np.arange(PROMPT_PAD)]).astype(np.float32)
    angle = (position[:, None] * frequency[None, :]).astype(np.float32)
    cosine = np.cos(angle.astype(np.float64)).astype(np.float32)
    sine = np.sin(angle.astype(np.float64)).astype(np.float32)
    return np.concatenate([cosine, cosine], axis=1), np.concatenate([-sine, sine], axis=1)


def dot(a, b):
    return lax.dot_general(a, b, (((1,), (0,)), ((), ())), preferred_element_type=F32)


def dot_t(a, b):
    return lax.dot_general(a, b, (((1,), (1,)), ((), ())), preferred_element_type=F32)


def tail_rows(tiles):
    last = jnp.concatenate(tiles + [jnp.zeros((12, 128), F32)], axis=0)
    return last[0:16], last[16:32]


def kernel(
    task_of, lengths, slot, text_hbm, prompts_hbm, gain, wq_hbm, wk_hbm, wv_hbm, cot_hbm, cos_hbm, sin_hbm,
    ot_dst, gr_dst,
    inverse_slot, last_of,
    text_all, prm_all, pr_loc, ct_loc, w_all, cos_t, sin_t, acc, nb, inv_t, inv_p, s_col,
    sst_all, ssp_all, spt_all, sx_all,
    pp_src, pp_mid, pp_send, pp_dst,
    ct_src, ct_mid, ct_send, ct_dst,
    ot_src, ot_mid, ot_send,
    gr_src, gr_mid, gr_send, gr_run,
    u_ext, u_t, u_p, o_full, gcat, rs_own, rs_tx, rs_rx,
    local_sem, ag_s, ag_r, rs_s, rs_r, sm_s, sm_r, a2_s, a2_r,
):
    d = lax.axis_index("dp")
    z = lax.axis_index("tensor")

    def mod8(v):
        return lax.rem(v + 16, NZ)

    loads = [
        pltpu.make_async_copy(prompts_hbm.at[0], pr_loc, local_sem.at[0]),
        pltpu.make_async_copy(text_hbm.at[0], text_all.at[z], local_sem.at[1]),
        pltpu.make_async_copy(cot_hbm.at[0], ct_loc, local_sem.at[2]),
        pltpu.make_async_copy(wq_hbm, w_all.at[:, pl.ds(0, WIDTH)], local_sem.at[3]),
        pltpu.make_async_copy(wk_hbm, w_all.at[:, pl.ds(WIDTH, WIDTH)], local_sem.at[4]),
        pltpu.make_async_copy(wv_hbm, w_all.at[:, pl.ds(2 * WIDTH, WIDTH)], local_sem.at[5]),
        pltpu.make_async_copy(cos_hbm, cos_t, local_sem.at[6]),
        pltpu.make_async_copy(sin_hbm, sin_t, local_sem.at[7]),
    ]
    for load in loads:
        load.start()

    barrier = pltpu.get_barrier_semaphore()

    def greet_dp(i, carry):
        pl.semaphore_signal(barrier, inc=1, device_id={"dp": lax.rem(d + i, ND)}, device_id_type=MESH)
        return carry

    def greet_z(i, carry):
        pl.semaphore_signal(barrier, inc=1, device_id={"tensor": lax.rem(z + i, NZ)}, device_id_type=MESH)
        return carry

    lax.fori_loop(1, NZ, greet_z, 0)
    lax.fori_loop(1, ND, greet_dp, 0)

    def remote(src, dst, s_sem, r_sem, where):
        return pltpu.make_async_remote_copy(
            src_ref=src, dst_ref=dst, send_sem=s_sem, recv_sem=r_sem, device_id=where, device_id_type=MESH
        )

    mine_r = lax.div(d * R_PIECES + ND - 1, ND)
    there_r = jnp.logical_and(mine_r < R_PIECES, lax.div(mine_r * ND, R_PIECES) == d)
    PP, CT, OT, GR, SP = range(5)

    def scatter_one(src, mid, which, p, m):
        @pl.when(m != d)
        def _():
            remote(src.at[p], mid.at[d], a2_s.at[which, 0], a2_r.at[which, 0], {"dp": m}).start()

        @pl.when(m == d)
        def _():
            mid[d] = src[p]

    def scatter_rows(src, mid, which):
        def body(i, carry):
            p = lax.rem(d + i, R_PIECES)
            scatter_one(src, mid, which, p, lax.div(p * ND, R_PIECES))
            return carry

        lax.fori_loop(0, R_PIECES, body, 0)

    def scatter_all(src, mid, which):
        def body(i, carry):
            m = lax.rem(d + i, ND)
            remote(src.at[m], mid.at[d], a2_s.at[which, 0], a2_r.at[which, 0], {"dp": m}).start()
            return carry

        lax.fori_loop(1, ND, body, 0)
        mid[d] = src[d]

    def await_bytes(ref, sem, count):
        part = ref.at[pl.ds(0, count)]
        pltpu.make_async_copy(part, part, sem).wait()

    def await_middle(mid, which):
        await_bytes(mid, a2_r.at[which, 0], ND - 1)

    def relay(value, send, dst, which, mine):
        def body(i, carry):
            e = lax.rem(d + i, ND)
            send[e] = value(e)
            remote(send.at[e], dst.at[mine], a2_s.at[which, 1], a2_r.at[which, 1], {"dp": e}).start()
            return carry

        lax.fori_loop(1, ND, body, 0)
        dst[mine] = value(d)

    def await_rows(ref, sem):
        @pl.when(there_r)
        def _():
            await_bytes(ref, sem, R_PIECES - 1)

        @pl.when(jnp.logical_not(there_r))
        def _():
            await_bytes(ref, sem, R_PIECES)

    def send_small(ref, which):
        def body(i, carry):
            remote(ref.at[z], ref.at[z], sm_s.at[which], sm_r.at[which], {"tensor": lax.rem(z + i, NZ)}).start()
            return carry

        lax.fori_loop(1, NZ, body, 0)

    def await_small(ref, sem):
        part = ref.at[pl.ds(0, NZ - 1)]
        pltpu.make_async_copy(part, part, sem).wait()

    SIGN = (1, -1)

    def ring_rows(c, j):
        first, count = SUBS[j]
        return (text_all if j < TEXT_SUB else prm_all).at[c, pl.ds(first, count), :]

    def ring_send(way, k, j):
        rows = ring_rows(mod8(z - SIGN[way] * (k - 1)), j)
        return remote(rows, rows, ag_s.at[way, k - 1, j], ag_r.at[way, k - 1, j], {"tensor": mod8(z + SIGN[way])})

    def ring_recv(way, k, j):
        rows = ring_rows(mod8(z - SIGN[way] * k), j)
        return remote(rows, rows, ag_s.at[way, k - 1, j], ag_r.at[way, k - 1, j], {"tensor": mod8(z + SIGN[way])})

    def ring_step(k, subs):
        for j in subs:
            for way in range(2):
                if k < 4 or j in LAST[way]:
                    ring_recv(way, k, j).wait_recv()
                    if k < 3 or (k == 3 and j in LAST[way]):
                        ring_send(way, k + 1, j).start()

    TEXT_SUBS, PROMPT_SUBS = range(TEXT_SUB), range(TEXT_SUB, len(SUBS))

    def lane_sums(squares, rows):
        return jnp.broadcast_to(jnp.sum(squares, axis=1, keepdims=True), (rows, 128)).T[0:1]

    def total_of(ref):
        total = ref[0]
        for i in range(1, NZ):
            total = total + ref[i]
        return total

    def inverse(squares, rows):
        inv = lax.rsqrt(squares * (1.0 / (NZ * COLS)) + EPS)
        return jnp.broadcast_to(inv, (128, rows)).T

    def project(c):
        for t in range(TILES):
            lanes = slice(128 * t, 128 * t + 128)
            scale = gain[c, :, lanes]
            nb[0:TEXT, lanes] = (text_all[c, :, lanes].astype(F32) * inv_t[...] * scale).astype(BF)
            nb[TEXT:, lanes] = (prm_all[c, :, lanes].astype(F32) * inv_p[...] * scale).astype(BF)
        rows = pl.ds(pl.multiple_of(c * COLS, COLS), COLS)
        for n in range(3):
            wide = slice(WIDTH * n, WIDTH * n + WIDTH)
            acc[:, wide] += dot(nb[...], w_all[rows, wide])

    def project_each(k, count):
        def body(i, carry):
            project(mod8(z + k * (i - 1) if count == 3 else z + k * (2 * i - 1)))
            return carry

        lax.fori_loop(0, count, body, 0)

    loads[0].wait()
    for c in range(TILES):
        for g in range(G_HIGH):
            pp_src[c * G_HIGH + g] = pr_loc[G_ROWS * g : G_ROWS * g + G_ROWS, 128 * c : 128 * c + 128]
    first, second = tail_rows([pr_loc[96:100, 128 * c : 128 * c + 128].astype(F32) for c in range(TILES)])
    pp_src[30] = first.astype(BF)
    pp_src[31] = second.astype(BF)
    total = jnp.zeros((PROMPT, 128), F32)
    for c in range(TILES):
        x = pr_loc[:, 128 * c : 128 * c + 128].astype(F32)
        total = total + x * x
    total = jnp.concatenate([total, jnp.zeros((PROMPT_PAD - PROMPT, 128), F32)], axis=0)
    ssp_all[z] = lane_sums(total, PROMPT_PAD)
    loads[1].wait()
    total = jnp.zeros((TEXT, 128), F32)
    for c in range(TILES):
        x = text_all[z, :, 128 * c : 128 * c + 128].astype(F32)
        total = total + x * x
    sst_all[z] = lane_sums(total, TEXT)
    def look_up(s, carry):
        found, upto = jnp.int32(0), jnp.int32(0)
        for e in range(ND):
            found = jnp.where(slot[e] == s, e, found)
            upto = upto + jnp.where(task_of[e] <= s, 1, 0)
        inverse_slot[s] = found
        last_of[s] = upto - 1
        return carry

    lax.fori_loop(0, ND, look_up, 0)
    pl.semaphore_wait(barrier, ND - 1 + NZ - 1)
    send_small(ssp_all, 1)
    send_small(sst_all, 0)
    for j in TEXT_SUBS:
        for way in range(2):
            ring_send(way, 1, j).start()
    scatter_all(pp_src, pp_mid, PP)
    loads[2].wait()
    for c in range(HEADS):
        lanes = slice(128 * c, 128 * c + 128)
        for g in range(R_HIGH - 1):
            ct_src[c * R_HIGH + g] = ct_loc[R_ROWS * g : R_ROWS * g + R_ROWS, lanes]
        ct_src[c * R_HIGH + 8] = jnp.zeros((R_ROWS, 128), BF)
        ct_src[c * R_HIGH + 8, 0:36] = ct_loc[320:356, lanes]
    prm_all[:, PROMPT_SENT:, :] = jnp.zeros((NZ, PROMPT_PAD - PROMPT_SENT, COLS), BF)
    acc[...] = jnp.zeros_like(acc)
    await_bytes(ssp_all, sm_r.at[1], NZ - 1)
    spt_all[d] = total_of(ssp_all)

    def tell_dp(i, carry):
        m = lax.rem(d + i, ND)
        remote(spt_all.at[d], spt_all.at[d], a2_s.at[SP, 0], a2_r.at[SP, 0], {"dp": m}).start()
        return carry

    lax.fori_loop(1, ND, tell_dp, 0)
    ring_step(1, (0,))
    await_middle(pp_mid, PP)
    relay(lambda e: pp_mid[task_of[e]], pp_send, pp_dst, PP, d)
    ring_step(1, (1, 2))
    await_bytes(sst_all, sm_r.at[0], NZ - 1)
    inv_t[...] = inverse(total_of(sst_all), TEXT)
    ring_step(1, (3,))
    await_bytes(pp_dst, a2_r.at[PP, 1], ND - 1)
    for c in range(TILES):
        lanes = slice(128 * c, 128 * c + 128)
        for g in range(G_HIGH):
            prm_all[z, G_ROWS * g : G_ROWS * g + G_ROWS, lanes] = pp_dst[c * G_HIGH + g]
        end = pp_dst[30 + c // 4].astype(F32)[4 * (c % 4) : 4 * (c % 4) + 4]
        prm_all[z, 96:104, lanes] = jnp.concatenate([end, jnp.zeros((4, 128), F32)], axis=0).astype(BF)
    for j in PROMPT_SUBS:
        for way in range(2):
            ring_send(way, 1, j).start()
    scatter_rows(ct_src, ct_mid, CT)
    ring_step(2, TEXT_SUBS)
    await_bytes(spt_all, a2_r.at[SP, 0], ND - 1)
    inv_p[...] = inverse(spt_all[task_of[d]], PROMPT_PAD)
    ring_step(1, PROMPT_SUBS)
    for load in loads[3:6]:
        load.wait()
    project_each(1, 3)
    ring_step(3, TEXT_SUBS)
    @pl.when(there_r)
    def _():
        await_middle(ct_mid, CT)
        relay(lambda e: ct_mid[slot[e]], ct_send, ct_dst, CT, mine_r)

    ring_step(2, PROMPT_SUBS)
    project_each(2, 2)
    ring_step(4, TEXT_SUBS)
    ring_step(3, PROMPT_SUBS)
    project_each(3, 2)
    length = lengths[d]
    await_rows(ct_dst, a2_r.at[CT, 1])
    for c in range(HEADS):
        for g in range(R_HIGH):
            u_ext[R_ROWS * g : R_ROWS * g + R_ROWS, 128 * c : 128 * c + 128] = ct_dst[c * R_HIGH + g].astype(F32)
    u_ext[R_ROWS * R_HIGH :] = jnp.zeros((ROWS_PAD - R_ROWS * R_HIGH, WIDTH), F32)
    text_row = lax.broadcasted_iota(jnp.int32, (TEXT, 128), 0)
    prompt_row = lax.broadcasted_iota(jnp.int32, (PROMPT_PAD, 128), 0)
    for h in range(HEADS):
        lanes = slice(HD * h, HD * h + HD)
        x = u_ext[:, lanes]
        shifted = pltpu.roll(x, ROWS_PAD - PROMPT, 0)
        u_t[:, lanes] = jnp.where(text_row < length, shifted[0:TEXT], 0.0).astype(BF)
        u_p[:, lanes] = jnp.where(prompt_row < PROMPT, x[0:PROMPT_PAD], 0.0).astype(BF)
    loads[6].wait()
    loads[7].wait()

    ring_step(4, PROMPT_SUBS)
    project(mod8(z + 4))

    score_scale = 1.0 / math.sqrt(HD)
    cos_all, sin_all = cos_t[...], sin_t[...]
    cos_p, sin_p = cos_all[TEXT:], sin_all[TEXT:]
    row_tt = lax.broadcasted_iota(jnp.int32, (TEXT, TEXT), 0)
    col_tt = lax.broadcasted_iota(jnp.int32, (TEXT, TEXT), 1)
    ok_tt = (col_tt <= row_tt) & (col_tt < length)
    ok_tp = lax.broadcasted_iota(jnp.int32, (TEXT, PROMPT_PAD), 1) < PROMPT
    row_pp = lax.broadcasted_iota(jnp.int32, (PROMPT_PAD, PROMPT_PAD), 0)
    col_pp = lax.broadcasted_iota(jnp.int32, (PROMPT_PAD, PROMPT_PAD), 1)
    ok_pp = (col_pp <= row_pp) & (col_pp < PROMPT)
    s_part = jnp.zeros((PROMPT_PAD, HD), F32)
    for h in range(HEADS):
        lanes = slice(HD * h, HD * h + HD)
        pre_q = acc[:, HD * h : HD * h + HD]
        pre_k = acc[:, WIDTH + HD * h : WIDTH + HD * h + HD]
        pre_v = acc[:, 2 * WIDTH + HD * h : 2 * WIDTH + HD * h + HD]
        q = (pre_q * cos_all + pltpu.roll(pre_q, HALF, 1) * sin_all).astype(BF)
        k = (pre_k * cos_all + pltpu.roll(pre_k, HALF, 1) * sin_all).astype(BF)
        v = pre_v.astype(BF)
        qt, qp, kt, kp, vt, vp = q[:TEXT], q[TEXT:], k[:TEXT], k[TEXT:], v[:TEXT], v[TEXT:]
        s_tt = jnp.where(ok_tt, dot_t(qt, kt) * score_scale, -1e30)
        s_tp = jnp.where(ok_tp, dot_t(qt, kp) * score_scale, -1e30)
        s_pp = jnp.where(ok_pp, dot_t(qp, kp) * score_scale, -1e30)
        peak = jnp.maximum(jnp.max(s_tt, axis=1, keepdims=True), jnp.max(s_tp, axis=1, keepdims=True))
        e_tt = jnp.where(ok_tt, jnp.exp(s_tt - peak), 0.0)
        e_tp = jnp.where(ok_tp, jnp.exp(s_tp - peak), 0.0)
        norm = 1.0 / (jnp.sum(e_tt, axis=1, keepdims=True) + jnp.sum(e_tp, axis=1, keepdims=True))
        p_tt, p_tp = e_tt * norm, e_tp * norm
        e_pp = jnp.where(ok_pp, jnp.exp(s_pp - jnp.max(s_pp, axis=1, keepdims=True)), 0.0)
        p_pp = e_pp * (1.0 / jnp.sum(e_pp, axis=1, keepdims=True))
        mixed = dot(p_tt.astype(BF), vt) + dot(p_tp.astype(BF), vp)
        o_full[0:TEXT, lanes] = jnp.where(text_row < length, mixed, 0.0)
        o_full[TEXT:, lanes] = dot(p_pp.astype(BF), vp)
        ut, up = u_t[:, lanes], u_p[:, lanes]
        d_tt, d_tp, d_pp = dot_t(ut, vt), dot_t(ut, vp), dot_t(up, vp)
        delta_t = jnp.sum(p_tt * d_tt, axis=1, keepdims=True) + jnp.sum(p_tp * d_tp, axis=1, keepdims=True)
        g_tp = p_tp * (d_tp - delta_t)
        g_pp = p_pp * (d_pp - jnp.sum(p_pp * d_pp, axis=1, keepdims=True))
        grad_q = dot(g_pp.astype(BF), kp) * score_scale
        grad_k = (dot(g_tp.T.astype(BF), qt) + dot(g_pp.T.astype(BF), qp)) * score_scale
        grad_v = (dot(p_tp.T.astype(BF), ut) + dot(p_pp.T.astype(BF), up)).astype(BF)
        grad_q = (grad_q * cos_p - pltpu.roll(grad_q, HALF, 1) * sin_p).astype(BF)
        grad_k = (grad_k * cos_p - pltpu.roll(grad_k, HALF, 1) * sin_p).astype(BF)
        gcat[:, HD * h : HD * h + HD] = grad_q
        gcat[:, WIDTH + HD * h : WIDTH + HD * h + HD] = grad_k
        gcat[:, 2 * WIDTH + HD * h : 2 * WIDTH + HD * h + HD] = grad_v
        s_part = s_part + grad_q.astype(F32) * pre_q[TEXT:] + grad_k.astype(F32) * pre_k[TEXT:]
        s_part = s_part + grad_v.astype(F32) * pre_v[TEXT:]

    def grad_block(j):
        rows = pl.ds(pl.multiple_of(j * COLS, COLS), COLS)
        return dot_t(gcat[0:PROMPT_SENT], w_all[rows, :])

    def rs_copy(way, step, t):
        return remote(
            rs_tx.at[way, step, t], rs_rx.at[way, step, t], rs_s.at[way, step, t], rs_r.at[way, step, t],
            {"tensor": mod8(z + SIGN[way])},
        )

    def rs_put(way, step, t, value):
        rs_tx[way, step, t] = value.astype(BF)
        rs_copy(way, step, t).start()

    block = grad_block(mod8(z + 4))
    for way in range(2):
        for t in RS_LAST[way]:
            rs_put(way, 0, t, block[:, 128 * t : 128 * t + 128])
    blocks = (grad_block(mod8(z + 3)), grad_block(mod8(z - 3)))
    for way in range(2):
        for t in RS_LAST[1 - way]:
            rs_put(way, 1, t, blocks[way][:, 128 * t : 128 * t + 128])
    for way in range(2):
        for t in RS_LAST[way]:
            rs_own[way, t] = blocks[way][:, 128 * t : 128 * t + 128]
    sx_all[z] = lane_sums(s_part, PROMPT_PAD)
    send_small(sx_all, 2)

    for h in range(HEADS):
        lanes = slice(HD * h, HD * h + HD)
        x = o_full[:, lanes]
        head_row = lax.broadcasted_iota(jnp.int32, (ROWS_PAD, 128), 0)
        outer = jnp.where(head_row < PROMPT, jnp.concatenate([x[TEXT:], x[:TEXT]], axis=0), pltpu.roll(x, PROMPT, 0))
        outer = outer.astype(BF)
        for g in range(R_HIGH):
            ot_src[h * R_HIGH + g] = outer[R_ROWS * g : R_ROWS * g + R_ROWS]
    scatter_rows(ot_src, ot_mid, OT)

    for t in (0, 1, 2):
        for way in range(2):
            if t < len(RS_LAST[way]):
                tile = RS_LAST[way][t]
                rs_copy(way, 0, tile).wait_recv()
                rs_put(way, 1, tile, rs_own[way, tile] + rs_rx[way, 0, tile].astype(F32))
    for step in (2, 3):
        blocks = (grad_block(mod8(z + 4 - step)), grad_block(mod8(z - 4 + step)))
        for i in range(TILES):
            for way in range(2):
                t = RS_ORDER[way][i]
                rs_copy(way, step - 1, t).wait_recv()
                value = blocks[way][:, 128 * t : 128 * t + 128] + rs_rx[way, step - 1, t].astype(F32)
                rs_put(way, step, t, value)
        if step == 2:

            @pl.when(there_r)
            def _():
                await_middle(ot_mid, OT)
                relay(lambda s: ot_mid[inverse_slot[s]], ot_send, ot_dst, OT, mine_r)

    own = grad_block(z)
    await_bytes(sx_all, sm_r.at[2], NZ - 1)
    s_col[...] = jnp.broadcast_to(total_of(sx_all) * (1.0 / (NZ * COLS)), (128, PROMPT_PAD)).T
    inv = inv_p[0:PROMPT_SENT]
    second = inv * inv * s_col[0:PROMPT_SENT]
    ends = []
    for t in range(TILES):
        lanes = slice(128 * t, 128 * t + 128)
        value = own[:, lanes]
        for way in range(2):
            rs_copy(way, 3, t).wait_recv()
            value = value + rs_rx[way, 3, t].astype(F32)
        value = inv * (value * gain[z, :, lanes]) - prm_all[z, 0:PROMPT_SENT, lanes].astype(F32) * second
        low = value.astype(BF)
        for g in range(G_HIGH):
            p = t * G_HIGH + g
            gr_src[p] = low[G_ROWS * g : G_ROWS * g + G_ROWS]
            scatter_one(gr_src, gr_mid, GR, p, p)
        ends.append(value[96:100])
    first, second = tail_rows(ends)
    for p, value in ((30, first), (31, second)):
        gr_src[p] = value.astype(BF)
        scatter_one(gr_src, gr_mid, GR, p, p)
    await_middle(gr_mid, GR)
    before = jnp.zeros((G_ROWS, 128), F32)
    for e in range(ND):
        now = gr_mid[e].astype(F32)
        if e > 0:
            now = now + jnp.where(task_of[e] == task_of[e - 1], before, 0.0)
        gr_run[e] = now
        before = now

    def task_sum(t):
        at = jnp.maximum(last_of[t], 0)
        return jnp.where(task_of[at] == t, gr_run[at], 0.0).astype(BF)

    relay(task_sum, gr_send, gr_dst, GR, d)
    await_rows(ot_dst, a2_r.at[OT, 1])
    await_bytes(gr_dst, a2_r.at[GR, 1], ND - 1)
    await_bytes(spt_all, a2_s.at[SP, 0], ND - 1)
    await_bytes(pp_src, a2_s.at[PP, 0], ND - 1)
    await_bytes(pp_send, a2_s.at[PP, 1], ND - 1)
    await_bytes(gr_src, a2_s.at[GR, 0], ND - 1)
    await_bytes(gr_send, a2_s.at[GR, 1], ND - 1)
    await_rows(ct_src, a2_s.at[CT, 0])
    await_rows(ot_src, a2_s.at[OT, 0])

    @pl.when(there_r)
    def _():
        await_bytes(ct_send, a2_s.at[CT, 1], ND - 1)
        await_bytes(ot_send, a2_s.at[OT, 1], ND - 1)

    for which, ref in enumerate((sst_all, ssp_all, sx_all)):
        await_bytes(ref, sm_s.at[which], NZ - 1)
    for way in range(2):
        for j in range(len(SUBS)):
            for k in range(1, 5):
                if k < 4 or j in LAST[way]:
                    ring_send(way, k, j).wait_send()
        for step in range(4):
            for t in range(TILES):
                if step > 0 or t in RS_LAST[way]:
                    rs_copy(way, step, t).wait_send()


def assemble(ot_ref, gr_ref, out_ref, pg_ref):
    for c in range(HEADS):
        lanes = slice(128 * c, 128 * c + 128)
        for g in range(R_HIGH - 1):
            out_ref[0, R_ROWS * g : R_ROWS * g + R_ROWS, lanes] = ot_ref[c * R_HIGH + g]
        out_ref[0, 320:356, lanes] = ot_ref[c * R_HIGH + 8, 0:36]
    for c in range(TILES):
        lanes = slice(128 * c, 128 * c + 128)
        for g in range(G_HIGH):
            pg_ref[G_ROWS * g : G_ROWS * g + G_ROWS, 0, lanes] = gr_ref[c * G_HIGH + g].astype(F32)
        pg_ref[96:100, 0, lanes] = gr_ref[30 + c // 4].astype(F32)[4 * (c % 4) : 4 * (c % 4) + 4]


def on_device(text, prompts, gain, w_query, w_key, w_value, cotangent, task_of, lengths, slot):
    cosine, sine = rope_constants()
    vmem, dma, smem = pltpu.VMEM, pltpu.SemaphoreType.DMA, pltpu.SMEM
    anywhere = pl.BlockSpec(memory_space=pl.ANY)
    whole = pl.BlockSpec(memory_space=pltpu.VMEM)
    scalars = pl.BlockSpec(memory_space=pltpu.SMEM)
    g_piece, r_piece = (G_ROWS, 128), (R_ROWS, 128)
    out_pieces, grad_pieces = pl.pallas_call(
        kernel,
        out_shape=(
            pltpu.VMEM((R_PIECES, *r_piece), BF),
            pltpu.VMEM((ND, *g_piece), BF),
        ),
        in_specs=[scalars] * 3 + [anywhere, anywhere, whole] + [anywhere] * 6,
        out_specs=(whole, whole),
        scratch_shapes=[
            smem((ND,), jnp.int32), smem((ND,), jnp.int32),
            vmem((NZ, TEXT, COLS), BF), vmem((NZ, PROMPT_PAD, COLS), BF), vmem((PROMPT, COLS), BF),
            vmem((ROWS, WIDTH), BF), vmem((NZ * COLS, ALL), BF),
            vmem((ROWS_PAD, HD), F32), vmem((ROWS_PAD, HD), F32),
            vmem((ROWS_PAD, ALL), F32), vmem((ROWS_PAD, COLS), BF),
            vmem((TEXT, 128), F32), vmem((PROMPT_PAD, 128), F32), vmem((PROMPT_PAD, 128), F32),
            vmem((NZ, 1, TEXT), F32), vmem((NZ, 1, PROMPT_PAD), F32), vmem((ND, 1, PROMPT_PAD), F32),
            vmem((NZ, 1, PROMPT_PAD), F32),
            vmem((ND, *g_piece), BF), vmem((ND, *g_piece), BF), vmem((ND, *g_piece), BF), vmem((ND, *g_piece), BF),
            vmem((R_PIECES, *r_piece), BF), vmem((ND, *r_piece), BF), vmem((ND, *r_piece), BF), vmem((R_PIECES, *r_piece), BF),
            vmem((R_PIECES, *r_piece), BF), vmem((ND, *r_piece), BF), vmem((ND, *r_piece), BF),
            vmem((ND, *g_piece), BF), vmem((ND, *g_piece), BF), vmem((ND, *g_piece), BF), vmem((ND, *g_piece), F32),
            vmem((ROWS_PAD, WIDTH), F32), vmem((TEXT, WIDTH), BF), vmem((PROMPT_PAD, WIDTH), BF),
            vmem((ROWS_PAD, WIDTH), F32), vmem((PROMPT_PAD, ALL), BF),
            vmem((2, TILES, PROMPT_SENT, 128), F32),
            vmem((2, 4, TILES, PROMPT_SENT, 128), BF), vmem((2, 4, TILES, PROMPT_SENT, 128), BF),
            dma((8,)), dma((2, 4, len(SUBS))), dma((2, 4, len(SUBS))), dma((2, 4, TILES)), dma((2, 4, TILES)),
            dma((3,)), dma((3,)), dma((5, 2)), dma((5, 2)),
        ],
        compiler_params=pltpu.CompilerParams(
            collective_id=0, has_side_effects=True, vmem_limit_bytes=56 * 1024 * 1024
        ),
    )(
        task_of, lengths, slot, text, prompts, gain.reshape(NZ, 1, COLS), w_query, w_key, w_value, cotangent,
        jnp.asarray(cosine), jnp.asarray(sine),
    )
    attn_out, prompt_grad = pl.pallas_call(
        assemble,
        out_shape=(
            jax.ShapeDtypeStruct((1, ROWS, WIDTH), BF),
            jax.ShapeDtypeStruct((PROMPT, 1, COLS), F32),
        ),
        in_specs=[whole, whole],
        out_specs=(whole, whole),
    )(*(pltpu.with_memory_space_constraint(x, pltpu.VMEM) for x in (out_pieces, grad_pieces)))
    return attn_out, prompt_grad.reshape(1, PROMPT, COLS)


def solution(mesh):
    in_specs = (
        P("dp", None, "tensor"),
        P("dp", None, "tensor"),
        P(),
        P(None, "tensor"),
        P(None, "tensor"),
        P(None, "tensor"),
        P("dp", None, "tensor"),
        P(),
        P(),
        P(),
    )
    out_specs = (P("dp", None, "tensor"), P("dp", None, "tensor"))
    return jax.shard_map(on_device, mesh=mesh, in_specs=in_specs, out_specs=out_specs, check_vma=False)
```

```python
import math

import jax
import jax.numpy as jnp
import numpy as np
from jax import lax
from jax.experimental import pallas as pl
from jax.experimental.pallas import tpu as pltpu
from jax.sharding import PartitionSpec as P

HD = 128
HALF = 64
EPS = 1e-05
MESH = pl.DeviceIdType.MESH
BF = jnp.bfloat16
F32 = jnp.float32

TEXT = 256
PROMPT = 100
PROMPT_PAD = 128
PROMPT_SENT = 104
ROWS = TEXT + PROMPT
ROWS_PAD = TEXT + PROMPT_PAD
COLS = 640
TILES = COLS // 128
HEADS = 3
WIDTH = HEADS * HD
ALL = 3 * WIDTH
NZ = 8
ND = 32
G_ROWS = 16
G_HIGH = 6
R_ROWS = 40
R_HIGH = 9
R_PIECES = HEADS * R_HIGH
TEXT_SUB = 4
SUBS = ((0, 64), (64, 64), (128, 64), (192, 64), (0, 56), (56, 48))
LAST = ((0, 1, 4), (2, 3, 5))
LATE = (1, 3)
TEXT_ORDER = ((0, 2), (1, 3), (2, 0), (3, 1))
PROMPT_ORDER = ((4, 5), (5, 4))
RS_LAST = ((0, 1, 2), (3, 4))
RS_ORDER = ((3, 4, 0, 1, 2), (0, 1, 2, 3, 4))


def rope_constants():
    frequency = (np.float32(10000.0) ** (-np.arange(HALF, dtype=np.float32) / np.float32(HALF))).astype(np.float32)
    position = np.concatenate([np.arange(PROMPT_PAD), np.arange(TEXT) + PROMPT]).astype(np.float32)
    angle = (position[:, None] * frequency[None, :]).astype(np.float32)
    cosine = np.cos(angle.astype(np.float64)).astype(np.float32)
    sine = np.sin(angle.astype(np.float64)).astype(np.float32)
    return np.concatenate([cosine, cosine], axis=1), np.concatenate([-sine, sine], axis=1)


def dot(a, b):
    return lax.dot_general(a, b, (((1,), (0,)), ((), ())), preferred_element_type=F32)


def dot_t(a, b):
    return lax.dot_general(a, b, (((1,), (1,)), ((), ())), preferred_element_type=F32)


def tail_rows(tiles):
    last = jnp.concatenate(tiles + [jnp.zeros((12, 128), F32)], axis=0)
    return last[0:16], last[16:32]


def kernel(
    task_hbm, lengths_hbm, slot_hbm, text_hbm, prompts_hbm, gain_hbm, wq_hbm, wk_hbm, wv_hbm, cot_hbm, cos_hbm, sin_hbm,
    ot_dst, gr_dst,
    task_of, lengths, slot, inverse_slot, last_of, gain,
    text_all, prm_all, pr_loc, ct_loc, w_all, cos_t, sin_t, acc, nb, inv_t, inv_p, s_col,
    sst_all, ssp_all, spt_all, sx_all,
    pp_src, pp_mid, pp_send, pp_dst,
    ct_src, ct_mid, ct_send, ct_dst,
    ot_src, ot_mid, ot_send,
    gr_src, gr_mid, gr_send, gr_run,
    u_ext, u_all, o_full, gcat, rs_own, rs_tx, rs_rx,
    local_sem, ag_s, ag_r, rs_s, rs_r, sm_s, sm_r, a2_s, a2_r,
):
    d = lax.axis_index("dp")
    z = lax.axis_index("tensor")

    def mod8(v):
        return lax.rem(v + 16, NZ)

    loads = [
        pltpu.make_async_copy(prompts_hbm.at[0], pr_loc, local_sem.at[0]),
        pltpu.make_async_copy(text_hbm.at[0], text_all.at[z], local_sem.at[1]),
        pltpu.make_async_copy(cot_hbm.at[0], ct_loc, local_sem.at[2]),
        pltpu.make_async_copy(wq_hbm, w_all.at[:, pl.ds(0, WIDTH)], local_sem.at[3]),
        pltpu.make_async_copy(wk_hbm, w_all.at[:, pl.ds(WIDTH, WIDTH)], local_sem.at[4]),
        pltpu.make_async_copy(wv_hbm, w_all.at[:, pl.ds(2 * WIDTH, WIDTH)], local_sem.at[5]),
        pltpu.make_async_copy(cos_hbm, cos_t, local_sem.at[6]),
        pltpu.make_async_copy(sin_hbm, sin_t, local_sem.at[7]),
        pltpu.make_async_copy(gain_hbm, gain, local_sem.at[8]),
        pltpu.make_async_copy(task_hbm, task_of, local_sem.at[9]),
        pltpu.make_async_copy(lengths_hbm, lengths, local_sem.at[10]),
        pltpu.make_async_copy(slot_hbm, slot, local_sem.at[11]),
    ]
    barrier = pltpu.get_barrier_semaphore()

    def greet_dp(i, carry):
        pl.semaphore_signal(barrier, inc=1, device_id={"dp": lax.rem(d + i, ND)}, device_id_type=MESH)
        return carry

    def greet_z(i, carry):
        pl.semaphore_signal(barrier, inc=1, device_id={"tensor": lax.rem(z + i, NZ)}, device_id_type=MESH)
        return carry

    lax.fori_loop(1, NZ, greet_z, 0)
    lax.fori_loop(1, ND, greet_dp, 0)
    for load in loads:
        load.start()

    def remote(src, dst, s_sem, r_sem, where):
        return pltpu.make_async_remote_copy(
            src_ref=src, dst_ref=dst, send_sem=s_sem, recv_sem=r_sem, device_id=where, device_id_type=MESH
        )

    mine_r = lax.div(d * R_PIECES + ND - 1, ND)
    there_r = jnp.logical_and(mine_r < R_PIECES, lax.div(mine_r * ND, R_PIECES) == d)
    PP, CT, OT, GR, SP = range(5)

    def scatter_one(src, mid, which, p, m):
        @pl.when(m != d)
        def _():
            remote(src.at[p], mid.at[d], a2_s.at[which, 0], a2_r.at[which, 0], {"dp": m}).start()

        @pl.when(m == d)
        def _():
            mid[d] = src[p]

    def scatter_rows(src, mid, which):
        def body(i, carry):
            p = lax.rem(d + i, R_PIECES)
            scatter_one(src, mid, which, p, lax.div(p * ND, R_PIECES))
            return carry

        lax.fori_loop(0, R_PIECES, body, 0)

    def scatter_all(src, mid, which):
        def body(i, carry):
            m = lax.rem(d + i, ND)
            remote(src.at[m], mid.at[d], a2_s.at[which, 0], a2_r.at[which, 0], {"dp": m}).start()
            return carry

        lax.fori_loop(1, ND, body, 0)
        mid[d] = src[d]

    def await_bytes(ref, sem, count):
        part = ref.at[pl.ds(0, count)]
        pltpu.make_async_copy(part, part, sem).wait()

    def await_middle(mid, which):
        await_bytes(mid, a2_r.at[which, 0], ND - 1)

    def relay(value, send, dst, which, mine):
        def body(i, carry):
            e = lax.rem(d + i, ND)
            send[e] = value(e)
            remote(send.at[e], dst.at[mine], a2_s.at[which, 1], a2_r.at[which, 1], {"dp": e}).start()
            return carry

        lax.fori_loop(1, ND, body, 0)
        dst[mine] = value(d)

    def await_rows(ref, sem):
        @pl.when(there_r)
        def _():
            await_bytes(ref, sem, R_PIECES - 1)

        @pl.when(jnp.logical_not(there_r))
        def _():
            await_bytes(ref, sem, R_PIECES)

    def send_small(ref, which):
        def body(i, carry):
            remote(ref.at[z], ref.at[z], sm_s.at[which], sm_r.at[which], {"tensor": lax.rem(z + i, NZ)}).start()
            return carry

        lax.fori_loop(1, NZ, body, 0)

    def await_small(ref, sem):
        part = ref.at[pl.ds(0, NZ - 1)]
        pltpu.make_async_copy(part, part, sem).wait()

    SIGN = (1, -1)

    def ring_rows(c, j):
        first, count = SUBS[j]
        return (text_all if j < TEXT_SUB else prm_all).at[c, pl.ds(first, count), :]

    def ring_send(way, k, j):
        rows = ring_rows(mod8(z - SIGN[way] * (k - 1)), j)
        return remote(rows, rows, ag_s.at[way, k - 1, j], ag_r.at[way, k - 1, j], {"tensor": mod8(z + SIGN[way])})

    def ring_recv(way, k, j):
        rows = ring_rows(mod8(z - SIGN[way] * k), j)
        return remote(rows, rows, ag_s.at[way, k - 1, j], ag_r.at[way, k - 1, j], {"tensor": mod8(z + SIGN[way])})

    def ring_step(k, pairs):
        for pair in pairs:
            for way, j in enumerate(pair):
                if k < 4 or j in LAST[way]:
                    ring_recv(way, k, j).wait_recv()
                    if k < 3 or (k == 3 and j in LAST[way] and j not in LATE):
                        ring_send(way, k + 1, j).start()

    def ring_begin(pairs):
        for pair in pairs:
            for way, j in enumerate(pair):
                ring_send(way, 1, j).start()

    def lane_sums(squares, rows):
        return jnp.broadcast_to(jnp.sum(squares, axis=1, keepdims=True), (rows, 128)).T[0:1]

    def total_of(ref):
        total = ref[0]
        for i in range(1, NZ):
            total = total + ref[i]
        return total

    def inverse(squares, rows):
        inv = lax.rsqrt(squares * (1.0 / (NZ * COLS)) + EPS)
        return jnp.broadcast_to(inv, (128, rows)).T

    def normed_text(c):
        for t in range(TILES):
            lanes = slice(128 * t, 128 * t + 128)
            nb[PROMPT_PAD:, lanes] = (text_all[c, :, lanes].astype(F32) * inv_t[...] * gain[c, :, lanes]).astype(BF)

    def normed_prompts(c):
        for t in range(TILES):
            lanes = slice(128 * t, 128 * t + 128)
            nb[0:PROMPT_PAD, lanes] = (prm_all[c, :, lanes].astype(F32) * inv_p[...] * gain[c, :, lanes]).astype(BF)

    def multiply(c):
        rows = pl.ds(pl.multiple_of(c * COLS, COLS), COLS)
        for n in range(3):
            wide = slice(WIDTH * n, WIDTH * n + WIDTH)
            acc[:, wide] += dot(nb[...], w_all[rows, wide])

    def project(c):
        normed_text(c)
        normed_prompts(c)
        multiply(c)

    def project_each(k, count):
        def body(i, carry):
            project(mod8(z + k * (i - 1) if count == 3 else z + k * (2 * i - 1)))
            return carry

        lax.fori_loop(0, count, body, 0)

    loads[0].wait()
    for c in range(TILES):
        for g in range(G_HIGH):
            pp_src[c * G_HIGH + g] = pr_loc[G_ROWS * g : G_ROWS * g + G_ROWS, 128 * c : 128 * c + 128]
    first, second = tail_rows([pr_loc[96:100, 128 * c : 128 * c + 128].astype(F32) for c in range(TILES)])
    pp_src[30] = first.astype(BF)
    pp_src[31] = second.astype(BF)
    total = jnp.zeros((PROMPT, 128), F32)
    for c in range(TILES):
        x = pr_loc[:, 128 * c : 128 * c + 128].astype(F32)
        total = total + x * x
    total = jnp.concatenate([total, jnp.zeros((PROMPT_PAD - PROMPT, 128), F32)], axis=0)
    ssp_all[z] = lane_sums(total, PROMPT_PAD)
    loads[1].wait()
    total = jnp.zeros((TEXT, 128), F32)
    for c in range(TILES):
        x = text_all[z, :, 128 * c : 128 * c + 128].astype(F32)
        total = total + x * x
    sst_all[z] = lane_sums(total, TEXT)
    pl.semaphore_wait(barrier, ND - 1 + NZ - 1)
    send_small(ssp_all, 1)
    send_small(sst_all, 0)
    ring_begin(TEXT_ORDER)
    scatter_all(pp_src, pp_mid, PP)
    loads[2].wait()
    for c in range(HEADS):
        lanes = slice(128 * c, 128 * c + 128)
        for g in range(R_HIGH - 1):
            ct_src[c * R_HIGH + g] = ct_loc[R_ROWS * g : R_ROWS * g + R_ROWS, lanes]
        ct_src[c * R_HIGH + 8] = jnp.zeros((R_ROWS, 128), BF)
        ct_src[c * R_HIGH + 8, 0:36] = ct_loc[320:356, lanes]
    prm_all[:, PROMPT_SENT:, :] = jnp.zeros((NZ, PROMPT_PAD - PROMPT_SENT, COLS), BF)
    acc[...] = jnp.zeros_like(acc)
    for load in loads[9:]:
        load.wait()
    def look_up(s, carry):
        found, upto = jnp.int32(0), jnp.int32(0)
        for e in range(ND):
            found = jnp.where(slot[e] == s, e, found)
            upto = upto + jnp.where(task_of[e] <= s, 1, 0)
        inverse_slot[s] = found
        last_of[s] = upto - 1
        return carry

    lax.fori_loop(0, ND, look_up, 0)
    await_bytes(ssp_all, sm_r.at[1], NZ - 1)
    spt_all[d] = total_of(ssp_all)

    def tell_dp(i, carry):
        m = lax.rem(d + i, ND)
        remote(spt_all.at[d], spt_all.at[d], a2_s.at[SP, 0], a2_r.at[SP, 0], {"dp": m}).start()
        return carry

    lax.fori_loop(1, ND, tell_dp, 0)
    ring_step(1, TEXT_ORDER[:1])
    await_middle(pp_mid, PP)
    relay(lambda e: pp_mid[task_of[e]], pp_send, pp_dst, PP, d)
    ring_step(1, TEXT_ORDER[1:3])
    await_bytes(sst_all, sm_r.at[0], NZ - 1)
    inv_t[...] = inverse(total_of(sst_all), TEXT)
    ring_step(1, TEXT_ORDER[3:])
    await_bytes(pp_dst, a2_r.at[PP, 1], ND - 1)
    for c in range(TILES):
        lanes = slice(128 * c, 128 * c + 128)
        for g in range(G_HIGH):
            prm_all[z, G_ROWS * g : G_ROWS * g + G_ROWS, lanes] = pp_dst[c * G_HIGH + g]
        end = pp_dst[30 + c // 4].astype(F32)[4 * (c % 4) : 4 * (c % 4) + 4]
        prm_all[z, 96:104, lanes] = jnp.concatenate([end, jnp.zeros((4, 128), F32)], axis=0).astype(BF)
    ring_begin(PROMPT_ORDER)
    scatter_rows(ct_src, ct_mid, CT)
    ring_step(2, TEXT_ORDER)
    await_bytes(spt_all, a2_r.at[SP, 0], ND - 1)
    inv_p[...] = inverse(spt_all[task_of[d]], PROMPT_PAD)
    ring_step(1, PROMPT_ORDER)
    for load in loads[3:6] + loads[8:9]:
        load.wait()
    project_each(1, 3)
    ring_step(3, TEXT_ORDER)
    @pl.when(there_r)
    def _():
        await_middle(ct_mid, CT)
        relay(lambda e: ct_mid[slot[e]], ct_send, ct_dst, CT, mine_r)

    ring_step(2, PROMPT_ORDER)
    for way in range(2):
        ring_send(way, 4, LATE[way]).start()
    project_each(2, 2)
    ring_step(3, PROMPT_ORDER)
    project_each(3, 2)
    length = lengths[d]
    await_rows(ct_dst, a2_r.at[CT, 1])
    for c in range(HEADS):
        for g in range(R_HIGH):
            u_ext[R_ROWS * g : R_ROWS * g + R_ROWS, 128 * c : 128 * c + 128] = ct_dst[c * R_HIGH + g].astype(F32)
    u_ext[R_ROWS * R_HIGH :] = jnp.zeros((ROWS_PAD - R_ROWS * R_HIGH, WIDTH), F32)
    row = lax.broadcasted_iota(jnp.int32, (ROWS_PAD, HD), 0)
    live = (row < PROMPT) | ((row >= PROMPT_PAD) & (row < length + PROMPT_PAD))
    for h in range(HEADS):
        lanes = slice(HD * h, HD * h + HD)
        x = u_ext[:, lanes]
        x = jnp.where(row < PROMPT_PAD, x, pltpu.roll(x, PROMPT_PAD - PROMPT, 0))
        u_all[:, lanes] = jnp.where(live, x, 0.0).astype(BF)
    loads[6].wait()
    loads[7].wait()

    ring_step(4, TEXT_ORDER)
    normed_text(mod8(z + 4))
    ring_step(4, PROMPT_ORDER)
    normed_prompts(mod8(z + 4))
    multiply(mod8(z + 4))

    score_scale = 1.0 / math.sqrt(HD)
    cos_all, sin_all = cos_t[...], sin_t[...]
    cos_p, sin_p = cos_all[:PROMPT_PAD], sin_all[:PROMPT_PAD]
    block_rows = [slice(128 * b, 128 * b + 128) for b in range(3)]
    allowed = []
    for b in range(3):
        shape = (128, 128 * b + 128)
        r = lax.broadcasted_iota(jnp.int32, shape, 0) + 128 * b
        c = lax.broadcasted_iota(jnp.int32, shape, 1)
        allowed.append((c <= r) & ((c < PROMPT) | ((c >= PROMPT_PAD) & (c < length + PROMPT_PAD))))
    at_q = [slice(HD * h, HD * h + HD) for h in range(HEADS)]
    at_k = [slice(WIDTH + HD * h, WIDTH + HD * h + HD) for h in range(HEADS)]
    at_v = [slice(2 * WIDTH + HD * h, 2 * WIDTH + HD * h + HD) for h in range(HEADS)]
    every = [(h, b) for h in range(HEADS) for b in range(3)]

    def turned(pre):
        return (pre * cos_all + pltpu.roll(pre, HALF, 1) * sin_all).astype(BF)

    def keys(b):
        return slice(0, 128 * b + 128)

    q = [turned(acc[:, at_q[h]]) for h in range(HEADS)]
    k = [turned(acc[:, at_k[h]]) for h in range(HEADS)]
    v = [acc[:, at_v[h]].astype(BF) for h in range(HEADS)]
    u = [u_all[:, at_q[h]] for h in range(HEADS)]
    scores = {
        (h, b): jnp.where(allowed[b], dot_t(q[h][block_rows[b]], k[h][keys(b)]) * score_scale, -1e30) for h, b in every
    }
    grad_prob = {(h, b): dot_t(u[h][block_rows[b]], v[h][keys(b)]) for h, b in every}
    peak = {at: jnp.max(scores[at], axis=1, keepdims=True) for at in every}
    weights = {at: jnp.exp(scores[at] - peak[at]) for at in every}
    norm = {at: 1.0 / jnp.sum(weights[at], axis=1, keepdims=True) for at in every}
    prob = {at: weights[at] * norm[at] for at in every}
    delta = {at: jnp.sum(prob[at] * grad_prob[at], axis=1, keepdims=True) for at in every}
    grads = {
        at: prob[at][:, :PROMPT_PAD] * (grad_prob[at][:, :PROMPT_PAD] - delta[at]) for at in every
    }
    for h, b in every:
        mixed = dot(prob[h, b].astype(BF), v[h][keys(b)])
        o_full[block_rows[b], at_q[h]] = mixed if b == 0 else jnp.where(live[block_rows[b]], mixed, 0.0)
    grad_t = [jnp.concatenate([grads[h, b].T for b in range(3)], axis=1).astype(BF) for h in range(HEADS)]
    prob_t = [jnp.concatenate([prob[h, b][:, :PROMPT_PAD].T for b in range(3)], axis=1).astype(BF) for h in range(HEADS)]
    grad_q = [dot(grads[h, 0].astype(BF), k[h][:PROMPT_PAD]) * score_scale for h in range(HEADS)]
    grad_k = [dot(grad_t[h], q[h]) * score_scale for h in range(HEADS)]
    grad_v = [dot(prob_t[h], u[h]).astype(BF) for h in range(HEADS)]
    grad_q = [(g * cos_p - pltpu.roll(g, HALF, 1) * sin_p).astype(BF) for g in grad_q]
    grad_k = [(g * cos_p - pltpu.roll(g, HALF, 1) * sin_p).astype(BF) for g in grad_k]
    s_part = jnp.zeros((PROMPT_PAD, HD), F32)
    for h in range(HEADS):
        for at, grad in ((at_q[h], grad_q[h]), (at_k[h], grad_k[h]), (at_v[h], grad_v[h])):
            gcat[:, at] = grad
            s_part = s_part + grad.astype(F32) * acc[0:PROMPT_PAD, at]

    def grad_block(j):
        rows = pl.ds(pl.multiple_of(j * COLS, COLS), COLS)
        return dot_t(gcat[0:PROMPT_SENT], w_all[rows, :])

    def rs_copy(way, step, t):
        return remote(
            rs_tx.at[way, step, t], rs_rx.at[way, step, t], rs_s.at[way, step, t], rs_r.at[way, step, t],
            {"tensor": mod8(z + SIGN[way])},
        )

    def rs_put(way, step, t, value):
        rs_tx[way, step, t] = value.astype(BF)
        rs_copy(way, step, t).start()

    for way in range(2):
        first, count = RS_LAST[way][0], len(RS_LAST[way])
        rows = pl.ds(pl.multiple_of(mod8(z + 4) * COLS + 128 * first, 128), 128 * count)
        part = dot_t(gcat[0:PROMPT_SENT], w_all[rows, :])
        for i in range(count):
            rs_put(way, 0, first + i, part[:, 128 * i : 128 * i + 128])
    blocks = (grad_block(mod8(z + 3)), grad_block(mod8(z - 3)))
    for way in range(2):
        for t in RS_LAST[1 - way]:
            rs_put(way, 1, t, blocks[way][:, 128 * t : 128 * t + 128])
    for way in range(2):
        for t in RS_LAST[way]:
            rs_own[way, t] = blocks[way][:, 128 * t : 128 * t + 128]
    sx_all[z] = lane_sums(s_part, PROMPT_PAD)
    send_small(sx_all, 2)

    for h in range(HEADS):
        lanes = slice(HD * h, HD * h + HD)
        x = o_full[:, lanes]
        outer = jnp.where(row < PROMPT, x, pltpu.roll(x, ROWS_PAD - (PROMPT_PAD - PROMPT), 0))
        outer = outer.astype(BF)
        for g in range(R_HIGH):
            ot_src[h * R_HIGH + g] = outer[R_ROWS * g : R_ROWS * g + R_ROWS]
    scatter_rows(ot_src, ot_mid, OT)

    def relay_out():
        @pl.when(there_r)
        def _():
            await_middle(ot_mid, OT)
            relay(lambda s: ot_mid[inverse_slot[s]], ot_send, ot_dst, OT, mine_r)

    for t in (0, 1, 2):
        for way in range(2):
            if t < len(RS_LAST[way]):
                tile = RS_LAST[way][t]
                rs_copy(way, 0, tile).wait_recv()
                rs_put(way, 1, tile, rs_own[way, tile] + rs_rx[way, 0, tile].astype(F32))
    for step in (2, 3):
        blocks = (grad_block(mod8(z + 4 - step)), grad_block(mod8(z - 4 + step)))
        for i in range(TILES):
            for way in range(2):
                t = RS_ORDER[way][i]
                rs_copy(way, step - 1, t).wait_recv()
                value = blocks[way][:, 128 * t : 128 * t + 128] + rs_rx[way, step - 1, t].astype(F32)
                rs_put(way, step, t, value)
            if step == 3 and i == 1:
                relay_out()

    own = grad_block(z)
    await_bytes(sx_all, sm_r.at[2], NZ - 1)
    s_col[...] = jnp.broadcast_to(total_of(sx_all) * (1.0 / (NZ * COLS)), (128, PROMPT_PAD)).T
    inv = inv_p[0:PROMPT_SENT]
    second = inv * inv * s_col[0:PROMPT_SENT]
    ends = []
    for t in range(TILES):
        lanes = slice(128 * t, 128 * t + 128)
        value = own[:, lanes]
        for way in range(2):
            rs_copy(way, 3, t).wait_recv()
            value = value + rs_rx[way, 3, t].astype(F32)
        value = inv * (value * gain[z, :, lanes]) - prm_all[z, 0:PROMPT_SENT, lanes].astype(F32) * second
        low = value.astype(BF)
        for g in range(G_HIGH):
            p = t * G_HIGH + g
            gr_src[p] = low[G_ROWS * g : G_ROWS * g + G_ROWS]
            scatter_one(gr_src, gr_mid, GR, p, p)
        ends.append(value[96:100])
    first, second = tail_rows(ends)
    for p, value in ((30, first), (31, second)):
        gr_src[p] = value.astype(BF)
        scatter_one(gr_src, gr_mid, GR, p, p)
    await_middle(gr_mid, GR)
    before = jnp.zeros((G_ROWS, 128), F32)
    for e in range(ND):
        now = gr_mid[e].astype(F32)
        if e > 0:
            now = now + jnp.where(task_of[e] == task_of[e - 1], before, 0.0)
        gr_run[e] = now
        before = now

    def task_sum(t):
        at = jnp.maximum(last_of[t], 0)
        return jnp.where(task_of[at] == t, gr_run[at], 0.0).astype(BF)

    relay(task_sum, gr_send, gr_dst, GR, d)
    await_rows(ot_dst, a2_r.at[OT, 1])
    await_bytes(gr_dst, a2_r.at[GR, 1], ND - 1)
    await_bytes(spt_all, a2_s.at[SP, 0], ND - 1)
    await_bytes(pp_src, a2_s.at[PP, 0], ND - 1)
    await_bytes(pp_send, a2_s.at[PP, 1], ND - 1)
    await_bytes(gr_src, a2_s.at[GR, 0], ND - 1)
    await_bytes(gr_send, a2_s.at[GR, 1], ND - 1)
    await_rows(ct_src, a2_s.at[CT, 0])
    await_rows(ot_src, a2_s.at[OT, 0])

    @pl.when(there_r)
    def _():
        await_bytes(ct_send, a2_s.at[CT, 1], ND - 1)
        await_bytes(ot_send, a2_s.at[OT, 1], ND - 1)

    for which, ref in enumerate((sst_all, ssp_all, sx_all)):
        await_bytes(ref, sm_s.at[which], NZ - 1)
    for way in range(2):
        for j in range(len(SUBS)):
            for k in range(1, 5):
                if k < 4 or j in LAST[way]:
                    ring_send(way, k, j).wait_send()
        for step in range(4):
            for t in range(TILES):
                if step > 0 or t in RS_LAST[way]:
                    rs_copy(way, step, t).wait_send()


def assemble(ot_ref, gr_ref, out_ref, pg_ref):
    for c in range(HEADS):
        lanes = slice(128 * c, 128 * c + 128)
        for g in range(R_HIGH - 1):
            out_ref[0, R_ROWS * g : R_ROWS * g + R_ROWS, lanes] = ot_ref[c * R_HIGH + g]
        out_ref[0, 320:356, lanes] = ot_ref[c * R_HIGH + 8, 0:36]
    for c in range(TILES):
        lanes = slice(128 * c, 128 * c + 128)
        for g in range(G_HIGH):
            pg_ref[G_ROWS * g : G_ROWS * g + G_ROWS, 0, lanes] = gr_ref[c * G_HIGH + g].astype(F32)
        pg_ref[96:100, 0, lanes] = gr_ref[30 + c // 4].astype(F32)[4 * (c % 4) : 4 * (c % 4) + 4]


def on_device(text, prompts, gain, w_query, w_key, w_value, cotangent, task_of, lengths, slot):
    cosine, sine = rope_constants()
    vmem, dma, smem = pltpu.VMEM, pltpu.SemaphoreType.DMA, pltpu.SMEM
    anywhere = pl.BlockSpec(memory_space=pl.ANY)
    whole = pl.BlockSpec(memory_space=pltpu.VMEM)
    g_piece, r_piece = (G_ROWS, 128), (R_ROWS, 128)
    out_pieces, grad_pieces = pl.pallas_call(
        kernel,
        out_shape=(
            pltpu.VMEM((R_PIECES, *r_piece), BF),
            pltpu.VMEM((ND, *g_piece), BF),
        ),
        in_specs=[anywhere] * 12,
        out_specs=(whole, whole),
        scratch_shapes=[
            *[smem((ND,), jnp.int32)] * 5, vmem((NZ, 1, COLS), F32),
            vmem((NZ, TEXT, COLS), BF), vmem((NZ, PROMPT_PAD, COLS), BF), vmem((PROMPT, COLS), BF),
            vmem((ROWS, WIDTH), BF), vmem((NZ * COLS, ALL), BF),
            vmem((ROWS_PAD, HD), F32), vmem((ROWS_PAD, HD), F32),
            vmem((ROWS_PAD, ALL), F32), vmem((ROWS_PAD, COLS), BF),
            vmem((TEXT, 128), F32), vmem((PROMPT_PAD, 128), F32), vmem((PROMPT_PAD, 128), F32),
            vmem((NZ, 1, TEXT), F32), vmem((NZ, 1, PROMPT_PAD), F32), vmem((ND, 1, PROMPT_PAD), F32),
            vmem((NZ, 1, PROMPT_PAD), F32),
            vmem((ND, *g_piece), BF), vmem((ND, *g_piece), BF), vmem((ND, *g_piece), BF), vmem((ND, *g_piece), BF),
            vmem((R_PIECES, *r_piece), BF), vmem((ND, *r_piece), BF), vmem((ND, *r_piece), BF), vmem((R_PIECES, *r_piece), BF),
            vmem((R_PIECES, *r_piece), BF), vmem((ND, *r_piece), BF), vmem((ND, *r_piece), BF),
            vmem((ND, *g_piece), BF), vmem((ND, *g_piece), BF), vmem((ND, *g_piece), BF), vmem((ND, *g_piece), F32),
            vmem((ROWS_PAD, WIDTH), F32), vmem((ROWS_PAD, WIDTH), BF),
            vmem((ROWS_PAD, WIDTH), F32), vmem((PROMPT_PAD, ALL), BF),
            vmem((2, TILES, PROMPT_SENT, 128), F32),
            vmem((2, 4, TILES, PROMPT_SENT, 128), BF), vmem((2, 4, TILES, PROMPT_SENT, 128), BF),
            dma((12,)), dma((2, 4, len(SUBS))), dma((2, 4, len(SUBS))), dma((2, 4, TILES)), dma((2, 4, TILES)),
            dma((3,)), dma((3,)), dma((5, 2)), dma((5, 2)),
        ],
        compiler_params=pltpu.CompilerParams(
            collective_id=0, has_side_effects=True, vmem_limit_bytes=56 * 1024 * 1024
        ),
    )(
        task_of, lengths, slot, text, prompts, gain.reshape(NZ, 1, COLS), w_query, w_key, w_value, cotangent,
        jnp.asarray(cosine), jnp.asarray(sine),
    )
    attn_out, prompt_grad = pl.pallas_call(
        assemble,
        out_shape=(
            jax.ShapeDtypeStruct((1, ROWS, WIDTH), BF),
            jax.ShapeDtypeStruct((PROMPT, 1, COLS), F32),
        ),
        in_specs=[whole, whole],
        out_specs=(whole, whole),
    )(*(pltpu.with_memory_space_constraint(x, pltpu.VMEM) for x in (out_pieces, grad_pieces)))
    return attn_out, prompt_grad.reshape(1, PROMPT, COLS)


def solution(mesh):
    in_specs = (
        P("dp", None, "tensor"),
        P("dp", None, "tensor"),
        P(),
        P(None, "tensor"),
        P(None, "tensor"),
        P(None, "tensor"),
        P("dp", None, "tensor"),
        P(),
        P(),
        P(),
    )
    out_specs = (P("dp", None, "tensor"), P("dp", None, "tensor"))
    return jax.shard_map(on_device, mesh=mesh, in_specs=in_specs, out_specs=out_specs, check_vma=False)
```

```python
import math

import jax
import jax.numpy as jnp
import numpy as np
from jax import lax
from jax.experimental import pallas as pl
from jax.experimental.pallas import tpu as pltpu
from jax.sharding import PartitionSpec as P

HD = 128
HALF = 64
EPS = 1e-05
MESH = pl.DeviceIdType.MESH
BF = jnp.bfloat16
F32 = jnp.float32

TEXT = 256
PROMPT = 100
PROMPT_PAD = 128
PROMPT_SENT = 104
ROWS = TEXT + PROMPT
ROWS_PAD = TEXT + PROMPT_PAD
COLS = 640
TILES = COLS // 128
HEADS = 3
WIDTH = HEADS * HD
ALL = 3 * WIDTH
NZ = 8
ND = 32
G_ROWS = 16
G_HIGH = 6
R_ROWS = 40
R_HIGH = 9
R_PIECES = HEADS * R_HIGH
TEXT_SUB = 4
SUBS = ((0, 64), (64, 64), (128, 64), (192, 64), (0, 56), (56, 48))
LAST = ((0, 1, 4), (2, 3, 5))
LATE = (1, 3)
TEXT_ORDER = ((0, 2), (1, 3), (2, 0), (3, 1))
PROMPT_ORDER = ((4, 5), (5, 4))
RS_LAST = ((0, 1, 2), (3, 4))
RS_ORDER = ((3, 4, 0, 1, 2), (0, 1, 2, 3, 4))


def rope_constants():
    frequency = (np.float32(10000.0) ** (-np.arange(HALF, dtype=np.float32) / np.float32(HALF))).astype(np.float32)
    position = np.concatenate([np.arange(PROMPT_PAD), np.arange(TEXT) + PROMPT]).astype(np.float32)
    angle = (position[:, None] * frequency[None, :]).astype(np.float32)
    cosine = np.cos(angle.astype(np.float64)).astype(np.float32)
    sine = np.sin(angle.astype(np.float64)).astype(np.float32)
    return np.concatenate([cosine, cosine], axis=1), np.concatenate([-sine, sine], axis=1)


def dot(a, b):
    return lax.dot_general(a, b, (((1,), (0,)), ((), ())), preferred_element_type=F32)


def dot_t(a, b):
    return lax.dot_general(a, b, (((1,), (1,)), ((), ())), preferred_element_type=F32)


def tail_rows(tiles):
    last = jnp.concatenate(tiles + [jnp.zeros((12, 128), F32)], axis=0)
    return last[0:16], last[16:32]


def kernel(
    task_hbm, lengths_hbm, slot_hbm, text_hbm, prompts_hbm, gain_hbm, wq_hbm, wk_hbm, wv_hbm, cot_hbm, cos_hbm, sin_hbm,
    ot_dst, gr_dst,
    task_of, lengths, slot, inverse_slot, last_of, gain,
    text_all, prm_all, pr_loc, ct_loc, w_all, cos_t, sin_t, acc, nb, inv_t, inv_p, s_col,
    sst_all, ssp_all, spt_all, sx_all,
    pp_src, pp_mid, pp_send, pp_dst,
    ct_src, ct_mid, ct_send, ct_dst,
    ot_src, ot_mid, ot_send,
    gr_src, gr_mid, gr_send, gr_run,
    u_ext, u_all, o_full, gcat, rs_own, rs_tx, rs_rx,
    local_sem, ag_s, ag_r, rs_s, rs_r, sm_s, sm_r, a2_s, a2_r,
):
    d = lax.axis_index("dp")
    z = lax.axis_index("tensor")

    def mod8(v):
        return lax.rem(v + 16, NZ)

    loads = [
        pltpu.make_async_copy(prompts_hbm.at[0], pr_loc, local_sem.at[0]),
        pltpu.make_async_copy(text_hbm.at[0], text_all.at[z], local_sem.at[1]),
        pltpu.make_async_copy(cot_hbm.at[0], ct_loc, local_sem.at[2]),
        pltpu.make_async_copy(wq_hbm, w_all.at[:, pl.ds(0, WIDTH)], local_sem.at[3]),
        pltpu.make_async_copy(wk_hbm, w_all.at[:, pl.ds(WIDTH, WIDTH)], local_sem.at[4]),
        pltpu.make_async_copy(wv_hbm, w_all.at[:, pl.ds(2 * WIDTH, WIDTH)], local_sem.at[5]),
        pltpu.make_async_copy(cos_hbm, cos_t, local_sem.at[6]),
        pltpu.make_async_copy(sin_hbm, sin_t, local_sem.at[7]),
        pltpu.make_async_copy(gain_hbm, gain, local_sem.at[8]),
        pltpu.make_async_copy(task_hbm, task_of, local_sem.at[9]),
        pltpu.make_async_copy(lengths_hbm, lengths, local_sem.at[10]),
        pltpu.make_async_copy(slot_hbm, slot, local_sem.at[11]),
    ]
    barrier = pltpu.get_barrier_semaphore()

    def greet_dp(i, carry):
        pl.semaphore_signal(barrier, inc=1, device_id={"dp": lax.rem(d + i, ND)}, device_id_type=MESH)
        return carry

    def greet_z(i, carry):
        pl.semaphore_signal(barrier, inc=1, device_id={"tensor": lax.rem(z + i, NZ)}, device_id_type=MESH)
        return carry

    lax.fori_loop(1, NZ, greet_z, 0)
    lax.fori_loop(1, ND, greet_dp, 0)
    for load in loads:
        load.start()

    def remote(src, dst, s_sem, r_sem, where):
        return pltpu.make_async_remote_copy(
            src_ref=src, dst_ref=dst, send_sem=s_sem, recv_sem=r_sem, device_id=where, device_id_type=MESH
        )

    mine_r = lax.div(d * R_PIECES + ND - 1, ND)
    there_r = jnp.logical_and(mine_r < R_PIECES, lax.div(mine_r * ND, R_PIECES) == d)
    PP, CT, OT, GR, SP = range(5)

    def scatter_one(src, mid, which, p, m):
        @pl.when(m != d)
        def _():
            remote(src.at[p], mid.at[d], a2_s.at[which, 0], a2_r.at[which, 0], {"dp": m}).start()

        @pl.when(m == d)
        def _():
            mid[d] = src[p]

    def scatter_rows(src, mid, which):
        first = jnp.minimum(mine_r, R_PIECES - 1)

        def send_piece(p):
            m = lax.div(p * ND, R_PIECES)
            remote(src.at[p], mid.at[d], a2_s.at[which, 0], a2_r.at[which, 0], {"dp": m}).start()

        def body(i, carry):
            send_piece(lax.rem(first + i, R_PIECES))
            return carry

        lax.fori_loop(1, R_PIECES, body, 0)

        @pl.when(there_r)
        def _():
            mid[d] = src[first]

        @pl.when(jnp.logical_not(there_r))
        def _():
            send_piece(first)

    def scatter_all(src, mid, which):
        def body(i, carry):
            m = lax.rem(d + i, ND)
            remote(src.at[m], mid.at[d], a2_s.at[which, 0], a2_r.at[which, 0], {"dp": m}).start()
            return carry

        lax.fori_loop(1, ND, body, 0)
        mid[d] = src[d]

    def await_bytes(ref, sem, count):
        part = ref.at[pl.ds(0, count)]
        pltpu.make_async_copy(part, part, sem).wait()

    def await_middle(mid, which):
        await_bytes(mid, a2_r.at[which, 0], ND - 1)

    def relay(value, send, dst, which, mine):
        def body(i, carry):
            e = lax.rem(d + i, ND)
            send[e] = value(e)
            remote(send.at[e], dst.at[mine], a2_s.at[which, 1], a2_r.at[which, 1], {"dp": e}).start()
            return carry

        lax.fori_loop(1, ND, body, 0)
        dst[mine] = value(d)

    def await_rows(ref, sem):
        @pl.when(there_r)
        def _():
            await_bytes(ref, sem, R_PIECES - 1)

        @pl.when(jnp.logical_not(there_r))
        def _():
            await_bytes(ref, sem, R_PIECES)

    def send_small(ref, which):
        def body(i, carry):
            remote(ref.at[z], ref.at[z], sm_s.at[which], sm_r.at[which], {"tensor": lax.rem(z + i, NZ)}).start()
            return carry

        lax.fori_loop(1, NZ, body, 0)

    def await_small(ref, sem):
        part = ref.at[pl.ds(0, NZ - 1)]
        pltpu.make_async_copy(part, part, sem).wait()

    SIGN = (1, -1)

    def ring_rows(c, j):
        first, count = SUBS[j]
        return (text_all if j < TEXT_SUB else prm_all).at[c, pl.ds(first, count), :]

    def ring_send(way, k, j):
        rows = ring_rows(mod8(z - SIGN[way] * (k - 1)), j)
        return remote(rows, rows, ag_s.at[way, k - 1, j], ag_r.at[way, k - 1, j], {"tensor": mod8(z + SIGN[way])})

    def ring_recv(way, k, j):
        rows = ring_rows(mod8(z - SIGN[way] * k), j)
        return remote(rows, rows, ag_s.at[way, k - 1, j], ag_r.at[way, k - 1, j], {"tensor": mod8(z + SIGN[way])})

    def ring_step(k, pairs):
        for pair in pairs:
            for way, j in enumerate(pair):
                if k < 4 or j in LAST[way]:
                    ring_recv(way, k, j).wait_recv()
                    if k < 3 or (k == 3 and j in LAST[way] and j not in LATE):
                        ring_send(way, k + 1, j).start()

    def ring_begin(pairs):
        for pair in pairs:
            for way, j in enumerate(pair):
                ring_send(way, 1, j).start()

    def lane_sums(squares, rows):
        return jnp.broadcast_to(jnp.sum(squares, axis=1, keepdims=True), (rows, 128)).T[0:1]

    def total_of(ref):
        total = ref[0]
        for i in range(1, NZ):
            total = total + ref[i]
        return total

    def inverse(squares, rows):
        inv = lax.rsqrt(squares * (1.0 / (NZ * COLS)) + EPS)
        return jnp.broadcast_to(inv, (128, rows)).T

    def normed_text(c):
        for t in range(TILES):
            lanes = slice(128 * t, 128 * t + 128)
            nb[PROMPT_PAD:, lanes] = (text_all[c, :, lanes].astype(F32) * inv_t[...] * gain[c, :, lanes]).astype(BF)

    def normed_prompts(c):
        for t in range(TILES):
            lanes = slice(128 * t, 128 * t + 128)
            nb[0:PROMPT_PAD, lanes] = (prm_all[c, :, lanes].astype(F32) * inv_p[...] * gain[c, :, lanes]).astype(BF)

    def multiply(c, which=slice(0, ROWS_PAD)):
        rows = pl.ds(pl.multiple_of(c * COLS, COLS), COLS)
        for n in range(3):
            wide = slice(WIDTH * n, WIDTH * n + WIDTH)
            acc[which, wide] += dot(nb[which], w_all[rows, wide])

    def project(c):
        normed_text(c)
        normed_prompts(c)
        multiply(c)

    def project_each(k, count):
        def body(i, carry):
            project(mod8(z + k * (i - 1) if count == 3 else z + k * (2 * i - 1)))
            return carry

        lax.fori_loop(0, count, body, 0)

    loads[0].wait()
    for c in range(TILES):
        for g in range(G_HIGH):
            pp_src[c * G_HIGH + g] = pr_loc[G_ROWS * g : G_ROWS * g + G_ROWS, 128 * c : 128 * c + 128]
    first, second = tail_rows([pr_loc[96:100, 128 * c : 128 * c + 128].astype(F32) for c in range(TILES)])
    pp_src[30] = first.astype(BF)
    pp_src[31] = second.astype(BF)
    total = jnp.zeros((PROMPT, 128), F32)
    for c in range(TILES):
        x = pr_loc[:, 128 * c : 128 * c + 128].astype(F32)
        total = total + x * x
    total = jnp.concatenate([total, jnp.zeros((PROMPT_PAD - PROMPT, 128), F32)], axis=0)
    ssp_all[z] = lane_sums(total, PROMPT_PAD)
    loads[1].wait()
    total = jnp.zeros((TEXT, 128), F32)
    for c in range(TILES):
        x = text_all[z, :, 128 * c : 128 * c + 128].astype(F32)
        total = total + x * x
    sst_all[z] = lane_sums(total, TEXT)
    pl.semaphore_wait(barrier, ND - 1 + NZ - 1)
    send_small(ssp_all, 1)
    send_small(sst_all, 0)
    ring_begin(TEXT_ORDER)
    scatter_all(pp_src, pp_mid, PP)
    loads[2].wait()
    for c in range(HEADS):
        lanes = slice(128 * c, 128 * c + 128)
        for g in range(R_HIGH - 1):
            ct_src[c * R_HIGH + g] = ct_loc[R_ROWS * g : R_ROWS * g + R_ROWS, lanes]
        ct_src[c * R_HIGH + 8] = jnp.zeros((R_ROWS, 128), BF)
        ct_src[c * R_HIGH + 8, 0:36] = ct_loc[320:356, lanes]
    prm_all[:, PROMPT_SENT:, :] = jnp.zeros((NZ, PROMPT_PAD - PROMPT_SENT, COLS), BF)
    acc[...] = jnp.zeros_like(acc)
    for load in loads[9:]:
        load.wait()
    def look_up(s, carry):
        found, upto = jnp.int32(0), jnp.int32(0)
        for e in range(ND):
            found = jnp.where(slot[e] == s, e, found)
            upto = upto + jnp.where(task_of[e] <= s, 1, 0)
        inverse_slot[s] = found
        last_of[s] = upto - 1
        return carry

    lax.fori_loop(0, ND, look_up, 0)
    await_bytes(ssp_all, sm_r.at[1], NZ - 1)
    spt_all[d] = total_of(ssp_all)

    def tell_dp(i, carry):
        m = lax.rem(d + i, ND)
        remote(spt_all.at[d], spt_all.at[d], a2_s.at[SP, 0], a2_r.at[SP, 0], {"dp": m}).start()
        return carry

    lax.fori_loop(1, ND, tell_dp, 0)
    ring_step(1, TEXT_ORDER[:1])
    await_middle(pp_mid, PP)
    relay(lambda e: pp_mid[task_of[e]], pp_send, pp_dst, PP, d)
    ring_step(1, TEXT_ORDER[1:3])
    await_bytes(sst_all, sm_r.at[0], NZ - 1)
    inv_t[...] = inverse(total_of(sst_all), TEXT)
    ring_step(1, TEXT_ORDER[3:])
    await_bytes(pp_dst, a2_r.at[PP, 1], ND - 1)
    for c in range(TILES):
        lanes = slice(128 * c, 128 * c + 128)
        for g in range(G_HIGH):
            prm_all[z, G_ROWS * g : G_ROWS * g + G_ROWS, lanes] = pp_dst[c * G_HIGH + g]
        end = pp_dst[30 + c // 4].astype(F32)[4 * (c % 4) : 4 * (c % 4) + 4]
        prm_all[z, 96:104, lanes] = jnp.concatenate([end, jnp.zeros((4, 128), F32)], axis=0).astype(BF)
    ring_begin(PROMPT_ORDER)
    scatter_rows(ct_src, ct_mid, CT)
    ring_step(2, TEXT_ORDER)
    await_bytes(spt_all, a2_r.at[SP, 0], ND - 1)
    inv_p[...] = inverse(spt_all[task_of[d]], PROMPT_PAD)
    ring_step(1, PROMPT_ORDER)
    for load in loads[3:6] + loads[8:9]:
        load.wait()
    project_each(1, 3)
    ring_step(3, TEXT_ORDER)
    @pl.when(there_r)
    def _():
        await_middle(ct_mid, CT)
        relay(lambda e: ct_mid[slot[e]], ct_send, ct_dst, CT, mine_r)

    ring_step(2, PROMPT_ORDER)
    for way in range(2):
        ring_send(way, 4, LATE[way]).start()
    project_each(2, 2)
    ring_step(3, PROMPT_ORDER)
    project_each(3, 2)
    length = lengths[d]
    await_rows(ct_dst, a2_r.at[CT, 1])
    for c in range(HEADS):
        for g in range(R_HIGH):
            u_ext[R_ROWS * g : R_ROWS * g + R_ROWS, 128 * c : 128 * c + 128] = ct_dst[c * R_HIGH + g].astype(F32)
    u_ext[R_ROWS * R_HIGH :] = jnp.zeros((ROWS_PAD - R_ROWS * R_HIGH, WIDTH), F32)
    row = lax.broadcasted_iota(jnp.int32, (ROWS_PAD, HD), 0)
    live = (row < PROMPT) | ((row >= PROMPT_PAD) & (row < length + PROMPT_PAD))
    for h in range(HEADS):
        lanes = slice(HD * h, HD * h + HD)
        x = u_ext[:, lanes]
        x = jnp.where(row < PROMPT_PAD, x, pltpu.roll(x, PROMPT_PAD - PROMPT, 0))
        u_all[:, lanes] = jnp.where(live, x, 0.0).astype(BF)
    loads[6].wait()
    loads[7].wait()

    ring_step(4, TEXT_ORDER)
    normed_text(mod8(z + 4))
    multiply(mod8(z + 4), slice(PROMPT_PAD, ROWS_PAD))
    ring_step(4, PROMPT_ORDER)
    normed_prompts(mod8(z + 4))
    multiply(mod8(z + 4), slice(0, PROMPT_PAD))

    score_scale = 1.0 / math.sqrt(HD)
    cos_all, sin_all = cos_t[...], sin_t[...]
    cos_p, sin_p = cos_all[:PROMPT_PAD], sin_all[:PROMPT_PAD]
    block_rows = [slice(128 * b, 128 * b + 128) for b in range(3)]
    allowed = []
    for b in range(3):
        shape = (128, 128 * b + 128)
        r = lax.broadcasted_iota(jnp.int32, shape, 0) + 128 * b
        c = lax.broadcasted_iota(jnp.int32, shape, 1)
        allowed.append((c <= r) & ((c < PROMPT) | ((c >= PROMPT_PAD) & (c < length + PROMPT_PAD))))
    at_q = [slice(HD * h, HD * h + HD) for h in range(HEADS)]
    at_k = [slice(WIDTH + HD * h, WIDTH + HD * h + HD) for h in range(HEADS)]
    at_v = [slice(2 * WIDTH + HD * h, 2 * WIDTH + HD * h + HD) for h in range(HEADS)]
    every = [(h, b) for h in range(HEADS) for b in range(3)]

    def turned(pre):
        return (pre * cos_all + pltpu.roll(pre, HALF, 1) * sin_all).astype(BF)

    def keys(b):
        return slice(0, 128 * b + 128)

    q = [turned(acc[:, at_q[h]]) for h in range(HEADS)]
    k = [turned(acc[:, at_k[h]]) for h in range(HEADS)]
    v = [acc[:, at_v[h]].astype(BF) for h in range(HEADS)]
    u = [u_all[:, at_q[h]] for h in range(HEADS)]
    scores = {
        (h, b): jnp.where(allowed[b], dot_t(q[h][block_rows[b]], k[h][keys(b)]) * score_scale, -1e30) for h, b in every
    }
    grad_prob = {(h, b): dot_t(u[h][block_rows[b]], v[h][keys(b)]) for h, b in every}
    peak = {at: jnp.max(scores[at], axis=1, keepdims=True) for at in every}
    weights = {at: jnp.exp(scores[at] - peak[at]) for at in every}
    norm = {at: 1.0 / jnp.sum(weights[at], axis=1, keepdims=True) for at in every}
    prob = {at: weights[at] * norm[at] for at in every}
    delta = {at: jnp.sum(prob[at] * grad_prob[at], axis=1, keepdims=True) for at in every}
    grads = {
        at: prob[at][:, :PROMPT_PAD] * (grad_prob[at][:, :PROMPT_PAD] - delta[at]) for at in every
    }
    for h, b in every:
        mixed = dot(prob[h, b].astype(BF), v[h][keys(b)])
        o_full[block_rows[b], at_q[h]] = mixed if b == 0 else jnp.where(live[block_rows[b]], mixed, 0.0)
    grad_t = [jnp.concatenate([grads[h, b].T for b in range(3)], axis=1).astype(BF) for h in range(HEADS)]
    prob_t = [jnp.concatenate([prob[h, b][:, :PROMPT_PAD].T for b in range(3)], axis=1).astype(BF) for h in range(HEADS)]
    grad_q = [dot(grads[h, 0].astype(BF), k[h][:PROMPT_PAD]) * score_scale for h in range(HEADS)]
    grad_k = [dot(grad_t[h], q[h]) * score_scale for h in range(HEADS)]
    grad_v = [dot(prob_t[h], u[h]).astype(BF) for h in range(HEADS)]
    grad_q = [(g * cos_p - pltpu.roll(g, HALF, 1) * sin_p).astype(BF) for g in grad_q]
    grad_k = [(g * cos_p - pltpu.roll(g, HALF, 1) * sin_p).astype(BF) for g in grad_k]
    s_part = jnp.zeros((PROMPT_PAD, HD), F32)
    for h in range(HEADS):
        for at, grad in ((at_q[h], grad_q[h]), (at_k[h], grad_k[h]), (at_v[h], grad_v[h])):
            gcat[:, at] = grad
            s_part = s_part + grad.astype(F32) * acc[0:PROMPT_PAD, at]

    def grad_block(j):
        rows = pl.ds(pl.multiple_of(j * COLS, COLS), COLS)
        return dot_t(gcat[0:PROMPT_SENT], w_all[rows, :])

    def rs_copy(way, step, t):
        return remote(
            rs_tx.at[way, step, t], rs_rx.at[way, step, t], rs_s.at[way, step, t], rs_r.at[way, step, t],
            {"tensor": mod8(z + SIGN[way])},
        )

    def rs_put(way, step, t, value):
        rs_tx[way, step, t] = value.astype(BF)
        rs_copy(way, step, t).start()

    for way in range(2):
        first, count = RS_LAST[way][0], len(RS_LAST[way])
        rows = pl.ds(pl.multiple_of(mod8(z + 4) * COLS + 128 * first, 128), 128 * count)
        part = dot_t(gcat[0:PROMPT_SENT], w_all[rows, :])
        for i in range(count):
            rs_put(way, 0, first + i, part[:, 128 * i : 128 * i + 128])
    blocks = (grad_block(mod8(z + 3)), grad_block(mod8(z - 3)))
    for way in range(2):
        for t in RS_LAST[1 - way]:
            rs_put(way, 1, t, blocks[way][:, 128 * t : 128 * t + 128])
    for way in range(2):
        for t in RS_LAST[way]:
            rs_own[way, t] = blocks[way][:, 128 * t : 128 * t + 128]
    sx_all[z] = lane_sums(s_part, PROMPT_PAD)
    send_small(sx_all, 2)

    blocks = (grad_block(mod8(z + 2)), grad_block(mod8(z - 2)))
    for t in (0, 1, 2):
        for way in range(2):
            if t < len(RS_LAST[way]):
                tile = RS_LAST[way][t]
                rs_copy(way, 0, tile).wait_recv()
                rs_put(way, 1, tile, rs_own[way, tile] + rs_rx[way, 0, tile].astype(F32))
    for h in range(HEADS):
        lanes = slice(HD * h, HD * h + HD)
        x = o_full[:, lanes]
        outer = jnp.where(row < PROMPT, x, pltpu.roll(x, ROWS_PAD - (PROMPT_PAD - PROMPT), 0))
        outer = outer.astype(BF)
        for g in range(R_HIGH):
            ot_src[h * R_HIGH + g] = outer[R_ROWS * g : R_ROWS * g + R_ROWS]
    scatter_rows(ot_src, ot_mid, OT)

    for step in (2, 3):
        if step == 3:
            blocks = (grad_block(mod8(z + 1)), grad_block(mod8(z - 1)))
        for i in range(TILES):
            for way in range(2):
                t = RS_ORDER[way][i]
                rs_copy(way, step - 1, t).wait_recv()
                value = blocks[way][:, 128 * t : 128 * t + 128] + rs_rx[way, step - 1, t].astype(F32)
                rs_put(way, step, t, value)
    @pl.when(there_r)
    def _():
        await_middle(ot_mid, OT)
        relay(lambda s: ot_mid[inverse_slot[s]], ot_send, ot_dst, OT, mine_r)

    own = grad_block(z)
    await_bytes(sx_all, sm_r.at[2], NZ - 1)
    s_col[...] = jnp.broadcast_to(total_of(sx_all) * (1.0 / (NZ * COLS)), (128, PROMPT_PAD)).T
    inv = inv_p[0:PROMPT_SENT]
    second = inv * inv * s_col[0:PROMPT_SENT]
    ends = []
    for t in range(TILES):
        lanes = slice(128 * t, 128 * t + 128)
        value = own[:, lanes]
        for way in range(2):
            rs_copy(way, 3, t).wait_recv()
            value = value + rs_rx[way, 3, t].astype(F32)
        value = inv * (value * gain[z, :, lanes]) - prm_all[z, 0:PROMPT_SENT, lanes].astype(F32) * second
        low = value.astype(BF)
        for g in range(G_HIGH):
            p = t * G_HIGH + g
            gr_src[p] = low[G_ROWS * g : G_ROWS * g + G_ROWS]
            scatter_one(gr_src, gr_mid, GR, p, p)
        ends.append(value[96:100])
    first, second = tail_rows(ends)
    for p, value in ((30, first), (31, second)):
        gr_src[p] = value.astype(BF)
        scatter_one(gr_src, gr_mid, GR, p, p)
    await_middle(gr_mid, GR)
    before = jnp.zeros((G_ROWS, 128), F32)
    for e in range(ND):
        now = gr_mid[e].astype(F32)
        if e > 0:
            now = now + jnp.where(task_of[e] == task_of[e - 1], before, 0.0)
        gr_run[e] = now
        before = now

    def task_sum(t):
        at = jnp.maximum(last_of[t], 0)
        return jnp.where(task_of[at] == t, gr_run[at], 0.0).astype(BF)

    relay(task_sum, gr_send, gr_dst, GR, d)
    await_rows(ot_dst, a2_r.at[OT, 1])
    await_bytes(gr_dst, a2_r.at[GR, 1], ND - 1)
    await_bytes(spt_all, a2_s.at[SP, 0], ND - 1)
    await_bytes(pp_src, a2_s.at[PP, 0], ND - 1)
    await_bytes(pp_send, a2_s.at[PP, 1], ND - 1)
    await_bytes(gr_src, a2_s.at[GR, 0], ND - 1)
    await_bytes(gr_send, a2_s.at[GR, 1], ND - 1)
    await_rows(ct_src, a2_s.at[CT, 0])
    await_rows(ot_src, a2_s.at[OT, 0])

    @pl.when(there_r)
    def _():
        await_bytes(ct_send, a2_s.at[CT, 1], ND - 1)
        await_bytes(ot_send, a2_s.at[OT, 1], ND - 1)

    for which, ref in enumerate((sst_all, ssp_all, sx_all)):
        await_bytes(ref, sm_s.at[which], NZ - 1)
    for way in range(2):
        for j in range(len(SUBS)):
            for k in range(1, 5):
                if k < 4 or j in LAST[way]:
                    ring_send(way, k, j).wait_send()
        for step in range(4):
            for t in range(TILES):
                if step > 0 or t in RS_LAST[way]:
                    rs_copy(way, step, t).wait_send()


def assemble(ot_ref, gr_ref, out_ref, pg_ref):
    for c in range(HEADS):
        lanes = slice(128 * c, 128 * c + 128)
        for g in range(R_HIGH - 1):
            out_ref[0, R_ROWS * g : R_ROWS * g + R_ROWS, lanes] = ot_ref[c * R_HIGH + g]
        out_ref[0, 320:356, lanes] = ot_ref[c * R_HIGH + 8, 0:36]
    for c in range(TILES):
        lanes = slice(128 * c, 128 * c + 128)
        for g in range(G_HIGH):
            pg_ref[G_ROWS * g : G_ROWS * g + G_ROWS, 0, lanes] = gr_ref[c * G_HIGH + g].astype(F32)
        pg_ref[96:100, 0, lanes] = gr_ref[30 + c // 4].astype(F32)[4 * (c % 4) : 4 * (c % 4) + 4]


def on_device(text, prompts, gain, w_query, w_key, w_value, cotangent, task_of, lengths, slot):
    cosine, sine = rope_constants()
    vmem, dma, smem = pltpu.VMEM, pltpu.SemaphoreType.DMA, pltpu.SMEM
    anywhere = pl.BlockSpec(memory_space=pl.ANY)
    whole = pl.BlockSpec(memory_space=pltpu.VMEM)
    g_piece, r_piece = (G_ROWS, 128), (R_ROWS, 128)
    out_pieces, grad_pieces = pl.pallas_call(
        kernel,
        out_shape=(
            pltpu.VMEM((R_PIECES, *r_piece), BF),
            pltpu.VMEM((ND, *g_piece), BF),
        ),
        in_specs=[anywhere] * 12,
        out_specs=(whole, whole),
        scratch_shapes=[
            *[smem((ND,), jnp.int32)] * 5, vmem((NZ, 1, COLS), F32),
            vmem((NZ, TEXT, COLS), BF), vmem((NZ, PROMPT_PAD, COLS), BF), vmem((PROMPT, COLS), BF),
            vmem((ROWS, WIDTH), BF), vmem((NZ * COLS, ALL), BF),
            vmem((ROWS_PAD, HD), F32), vmem((ROWS_PAD, HD), F32),
            vmem((ROWS_PAD, ALL), F32), vmem((ROWS_PAD, COLS), BF),
            vmem((TEXT, 128), F32), vmem((PROMPT_PAD, 128), F32), vmem((PROMPT_PAD, 128), F32),
            vmem((NZ, 1, TEXT), F32), vmem((NZ, 1, PROMPT_PAD), F32), vmem((ND, 1, PROMPT_PAD), F32),
            vmem((NZ, 1, PROMPT_PAD), F32),
            vmem((ND, *g_piece), BF), vmem((ND, *g_piece), BF), vmem((ND, *g_piece), BF), vmem((ND, *g_piece), BF),
            vmem((R_PIECES, *r_piece), BF), vmem((ND, *r_piece), BF), vmem((ND, *r_piece), BF), vmem((R_PIECES, *r_piece), BF),
            vmem((R_PIECES, *r_piece), BF), vmem((ND, *r_piece), BF), vmem((ND, *r_piece), BF),
            vmem((ND, *g_piece), BF), vmem((ND, *g_piece), BF), vmem((ND, *g_piece), BF), vmem((ND, *g_piece), F32),
            vmem((ROWS_PAD, WIDTH), F32), vmem((ROWS_PAD, WIDTH), BF),
            vmem((ROWS_PAD, WIDTH), F32), vmem((PROMPT_PAD, ALL), BF),
            vmem((2, TILES, PROMPT_SENT, 128), F32),
            vmem((2, 4, TILES, PROMPT_SENT, 128), BF), vmem((2, 4, TILES, PROMPT_SENT, 128), BF),
            dma((12,)), dma((2, 4, len(SUBS))), dma((2, 4, len(SUBS))), dma((2, 4, TILES)), dma((2, 4, TILES)),
            dma((3,)), dma((3,)), dma((5, 2)), dma((5, 2)),
        ],
        compiler_params=pltpu.CompilerParams(
            collective_id=0, has_side_effects=True, vmem_limit_bytes=56 * 1024 * 1024
        ),
    )(
        task_of, lengths, slot, text, prompts, gain.reshape(NZ, 1, COLS), w_query, w_key, w_value, cotangent,
        jnp.asarray(cosine), jnp.asarray(sine),
    )
    attn_out, prompt_grad = pl.pallas_call(
        assemble,
        out_shape=(
            jax.ShapeDtypeStruct((1, ROWS, WIDTH), BF),
            jax.ShapeDtypeStruct((PROMPT, 1, COLS), F32),
        ),
        in_specs=[whole, whole],
        out_specs=(whole, whole),
    )(*(pltpu.with_memory_space_constraint(x, pltpu.VMEM) for x in (out_pieces, grad_pieces)))
    return attn_out, prompt_grad.reshape(1, PROMPT, COLS)


def solution(mesh):
    in_specs = (
        P("dp", None, "tensor"),
        P("dp", None, "tensor"),
        P(),
        P(None, "tensor"),
        P(None, "tensor"),
        P(None, "tensor"),
        P("dp", None, "tensor"),
        P(),
        P(),
        P(),
    )
    out_specs = (P("dp", None, "tensor"), P("dp", None, "tensor"))
    return jax.shard_map(on_device, mesh=mesh, in_specs=in_specs, out_specs=out_specs, check_vma=False)
```

```python
import math

import jax
import jax.numpy as jnp
import numpy as np
from jax import lax
from jax.experimental import pallas as pl
from jax.experimental.pallas import tpu as pltpu
from jax.sharding import PartitionSpec as P

HD = 128
HALF = 64
EPS = 1e-05
MESH = pl.DeviceIdType.MESH
BF = jnp.bfloat16
F32 = jnp.float32

TEXT = 256
PROMPT = 100
PROMPT_PAD = 128
PROMPT_SENT = 104
ROWS = TEXT + PROMPT
ROWS_PAD = TEXT + PROMPT_PAD
COLS = 640
TILES = COLS // 128
HEADS = 3
WIDTH = HEADS * HD
ALL = 3 * WIDTH
NZ = 8
ND = 32
G_ROWS = 16
G_HIGH = 6
R_ROWS = 40
R_HIGH = 9
R_PIECES = HEADS * R_HIGH
TEXT_SUB = 4
SUBS = ((0, 64), (64, 64), (128, 64), (192, 64), (0, 56), (56, 48))
LAST = ((0, 1, 4), (2, 3, 5))
LATE = (1, 3)
TEXT_ORDER = ((0, 2), (1, 3), (2, 0), (3, 1))
PROMPT_ORDER = ((4, 5), (5, 4))
RS_LAST = ((0, 1, 2), (3, 4))
RS_ORDER = ((3, 4, 0, 1, 2), (0, 1, 2, 3, 4))


def rope_constants():
    frequency = (np.float32(10000.0) ** (-np.arange(HALF, dtype=np.float32) / np.float32(HALF))).astype(np.float32)
    position = np.concatenate([np.arange(PROMPT_PAD), np.arange(TEXT) + PROMPT]).astype(np.float32)
    angle = (position[:, None] * frequency[None, :]).astype(np.float32)
    cosine = np.cos(angle.astype(np.float64)).astype(np.float32)
    sine = np.sin(angle.astype(np.float64)).astype(np.float32)
    return np.concatenate([cosine, cosine], axis=1), np.concatenate([-sine, sine], axis=1)


def dot(a, b):
    return lax.dot_general(a, b, (((1,), (0,)), ((), ())), preferred_element_type=F32)


def dot_t(a, b):
    return lax.dot_general(a, b, (((1,), (1,)), ((), ())), preferred_element_type=F32)


def tail_rows(tiles):
    last = jnp.concatenate(tiles + [jnp.zeros((12, 128), F32)], axis=0)
    return last[0:16], last[16:32]


def kernel(
    task_hbm, lengths_hbm, slot_hbm, text_hbm, prompts_hbm, gain_hbm, wq_hbm, wk_hbm, wv_hbm, cot_hbm, cos_hbm, sin_hbm,
    ot_dst, gr_dst,
    task_of, lengths, slot, inverse_slot, last_of, gain,
    text_all, prm_all, pr_loc, ct_loc, w_all, cos_t, sin_t, acc, nb, inv_t, inv_p, s_col,
    sst_all, ssp_all, spt_all, sx_all,
    pp_src, pp_mid, pp_send, pp_dst,
    ct_src, ct_mid, ct_send, ct_dst,
    ot_src, ot_mid, ot_send,
    gr_src, gr_mid, gr_send, gr_run,
    u_ext, u_all, o_full, gcat, rs_own, rs_tx, rs_rx,
    local_sem, ag_s, ag_r, rs_s, rs_r, sm_s, sm_r, a2_s, a2_r,
):
    d = lax.axis_index("dp")
    z = lax.axis_index("tensor")

    def mod8(v):
        return lax.rem(v + 16, NZ)

    loads = [
        pltpu.make_async_copy(prompts_hbm.at[0], pr_loc, local_sem.at[0]),
        pltpu.make_async_copy(text_hbm.at[0], text_all.at[z], local_sem.at[1]),
        pltpu.make_async_copy(cot_hbm.at[0], ct_loc, local_sem.at[2]),
        pltpu.make_async_copy(wq_hbm, w_all.at[:, pl.ds(0, WIDTH)], local_sem.at[3]),
        pltpu.make_async_copy(wk_hbm, w_all.at[:, pl.ds(WIDTH, WIDTH)], local_sem.at[4]),
        pltpu.make_async_copy(wv_hbm, w_all.at[:, pl.ds(2 * WIDTH, WIDTH)], local_sem.at[5]),
        pltpu.make_async_copy(cos_hbm, cos_t, local_sem.at[6]),
        pltpu.make_async_copy(sin_hbm, sin_t, local_sem.at[7]),
        pltpu.make_async_copy(gain_hbm, gain, local_sem.at[8]),
        pltpu.make_async_copy(task_hbm, task_of, local_sem.at[9]),
        pltpu.make_async_copy(lengths_hbm, lengths, local_sem.at[10]),
        pltpu.make_async_copy(slot_hbm, slot, local_sem.at[11]),
    ]
    barrier = pltpu.get_barrier_semaphore()

    def greet_dp(i, carry):
        pl.semaphore_signal(barrier, inc=1, device_id={"dp": lax.rem(d + i, ND)}, device_id_type=MESH)
        return carry

    def greet_z(i, carry):
        pl.semaphore_signal(barrier, inc=1, device_id={"tensor": lax.rem(z + i, NZ)}, device_id_type=MESH)
        return carry

    lax.fori_loop(1, NZ, greet_z, 0)
    lax.fori_loop(1, ND, greet_dp, 0)
    for load in loads:
        load.start()

    def far_first(i):
        return lax.rem(d + lax.rem(i + 15, ND - 1) + 1, ND)

    def remote(src, dst, s_sem, r_sem, where):
        return pltpu.make_async_remote_copy(
            src_ref=src, dst_ref=dst, send_sem=s_sem, recv_sem=r_sem, device_id=where, device_id_type=MESH
        )

    mine_r = lax.div(d * R_PIECES + ND - 1, ND)
    there_r = jnp.logical_and(mine_r < R_PIECES, lax.div(mine_r * ND, R_PIECES) == d)
    PP, CT, OT, GR, SP = range(5)

    def scatter_one(src, mid, which, p, m):
        @pl.when(m != d)
        def _():
            remote(src.at[p], mid.at[d], a2_s.at[which, 0], a2_r.at[which, 0], {"dp": m}).start()

        @pl.when(m == d)
        def _():
            mid[d] = src[p]

    def scatter_rows(src, mid, which):
        first = jnp.minimum(mine_r, R_PIECES - 1)

        def send_piece(p):
            m = lax.div(p * ND, R_PIECES)
            remote(src.at[p], mid.at[d], a2_s.at[which, 0], a2_r.at[which, 0], {"dp": m}).start()

        def body(i, carry):
            send_piece(lax.rem(first + i, R_PIECES))
            return carry

        lax.fori_loop(1, R_PIECES, body, 0)

        @pl.when(there_r)
        def _():
            mid[d] = src[first]

        @pl.when(jnp.logical_not(there_r))
        def _():
            send_piece(first)

    def scatter_all(src, mid, which):
        def body(i, carry):
            m = far_first(i)
            remote(src.at[m], mid.at[d], a2_s.at[which, 0], a2_r.at[which, 0], {"dp": m}).start()
            return carry

        lax.fori_loop(1, ND, body, 0)
        mid[d] = src[d]

    def await_bytes(ref, sem, count):
        part = ref.at[pl.ds(0, count)]
        pltpu.make_async_copy(part, part, sem).wait()

    def await_middle(mid, which):
        await_bytes(mid, a2_r.at[which, 0], ND - 1)

    def relay(value, send, dst, which, mine):
        def body(i, carry):
            e = far_first(i)
            send[e] = value(e)
            remote(send.at[e], dst.at[mine], a2_s.at[which, 1], a2_r.at[which, 1], {"dp": e}).start()
            return carry

        lax.fori_loop(1, ND, body, 0)
        dst[mine] = value(d)

    def await_rows(ref, sem):
        @pl.when(there_r)
        def _():
            await_bytes(ref, sem, R_PIECES - 1)

        @pl.when(jnp.logical_not(there_r))
        def _():
            await_bytes(ref, sem, R_PIECES)

    def send_small(ref, which):
        def body(i, carry):
            remote(ref.at[z], ref.at[z], sm_s.at[which], sm_r.at[which], {"tensor": lax.rem(z + i, NZ)}).start()
            return carry

        lax.fori_loop(1, NZ, body, 0)

    def await_small(ref, sem):
        part = ref.at[pl.ds(0, NZ - 1)]
        pltpu.make_async_copy(part, part, sem).wait()

    SIGN = (1, -1)

    def ring_rows(c, j):
        first, count = SUBS[j]
        return (text_all if j < TEXT_SUB else prm_all).at[c, pl.ds(first, count), :]

    def ring_send(way, k, j):
        rows = ring_rows(mod8(z - SIGN[way] * (k - 1)), j)
        return remote(rows, rows, ag_s.at[way, k - 1, j], ag_r.at[way, k - 1, j], {"tensor": mod8(z + SIGN[way])})

    def ring_recv(way, k, j):
        rows = ring_rows(mod8(z - SIGN[way] * k), j)
        return remote(rows, rows, ag_s.at[way, k - 1, j], ag_r.at[way, k - 1, j], {"tensor": mod8(z + SIGN[way])})

    def ring_step(k, pairs):
        for pair in pairs:
            for way, j in enumerate(pair):
                if k < 4 or j in LAST[way]:
                    ring_recv(way, k, j).wait_recv()
                    if k < 3 or (k == 3 and j in LAST[way] and j not in LATE):
                        ring_send(way, k + 1, j).start()

    def ring_begin(pairs):
        for pair in pairs:
            for way, j in enumerate(pair):
                ring_send(way, 1, j).start()

    def lane_sums(squares, rows):
        return jnp.broadcast_to(jnp.sum(squares, axis=1, keepdims=True), (rows, 128)).T[0:1]

    def total_of(ref):
        total = ref[0]
        for i in range(1, NZ):
            total = total + ref[i]
        return total

    def inverse(squares, rows):
        inv = lax.rsqrt(squares * (1.0 / (NZ * COLS)) + EPS)
        return jnp.broadcast_to(inv, (128, rows)).T

    def normed_text(c):
        for t in range(TILES):
            lanes = slice(128 * t, 128 * t + 128)
            nb[PROMPT_PAD:, lanes] = (text_all[c, :, lanes].astype(F32) * inv_t[...] * gain[c, :, lanes]).astype(BF)

    def normed_prompts(c):
        for t in range(TILES):
            lanes = slice(128 * t, 128 * t + 128)
            nb[0:PROMPT_PAD, lanes] = (prm_all[c, :, lanes].astype(F32) * inv_p[...] * gain[c, :, lanes]).astype(BF)

    def multiply(c, which=slice(0, ROWS_PAD)):
        rows = pl.ds(pl.multiple_of(c * COLS, COLS), COLS)
        for n in range(3):
            wide = slice(WIDTH * n, WIDTH * n + WIDTH)
            acc[which, wide] += dot(nb[which], w_all[rows, wide])

    def project(c):
        normed_text(c)
        normed_prompts(c)
        multiply(c)

    def project_each(k, count):
        def body(i, carry):
            project(mod8(z + k * (i - 1) if count == 3 else z + k * (2 * i - 1)))
            return carry

        lax.fori_loop(0, count, body, 0)

    loads[0].wait()
    for c in range(TILES):
        for g in range(G_HIGH):
            pp_src[c * G_HIGH + g] = pr_loc[G_ROWS * g : G_ROWS * g + G_ROWS, 128 * c : 128 * c + 128]
    first, second = tail_rows([pr_loc[96:100, 128 * c : 128 * c + 128].astype(F32) for c in range(TILES)])
    pp_src[30] = first.astype(BF)
    pp_src[31] = second.astype(BF)
    total = jnp.zeros((PROMPT, 128), F32)
    for c in range(TILES):
        x = pr_loc[:, 128 * c : 128 * c + 128].astype(F32)
        total = total + x * x
    total = jnp.concatenate([total, jnp.zeros((PROMPT_PAD - PROMPT, 128), F32)], axis=0)
    ssp_all[z] = lane_sums(total, PROMPT_PAD)
    loads[1].wait()
    total = jnp.zeros((TEXT, 128), F32)
    for c in range(TILES):
        x = text_all[z, :, 128 * c : 128 * c + 128].astype(F32)
        total = total + x * x
    sst_all[z] = lane_sums(total, TEXT)
    pl.semaphore_wait(barrier, ND - 1 + NZ - 1)
    send_small(ssp_all, 1)
    send_small(sst_all, 0)
    ring_begin(TEXT_ORDER)
    scatter_all(pp_src, pp_mid, PP)
    loads[2].wait()
    for c in range(HEADS):
        lanes = slice(128 * c, 128 * c + 128)
        for g in range(R_HIGH - 1):
            ct_src[c * R_HIGH + g] = ct_loc[R_ROWS * g : R_ROWS * g + R_ROWS, lanes]
        ct_src[c * R_HIGH + 8] = jnp.zeros((R_ROWS, 128), BF)
        ct_src[c * R_HIGH + 8, 0:36] = ct_loc[320:356, lanes]
    prm_all[:, PROMPT_SENT:, :] = jnp.zeros((NZ, PROMPT_PAD - PROMPT_SENT, COLS), BF)
    acc[...] = jnp.zeros_like(acc)
    for load in loads[9:]:
        load.wait()
    def look_up(s, carry):
        found, upto = jnp.int32(0), jnp.int32(0)
        for e in range(ND):
            found = jnp.where(slot[e] == s, e, found)
            upto = upto + jnp.where(task_of[e] <= s, 1, 0)
        inverse_slot[s] = found
        last_of[s] = upto - 1
        return carry

    lax.fori_loop(0, ND, look_up, 0)
    await_bytes(ssp_all, sm_r.at[1], NZ - 1)
    spt_all[d] = total_of(ssp_all)

    def tell_dp(i, carry):
        m = lax.rem(d + i, ND)
        remote(spt_all.at[d], spt_all.at[d], a2_s.at[SP, 0], a2_r.at[SP, 0], {"dp": m}).start()
        return carry

    lax.fori_loop(1, ND, tell_dp, 0)
    ring_step(1, TEXT_ORDER[:1])
    await_middle(pp_mid, PP)
    relay(lambda e: pp_mid[task_of[e]], pp_send, pp_dst, PP, d)
    ring_step(1, TEXT_ORDER[1:3])
    await_bytes(sst_all, sm_r.at[0], NZ - 1)
    inv_t[...] = inverse(total_of(sst_all), TEXT)
    ring_step(1, TEXT_ORDER[3:])
    await_bytes(pp_dst, a2_r.at[PP, 1], ND - 1)
    for c in range(TILES):
        lanes = slice(128 * c, 128 * c + 128)
        for g in range(G_HIGH):
            prm_all[z, G_ROWS * g : G_ROWS * g + G_ROWS, lanes] = pp_dst[c * G_HIGH + g]
        end = pp_dst[30 + c // 4].astype(F32)[4 * (c % 4) : 4 * (c % 4) + 4]
        prm_all[z, 96:104, lanes] = jnp.concatenate([end, jnp.zeros((4, 128), F32)], axis=0).astype(BF)
    ring_begin(PROMPT_ORDER)
    scatter_rows(ct_src, ct_mid, CT)
    ring_step(2, TEXT_ORDER)
    await_bytes(spt_all, a2_r.at[SP, 0], ND - 1)
    inv_p[...] = inverse(spt_all[task_of[d]], PROMPT_PAD)
    ring_step(1, PROMPT_ORDER)
    for load in loads[3:6] + loads[8:9]:
        load.wait()
    project_each(1, 3)
    ring_step(3, TEXT_ORDER)
    @pl.when(there_r)
    def _():
        await_middle(ct_mid, CT)
        relay(lambda e: ct_mid[slot[e]], ct_send, ct_dst, CT, mine_r)

    ring_step(2, PROMPT_ORDER)
    for way in range(2):
        ring_send(way, 4, LATE[way]).start()
    project_each(2, 2)
    ring_step(3, PROMPT_ORDER)
    project_each(3, 2)
    length = lengths[d]
    await_rows(ct_dst, a2_r.at[CT, 1])
    for c in range(HEADS):
        for g in range(R_HIGH):
            u_ext[R_ROWS * g : R_ROWS * g + R_ROWS, 128 * c : 128 * c + 128] = ct_dst[c * R_HIGH + g].astype(F32)
    u_ext[R_ROWS * R_HIGH :] = jnp.zeros((ROWS_PAD - R_ROWS * R_HIGH, WIDTH), F32)
    row = lax.broadcasted_iota(jnp.int32, (ROWS_PAD, HD), 0)
    live = (row < PROMPT) | ((row >= PROMPT_PAD) & (row < length + PROMPT_PAD))
    for h in range(HEADS):
        lanes = slice(HD * h, HD * h + HD)
        x = u_ext[:, lanes]
        x = jnp.where(row < PROMPT_PAD, x, pltpu.roll(x, PROMPT_PAD - PROMPT, 0))
        u_all[:, lanes] = jnp.where(live, x, 0.0).astype(BF)
    loads[6].wait()
    loads[7].wait()

    ring_step(4, TEXT_ORDER)
    normed_text(mod8(z + 4))
    multiply(mod8(z + 4), slice(PROMPT_PAD, ROWS_PAD))
    ring_step(4, PROMPT_ORDER)
    normed_prompts(mod8(z + 4))
    multiply(mod8(z + 4), slice(0, PROMPT_PAD))

    score_scale = 1.0 / math.sqrt(HD)
    cos_all, sin_all = cos_t[...], sin_t[...]
    cos_p, sin_p = cos_all[:PROMPT_PAD], sin_all[:PROMPT_PAD]
    block_rows = [slice(128 * b, 128 * b + 128) for b in range(3)]
    allowed = []
    for b in range(3):
        shape = (128, 128 * b + 128)
        r = lax.broadcasted_iota(jnp.int32, shape, 0) + 128 * b
        c = lax.broadcasted_iota(jnp.int32, shape, 1)
        allowed.append((c <= r) & ((c < PROMPT) | ((c >= PROMPT_PAD) & (c < length + PROMPT_PAD))))
    at_q = [slice(HD * h, HD * h + HD) for h in range(HEADS)]
    at_k = [slice(WIDTH + HD * h, WIDTH + HD * h + HD) for h in range(HEADS)]
    at_v = [slice(2 * WIDTH + HD * h, 2 * WIDTH + HD * h + HD) for h in range(HEADS)]
    every = [(h, b) for h in range(HEADS) for b in range(3)]

    def turned(pre):
        return (pre * cos_all + pltpu.roll(pre, HALF, 1) * sin_all).astype(BF)

    def keys(b):
        return slice(0, 128 * b + 128)

    q = [turned(acc[:, at_q[h]]) for h in range(HEADS)]
    k = [turned(acc[:, at_k[h]]) for h in range(HEADS)]
    v = [acc[:, at_v[h]].astype(BF) for h in range(HEADS)]
    u = [u_all[:, at_q[h]] for h in range(HEADS)]
    scores = {
        (h, b): jnp.where(allowed[b], dot_t(q[h][block_rows[b]], k[h][keys(b)]) * score_scale, -1e30) for h, b in every
    }
    grad_prob = {(h, b): dot_t(u[h][block_rows[b]], v[h][keys(b)]) for h, b in every}
    peak = {at: jnp.max(scores[at], axis=1, keepdims=True) for at in every}
    weights = {at: jnp.exp(scores[at] - peak[at]) for at in every}
    norm = {at: 1.0 / jnp.sum(weights[at], axis=1, keepdims=True) for at in every}
    prob = {at: weights[at] * norm[at] for at in every}
    delta = {at: jnp.sum(prob[at] * grad_prob[at], axis=1, keepdims=True) for at in every}
    grads = {
        at: prob[at][:, :PROMPT_PAD] * (grad_prob[at][:, :PROMPT_PAD] - delta[at]) for at in every
    }
    for h, b in every:
        mixed = dot(prob[h, b].astype(BF), v[h][keys(b)])
        o_full[block_rows[b], at_q[h]] = mixed if b == 0 else jnp.where(live[block_rows[b]], mixed, 0.0)
    grad_t = [jnp.concatenate([grads[h, b].T for b in range(3)], axis=1).astype(BF) for h in range(HEADS)]
    prob_t = [jnp.concatenate([prob[h, b][:, :PROMPT_PAD].T for b in range(3)], axis=1).astype(BF) for h in range(HEADS)]
    grad_q = [dot(grads[h, 0].astype(BF), k[h][:PROMPT_PAD]) * score_scale for h in range(HEADS)]
    grad_k = [dot(grad_t[h], q[h]) * score_scale for h in range(HEADS)]
    grad_v = [dot(prob_t[h], u[h]).astype(BF) for h in range(HEADS)]
    grad_q = [(g * cos_p - pltpu.roll(g, HALF, 1) * sin_p).astype(BF) for g in grad_q]
    grad_k = [(g * cos_p - pltpu.roll(g, HALF, 1) * sin_p).astype(BF) for g in grad_k]
    s_part = jnp.zeros((PROMPT_PAD, HD), F32)
    for h in range(HEADS):
        for at, grad in ((at_q[h], grad_q[h]), (at_k[h], grad_k[h]), (at_v[h], grad_v[h])):
            gcat[:, at] = grad
            s_part = s_part + grad.astype(F32) * acc[0:PROMPT_PAD, at]

    def grad_block(j):
        rows = pl.ds(pl.multiple_of(j * COLS, COLS), COLS)
        return dot_t(gcat[0:PROMPT_SENT], w_all[rows, :])

    def rs_copy(way, step, t):
        return remote(
            rs_tx.at[way, step, t], rs_rx.at[way, step, t], rs_s.at[way, step, t], rs_r.at[way, step, t],
            {"tensor": mod8(z + SIGN[way])},
        )

    def rs_put(way, step, t, value):
        rs_tx[way, step, t] = value.astype(BF)
        rs_copy(way, step, t).start()

    for way in range(2):
        first, count = RS_LAST[way][0], len(RS_LAST[way])
        rows = pl.ds(pl.multiple_of(mod8(z + 4) * COLS + 128 * first, 128), 128 * count)
        part = dot_t(gcat[0:PROMPT_SENT], w_all[rows, :])
        for i in range(count):
            rs_put(way, 0, first + i, part[:, 128 * i : 128 * i + 128])
    blocks = (grad_block(mod8(z + 3)), grad_block(mod8(z - 3)))
    for way in range(2):
        for t in RS_LAST[1 - way]:
            rs_put(way, 1, t, blocks[way][:, 128 * t : 128 * t + 128])
    for way in range(2):
        for t in RS_LAST[way]:
            rs_own[way, t] = blocks[way][:, 128 * t : 128 * t + 128]
    sx_all[z] = lane_sums(s_part, PROMPT_PAD)
    send_small(sx_all, 2)

    for h in range(HEADS):
        lanes = slice(HD * h, HD * h + HD)
        x = o_full[:, lanes]
        outer = jnp.where(row < PROMPT, x, pltpu.roll(x, ROWS_PAD - (PROMPT_PAD - PROMPT), 0))
        outer = outer.astype(BF)
        for g in range(R_HIGH):
            ot_src[h * R_HIGH + g] = outer[R_ROWS * g : R_ROWS * g + R_ROWS]
    scatter_rows(ot_src, ot_mid, OT)

    for t in (0, 1, 2):
        for way in range(2):
            if t < len(RS_LAST[way]):
                tile = RS_LAST[way][t]
                rs_copy(way, 0, tile).wait_recv()
                rs_put(way, 1, tile, rs_own[way, tile] + rs_rx[way, 0, tile].astype(F32))
    for step in (2, 3):
        blocks = (grad_block(mod8(z + 4 - step)), grad_block(mod8(z - 4 + step)))
        for i in range(TILES):
            for way in range(2):
                t = RS_ORDER[way][i]
                rs_copy(way, step - 1, t).wait_recv()
                value = blocks[way][:, 128 * t : 128 * t + 128] + rs_rx[way, step - 1, t].astype(F32)
                rs_put(way, step, t, value)
            if step == 3 and i == 1:

                @pl.when(there_r)
                def _():
                    await_middle(ot_mid, OT)
                    relay(lambda s: ot_mid[inverse_slot[s]], ot_send, ot_dst, OT, mine_r)

    own = grad_block(z)
    await_bytes(sx_all, sm_r.at[2], NZ - 1)
    s_col[...] = jnp.broadcast_to(total_of(sx_all) * (1.0 / (NZ * COLS)), (128, PROMPT_PAD)).T
    inv = inv_p[0:PROMPT_SENT]
    second = inv * inv * s_col[0:PROMPT_SENT]
    ends = []
    for t in range(TILES):
        lanes = slice(128 * t, 128 * t + 128)
        value = own[:, lanes]
        for way in range(2):
            rs_copy(way, 3, t).wait_recv()
            value = value + rs_rx[way, 3, t].astype(F32)
        value = inv * (value * gain[z, :, lanes]) - prm_all[z, 0:PROMPT_SENT, lanes].astype(F32) * second
        low = value.astype(BF)
        for g in range(G_HIGH):
            p = t * G_HIGH + g
            gr_src[p] = low[G_ROWS * g : G_ROWS * g + G_ROWS]
            scatter_one(gr_src, gr_mid, GR, p, p)
        ends.append(value[96:100])
    first, second = tail_rows(ends)
    for p, value in ((30, first), (31, second)):
        gr_src[p] = value.astype(BF)
        scatter_one(gr_src, gr_mid, GR, p, p)
    await_middle(gr_mid, GR)
    before = jnp.zeros((G_ROWS, 128), F32)
    for e in range(ND):
        now = gr_mid[e].astype(F32)
        if e > 0:
            now = now + jnp.where(task_of[e] == task_of[e - 1], before, 0.0)
        gr_run[e] = now
        before = now

    def task_sum(t):
        at = jnp.maximum(last_of[t], 0)
        return jnp.where(task_of[at] == t, gr_run[at], 0.0).astype(BF)

    relay(task_sum, gr_send, gr_dst, GR, d)
    await_rows(ot_dst, a2_r.at[OT, 1])
    await_bytes(gr_dst, a2_r.at[GR, 1], ND - 1)
    await_bytes(spt_all, a2_s.at[SP, 0], ND - 1)
    await_bytes(pp_src, a2_s.at[PP, 0], ND - 1)
    await_bytes(pp_send, a2_s.at[PP, 1], ND - 1)
    await_bytes(gr_src, a2_s.at[GR, 0], ND - 1)
    await_bytes(gr_send, a2_s.at[GR, 1], ND - 1)
    await_rows(ct_src, a2_s.at[CT, 0])
    await_rows(ot_src, a2_s.at[OT, 0])

    @pl.when(there_r)
    def _():
        await_bytes(ct_send, a2_s.at[CT, 1], ND - 1)
        await_bytes(ot_send, a2_s.at[OT, 1], ND - 1)

    for which, ref in enumerate((sst_all, ssp_all, sx_all)):
        await_bytes(ref, sm_s.at[which], NZ - 1)
    for way in range(2):
        for j in range(len(SUBS)):
            for k in range(1, 5):
                if k < 4 or j in LAST[way]:
                    ring_send(way, k, j).wait_send()
        for step in range(4):
            for t in range(TILES):
                if step > 0 or t in RS_LAST[way]:
                    rs_copy(way, step, t).wait_send()


def assemble(ot_ref, gr_ref, out_ref, pg_ref):
    for c in range(HEADS):
        lanes = slice(128 * c, 128 * c + 128)
        for g in range(R_HIGH - 1):
            out_ref[0, R_ROWS * g : R_ROWS * g + R_ROWS, lanes] = ot_ref[c * R_HIGH + g]
        out_ref[0, 320:356, lanes] = ot_ref[c * R_HIGH + 8, 0:36]
    for c in range(TILES):
        lanes = slice(128 * c, 128 * c + 128)
        for g in range(G_HIGH):
            pg_ref[G_ROWS * g : G_ROWS * g + G_ROWS, 0, lanes] = gr_ref[c * G_HIGH + g].astype(F32)
        pg_ref[96:100, 0, lanes] = gr_ref[30 + c // 4].astype(F32)[4 * (c % 4) : 4 * (c % 4) + 4]


def on_device(text, prompts, gain, w_query, w_key, w_value, cotangent, task_of, lengths, slot):
    cosine, sine = rope_constants()
    vmem, dma, smem = pltpu.VMEM, pltpu.SemaphoreType.DMA, pltpu.SMEM
    anywhere = pl.BlockSpec(memory_space=pl.ANY)
    whole = pl.BlockSpec(memory_space=pltpu.VMEM)
    g_piece, r_piece = (G_ROWS, 128), (R_ROWS, 128)
    out_pieces, grad_pieces = pl.pallas_call(
        kernel,
        out_shape=(
            pltpu.VMEM((R_PIECES, *r_piece), BF),
            pltpu.VMEM((ND, *g_piece), BF),
        ),
        in_specs=[anywhere] * 12,
        out_specs=(whole, whole),
        scratch_shapes=[
            *[smem((ND,), jnp.int32)] * 5, vmem((NZ, 1, COLS), F32),
            vmem((NZ, TEXT, COLS), BF), vmem((NZ, PROMPT_PAD, COLS), BF), vmem((PROMPT, COLS), BF),
            vmem((ROWS, WIDTH), BF), vmem((NZ * COLS, ALL), BF),
            vmem((ROWS_PAD, HD), F32), vmem((ROWS_PAD, HD), F32),
            vmem((ROWS_PAD, ALL), F32), vmem((ROWS_PAD, COLS), BF),
            vmem((TEXT, 128), F32), vmem((PROMPT_PAD, 128), F32), vmem((PROMPT_PAD, 128), F32),
            vmem((NZ, 1, TEXT), F32), vmem((NZ, 1, PROMPT_PAD), F32), vmem((ND, 1, PROMPT_PAD), F32),
            vmem((NZ, 1, PROMPT_PAD), F32),
            vmem((ND, *g_piece), BF), vmem((ND, *g_piece), BF), vmem((ND, *g_piece), BF), vmem((ND, *g_piece), BF),
            vmem((R_PIECES, *r_piece), BF), vmem((ND, *r_piece), BF), vmem((ND, *r_piece), BF), vmem((R_PIECES, *r_piece), BF),
            vmem((R_PIECES, *r_piece), BF), vmem((ND, *r_piece), BF), vmem((ND, *r_piece), BF),
            vmem((ND, *g_piece), BF), vmem((ND, *g_piece), BF), vmem((ND, *g_piece), BF), vmem((ND, *g_piece), F32),
            vmem((ROWS_PAD, WIDTH), F32), vmem((ROWS_PAD, WIDTH), BF),
            vmem((ROWS_PAD, WIDTH), F32), vmem((PROMPT_PAD, ALL), BF),
            vmem((2, TILES, PROMPT_SENT, 128), F32),
            vmem((2, 4, TILES, PROMPT_SENT, 128), BF), vmem((2, 4, TILES, PROMPT_SENT, 128), BF),
            dma((12,)), dma((2, 4, len(SUBS))), dma((2, 4, len(SUBS))), dma((2, 4, TILES)), dma((2, 4, TILES)),
            dma((3,)), dma((3,)), dma((5, 2)), dma((5, 2)),
        ],
        compiler_params=pltpu.CompilerParams(
            collective_id=0, has_side_effects=True, vmem_limit_bytes=56 * 1024 * 1024
        ),
    )(
        task_of, lengths, slot, text, prompts, gain.reshape(NZ, 1, COLS), w_query, w_key, w_value, cotangent,
        jnp.asarray(cosine), jnp.asarray(sine),
    )
    attn_out, prompt_grad = pl.pallas_call(
        assemble,
        out_shape=(
            jax.ShapeDtypeStruct((1, ROWS, WIDTH), BF),
            jax.ShapeDtypeStruct((PROMPT, 1, COLS), F32),
        ),
        in_specs=[whole, whole],
        out_specs=(whole, whole),
    )(*(pltpu.with_memory_space_constraint(x, pltpu.VMEM) for x in (out_pieces, grad_pieces)))
    return attn_out, prompt_grad.reshape(1, PROMPT, COLS)


def solution(mesh):
    in_specs = (
        P("dp", None, "tensor"),
        P("dp", None, "tensor"),
        P(),
        P(None, "tensor"),
        P(None, "tensor"),
        P(None, "tensor"),
        P("dp", None, "tensor"),
        P(),
        P(),
        P(),
    )
    out_specs = (P("dp", None, "tensor"), P("dp", None, "tensor"))
    return jax.shard_map(on_device, mesh=mesh, in_specs=in_specs, out_specs=out_specs, check_vma=False)
```

```python
import math

import jax
import jax.numpy as jnp
import numpy as np
from jax import lax
from jax.experimental import pallas as pl
from jax.experimental.pallas import tpu as pltpu
from jax.sharding import PartitionSpec as P

HD = 128
HALF = 64
EPS = 1e-05
MESH = pl.DeviceIdType.MESH
BF = jnp.bfloat16
F32 = jnp.float32

TEXT = 256
PROMPT = 100
PROMPT_PAD = 128
PROMPT_SENT = 104
ROWS = TEXT + PROMPT
ROWS_PAD = TEXT + PROMPT_PAD
COLS = 640
TILES = COLS // 128
HEADS = 3
WIDTH = HEADS * HD
ALL = 3 * WIDTH
NZ = 8
ND = 32
G_ROWS = 16
G_HIGH = 6
R_ROWS = 40
R_HIGH = 9
R_PIECES = HEADS * R_HIGH
TEXT_SUB = 4
SUBS = ((0, 64), (64, 64), (128, 64), (192, 64), (0, 56), (56, 48))
LAST = ((0, 1, 4), (2, 3, 5))
LATE = (1, 3)
TEXT_ORDER = ((0, 2), (1, 3), (2, 0), (3, 1))
PROMPT_ORDER = ((4, 5), (5, 4))
RS_LAST = ((0, 1, 2), (3, 4))
RS_ORDER = ((3, 4, 0, 1, 2), (0, 1, 2, 3, 4))
FINAL_ORDER = (0, 1, 3, 4, 2)


def rope_constants():
    frequency = (np.float32(10000.0) ** (-np.arange(HALF, dtype=np.float32) / np.float32(HALF))).astype(np.float32)
    position = np.concatenate([np.arange(PROMPT_PAD), np.arange(TEXT) + PROMPT]).astype(np.float32)
    angle = (position[:, None] * frequency[None, :]).astype(np.float32)
    cosine = np.cos(angle.astype(np.float64)).astype(np.float32)
    sine = np.sin(angle.astype(np.float64)).astype(np.float32)
    return np.concatenate([cosine, cosine], axis=1), np.concatenate([-sine, sine], axis=1)


def dot(a, b):
    return lax.dot_general(a, b, (((1,), (0,)), ((), ())), preferred_element_type=F32)


def dot_t(a, b):
    return lax.dot_general(a, b, (((1,), (1,)), ((), ())), preferred_element_type=F32)


def tail_rows(tiles):
    last = jnp.concatenate(tiles + [jnp.zeros((12, 128), F32)], axis=0)
    return last[0:16], last[16:32]


def kernel(
    task_hbm, lengths_hbm, slot_hbm, text_hbm, prompts_hbm, gain_hbm, wq_hbm, wk_hbm, wv_hbm, cot_hbm, cos_hbm, sin_hbm,
    ot_dst, gr_dst,
    task_of, lengths, slot, inverse_slot, last_of, gain,
    text_all, prm_all, pr_loc, ct_loc, w_all, cos_t, sin_t, acc, nb, inv_t, inv_p, s_col,
    sst_all, ssp_all, spt_all, sx_all,
    pp_src, pp_mid, pp_send, pp_dst,
    ct_src, ct_mid, ct_send, ct_dst,
    ot_src, ot_mid, ot_send,
    gr_src, gr_mid, gr_send, gr_run,
    u_ext, u_all, o_full, gcat, rs_own, rs_tx, rs_rx,
    local_sem, ag_s, ag_r, rs_s, rs_r, sm_s, sm_r, a2_s, a2_r,
):
    d = lax.axis_index("dp")
    z = lax.axis_index("tensor")

    def mod8(v):
        return lax.rem(v + 16, NZ)

    loads = [
        pltpu.make_async_copy(prompts_hbm.at[0], pr_loc, local_sem.at[0]),
        pltpu.make_async_copy(text_hbm.at[0], text_all.at[z], local_sem.at[1]),
        pltpu.make_async_copy(cot_hbm.at[0], ct_loc, local_sem.at[2]),
        pltpu.make_async_copy(wq_hbm, w_all.at[:, pl.ds(0, WIDTH)], local_sem.at[3]),
        pltpu.make_async_copy(wk_hbm, w_all.at[:, pl.ds(WIDTH, WIDTH)], local_sem.at[4]),
        pltpu.make_async_copy(wv_hbm, w_all.at[:, pl.ds(2 * WIDTH, WIDTH)], local_sem.at[5]),
        pltpu.make_async_copy(cos_hbm, cos_t, local_sem.at[6]),
        pltpu.make_async_copy(sin_hbm, sin_t, local_sem.at[7]),
        pltpu.make_async_copy(gain_hbm, gain, local_sem.at[8]),
        pltpu.make_async_copy(task_hbm, task_of, local_sem.at[9]),
        pltpu.make_async_copy(lengths_hbm, lengths, local_sem.at[10]),
        pltpu.make_async_copy(slot_hbm, slot, local_sem.at[11]),
    ]
    barrier = pltpu.get_barrier_semaphore()

    def greet_dp(i, carry):
        pl.semaphore_signal(barrier, inc=1, device_id={"dp": lax.rem(d + i, ND)}, device_id_type=MESH)
        return carry

    def greet_z(i, carry):
        pl.semaphore_signal(barrier, inc=1, device_id={"tensor": lax.rem(z + i, NZ)}, device_id_type=MESH)
        return carry

    lax.fori_loop(1, NZ, greet_z, 0)
    lax.fori_loop(1, ND, greet_dp, 0)
    for load in loads:
        load.start()

    def remote(src, dst, s_sem, r_sem, where):
        return pltpu.make_async_remote_copy(
            src_ref=src, dst_ref=dst, send_sem=s_sem, recv_sem=r_sem, device_id=where, device_id_type=MESH
        )

    mine_r = lax.div(d * R_PIECES + ND - 1, ND)
    there_r = jnp.logical_and(mine_r < R_PIECES, lax.div(mine_r * ND, R_PIECES) == d)
    PP, CT, OT, GR, SP = range(5)

    def scatter_grad(p):
        @pl.when(d != p)
        def _():
            remote(gr_src.at[p], gr_mid.at[d], a2_s.at[GR, 0], a2_r.at[GR, 0], {"dp": p}).start()

    def scatter_rows(src, mid, which):
        first = jnp.minimum(mine_r, R_PIECES - 1)

        def send_piece(p):
            m = lax.div(p * ND, R_PIECES)
            remote(src.at[p], mid.at[d], a2_s.at[which, 0], a2_r.at[which, 0], {"dp": m}).start()

        def body(i, carry):
            send_piece(lax.rem(first + i, R_PIECES))
            return carry

        lax.fori_loop(1, R_PIECES, body, 0)

        @pl.when(there_r)
        def _():
            mid[d] = src[first]

        @pl.when(jnp.logical_not(there_r))
        def _():
            send_piece(first)

    def scatter_all(src, mid, which):
        def body(i, carry):
            m = lax.rem(d + i, ND)
            remote(src.at[m], mid.at[d], a2_s.at[which, 0], a2_r.at[which, 0], {"dp": m}).start()
            return carry

        lax.fori_loop(1, ND, body, 0)
        mid[d] = src[d]

    def await_bytes(ref, sem, count):
        part = ref.at[pl.ds(0, count)]
        pltpu.make_async_copy(part, part, sem).wait()

    def await_middle(mid, which):
        await_bytes(mid, a2_r.at[which, 0], ND - 1)

    def relay(value, send, dst, which, mine):
        def body(i, carry):
            e = lax.rem(d + i, ND)
            send[e] = value(e)
            remote(send.at[e], dst.at[mine], a2_s.at[which, 1], a2_r.at[which, 1], {"dp": e}).start()
            return carry

        lax.fori_loop(1, ND, body, 0)
        dst[mine] = value(d)

    def await_rows(ref, sem):
        @pl.when(there_r)
        def _():
            await_bytes(ref, sem, R_PIECES - 1)

        @pl.when(jnp.logical_not(there_r))
        def _():
            await_bytes(ref, sem, R_PIECES)

    def send_small(ref, which):
        def body(i, carry):
            remote(ref.at[z], ref.at[z], sm_s.at[which], sm_r.at[which], {"tensor": lax.rem(z + i, NZ)}).start()
            return carry

        lax.fori_loop(1, NZ, body, 0)

    def await_small(ref, sem):
        part = ref.at[pl.ds(0, NZ - 1)]
        pltpu.make_async_copy(part, part, sem).wait()

    SIGN = (1, -1)

    def ring_rows(c, j):
        first, count = SUBS[j]
        return (text_all if j < TEXT_SUB else prm_all).at[c, pl.ds(first, count), :]

    def ring_send(way, k, j):
        rows = ring_rows(mod8(z - SIGN[way] * (k - 1)), j)
        return remote(rows, rows, ag_s.at[way, k - 1, j], ag_r.at[way, k - 1, j], {"tensor": mod8(z + SIGN[way])})

    def ring_recv(way, k, j):
        rows = ring_rows(mod8(z - SIGN[way] * k), j)
        return remote(rows, rows, ag_s.at[way, k - 1, j], ag_r.at[way, k - 1, j], {"tensor": mod8(z + SIGN[way])})

    def ring_step(k, pairs):
        for pair in pairs:
            for way, j in enumerate(pair):
                if k < 4 or j in LAST[way]:
                    ring_recv(way, k, j).wait_recv()
                    if k < 3 or (k == 3 and j in LAST[way] and j not in LATE):
                        ring_send(way, k + 1, j).start()

    def ring_begin(pairs):
        for pair in pairs:
            for way, j in enumerate(pair):
                ring_send(way, 1, j).start()

    def lane_sums(squares, rows):
        return jnp.broadcast_to(jnp.sum(squares, axis=1, keepdims=True), (rows, 128)).T[0:1]

    def total_of(ref):
        total = ref[0]
        for i in range(1, NZ):
            total = total + ref[i]
        return total

    def inverse(squares, rows):
        inv = lax.rsqrt(squares * (1.0 / (NZ * COLS)) + EPS)
        return jnp.broadcast_to(inv, (128, rows)).T

    def normed_text(c):
        for t in range(TILES):
            lanes = slice(128 * t, 128 * t + 128)
            nb[PROMPT_PAD:, lanes] = (text_all[c, :, lanes].astype(F32) * inv_t[...] * gain[c, :, lanes]).astype(BF)

    def normed_prompts(c):
        for t in range(TILES):
            lanes = slice(128 * t, 128 * t + 128)
            nb[0:PROMPT_PAD, lanes] = (prm_all[c, :, lanes].astype(F32) * inv_p[...] * gain[c, :, lanes]).astype(BF)

    def multiply(c, which=slice(0, ROWS_PAD)):
        rows = pl.ds(pl.multiple_of(c * COLS, COLS), COLS)
        for n in range(3):
            wide = slice(WIDTH * n, WIDTH * n + WIDTH)
            acc[which, wide] += dot(nb[which], w_all[rows, wide])

    def project(c):
        normed_text(c)
        normed_prompts(c)
        multiply(c)

    def project_each(k, count):
        def body(i, carry):
            project(mod8(z + k * (i - 1) if count == 3 else z + k * (2 * i - 1)))
            return carry

        lax.fori_loop(0, count, body, 0)

    loads[0].wait()
    for c in range(TILES):
        for g in range(G_HIGH):
            pp_src[c * G_HIGH + g] = pr_loc[G_ROWS * g : G_ROWS * g + G_ROWS, 128 * c : 128 * c + 128]
    first, second = tail_rows([pr_loc[96:100, 128 * c : 128 * c + 128].astype(F32) for c in range(TILES)])
    pp_src[30] = first.astype(BF)
    pp_src[31] = second.astype(BF)
    total = jnp.zeros((PROMPT, 128), F32)
    for c in range(TILES):
        x = pr_loc[:, 128 * c : 128 * c + 128].astype(F32)
        total = total + x * x
    total = jnp.concatenate([total, jnp.zeros((PROMPT_PAD - PROMPT, 128), F32)], axis=0)
    ssp_all[z] = lane_sums(total, PROMPT_PAD)
    loads[1].wait()
    total = jnp.zeros((TEXT, 128), F32)
    for c in range(TILES):
        x = text_all[z, :, 128 * c : 128 * c + 128].astype(F32)
        total = total + x * x
    sst_all[z] = lane_sums(total, TEXT)
    pl.semaphore_wait(barrier, ND - 1 + NZ - 1)
    send_small(ssp_all, 1)
    send_small(sst_all, 0)
    ring_begin(TEXT_ORDER)
    scatter_all(pp_src, pp_mid, PP)
    loads[2].wait()
    for c in range(HEADS):
        lanes = slice(128 * c, 128 * c + 128)
        for g in range(R_HIGH - 1):
            ct_src[c * R_HIGH + g] = ct_loc[R_ROWS * g : R_ROWS * g + R_ROWS, lanes]
        ct_src[c * R_HIGH + 8] = jnp.zeros((R_ROWS, 128), BF)
        ct_src[c * R_HIGH + 8, 0:36] = ct_loc[320:356, lanes]
    prm_all[:, PROMPT_SENT:, :] = jnp.zeros((NZ, PROMPT_PAD - PROMPT_SENT, COLS), BF)
    acc[...] = jnp.zeros_like(acc)
    for load in loads[9:]:
        load.wait()
    def look_up(s, carry):
        found, upto = jnp.int32(0), jnp.int32(0)
        for e in range(ND):
            found = jnp.where(slot[e] == s, e, found)
            upto = upto + jnp.where(task_of[e] <= s, 1, 0)
        inverse_slot[s] = found
        last_of[s] = upto - 1
        return carry

    lax.fori_loop(0, ND, look_up, 0)
    await_bytes(ssp_all, sm_r.at[1], NZ - 1)
    spt_all[d] = total_of(ssp_all)

    def tell_dp(i, carry):
        m = lax.rem(d + i, ND)
        remote(spt_all.at[d], spt_all.at[d], a2_s.at[SP, 0], a2_r.at[SP, 0], {"dp": m}).start()
        return carry

    lax.fori_loop(1, ND, tell_dp, 0)
    ring_step(1, TEXT_ORDER[:1])
    await_middle(pp_mid, PP)
    relay(lambda e: pp_mid[task_of[e]], pp_send, pp_dst, PP, d)
    ring_step(1, TEXT_ORDER[1:3])
    await_bytes(sst_all, sm_r.at[0], NZ - 1)
    inv_t[...] = inverse(total_of(sst_all), TEXT)
    ring_step(1, TEXT_ORDER[3:])
    await_bytes(pp_dst, a2_r.at[PP, 1], ND - 1)
    for c in range(TILES):
        lanes = slice(128 * c, 128 * c + 128)
        for g in range(G_HIGH):
            prm_all[z, G_ROWS * g : G_ROWS * g + G_ROWS, lanes] = pp_dst[c * G_HIGH + g]
        end = pp_dst[30 + c // 4].astype(F32)[4 * (c % 4) : 4 * (c % 4) + 4]
        prm_all[z, 96:104, lanes] = jnp.concatenate([end, jnp.zeros((4, 128), F32)], axis=0).astype(BF)
    ring_begin(PROMPT_ORDER)
    scatter_rows(ct_src, ct_mid, CT)
    ring_step(2, TEXT_ORDER)
    await_bytes(spt_all, a2_r.at[SP, 0], ND - 1)
    inv_p[...] = inverse(spt_all[task_of[d]], PROMPT_PAD)
    ring_step(1, PROMPT_ORDER)
    for load in loads[3:6] + loads[8:9]:
        load.wait()
    project_each(1, 3)
    ring_step(3, TEXT_ORDER)
    @pl.when(there_r)
    def _():
        await_middle(ct_mid, CT)
        relay(lambda e: ct_mid[slot[e]], ct_send, ct_dst, CT, mine_r)

    ring_step(2, PROMPT_ORDER)
    for way in range(2):
        ring_send(way, 4, LATE[way]).start()
    project_each(2, 2)
    ring_step(3, PROMPT_ORDER)
    project_each(3, 2)
    length = lengths[d]
    await_rows(ct_dst, a2_r.at[CT, 1])
    for c in range(HEADS):
        for g in range(R_HIGH):
            u_ext[R_ROWS * g : R_ROWS * g + R_ROWS, 128 * c : 128 * c + 128] = ct_dst[c * R_HIGH + g].astype(F32)
    u_ext[R_ROWS * R_HIGH :] = jnp.zeros((ROWS_PAD - R_ROWS * R_HIGH, WIDTH), F32)
    row = lax.broadcasted_iota(jnp.int32, (ROWS_PAD, HD), 0)
    live = (row < PROMPT) | ((row >= PROMPT_PAD) & (row < length + PROMPT_PAD))
    for h in range(HEADS):
        lanes = slice(HD * h, HD * h + HD)
        x = u_ext[:, lanes]
        x = jnp.where(row < PROMPT_PAD, x, pltpu.roll(x, PROMPT_PAD - PROMPT, 0))
        u_all[:, lanes] = jnp.where(live, x, 0.0).astype(BF)
    loads[6].wait()
    loads[7].wait()

    ring_step(4, TEXT_ORDER)
    normed_text(mod8(z + 4))
    multiply(mod8(z + 4), slice(PROMPT_PAD, ROWS_PAD))
    ring_step(4, PROMPT_ORDER)
    normed_prompts(mod8(z + 4))
    multiply(mod8(z + 4), slice(0, PROMPT_PAD))

    score_scale = 1.0 / math.sqrt(HD)
    cos_all, sin_all = cos_t[...], sin_t[...]
    cos_p, sin_p = cos_all[:PROMPT_PAD], sin_all[:PROMPT_PAD]
    block_rows = [slice(128 * b, 128 * b + 128) for b in range(3)]
    allowed = []
    for b in range(3):
        shape = (128, 128 * b + 128)
        r = lax.broadcasted_iota(jnp.int32, shape, 0) + 128 * b
        c = lax.broadcasted_iota(jnp.int32, shape, 1)
        allowed.append((c <= r) & ((c < PROMPT) | ((c >= PROMPT_PAD) & (c < length + PROMPT_PAD))))
    at_q = [slice(HD * h, HD * h + HD) for h in range(HEADS)]
    at_k = [slice(WIDTH + HD * h, WIDTH + HD * h + HD) for h in range(HEADS)]
    at_v = [slice(2 * WIDTH + HD * h, 2 * WIDTH + HD * h + HD) for h in range(HEADS)]
    every = [(h, b) for h in range(HEADS) for b in range(3)]

    def turned(pre):
        return (pre * cos_all + pltpu.roll(pre, HALF, 1) * sin_all).astype(BF)

    def keys(b):
        return slice(0, 128 * b + 128)

    q = [turned(acc[:, at_q[h]]) for h in range(HEADS)]
    k = [turned(acc[:, at_k[h]]) for h in range(HEADS)]
    v = [acc[:, at_v[h]].astype(BF) for h in range(HEADS)]
    u = [u_all[:, at_q[h]] for h in range(HEADS)]
    scores = {
        (h, b): jnp.where(allowed[b], dot_t(q[h][block_rows[b]], k[h][keys(b)]) * score_scale, -1e30) for h, b in every
    }
    grad_prob = {(h, b): dot_t(u[h][block_rows[b]], v[h][keys(b)]) for h, b in every}
    peak = {at: jnp.max(scores[at], axis=1, keepdims=True) for at in every}
    weights = {at: jnp.exp(scores[at] - peak[at]) for at in every}
    norm = {at: 1.0 / jnp.sum(weights[at], axis=1, keepdims=True) for at in every}
    prob = {at: weights[at] * norm[at] for at in every}
    delta = {at: jnp.sum(prob[at] * grad_prob[at], axis=1, keepdims=True) for at in every}
    grads = {
        at: prob[at][:, :PROMPT_PAD] * (grad_prob[at][:, :PROMPT_PAD] - delta[at]) for at in every
    }
    for h, b in every:
        mixed = dot(prob[h, b].astype(BF), v[h][keys(b)])
        o_full[block_rows[b], at_q[h]] = mixed if b == 0 else jnp.where(live[block_rows[b]], mixed, 0.0)
    grad_t = [jnp.concatenate([grads[h, b].T for b in range(3)], axis=1).astype(BF) for h in range(HEADS)]
    prob_t = [jnp.concatenate([prob[h, b][:, :PROMPT_PAD].T for b in range(3)], axis=1).astype(BF) for h in range(HEADS)]
    grad_q = [dot(grads[h, 0].astype(BF), k[h][:PROMPT_PAD]) * score_scale for h in range(HEADS)]
    grad_k = [dot(grad_t[h], q[h]) * score_scale for h in range(HEADS)]
    grad_v = [dot(prob_t[h], u[h]).astype(BF) for h in range(HEADS)]
    grad_q = [(g * cos_p - pltpu.roll(g, HALF, 1) * sin_p).astype(BF) for g in grad_q]
    grad_k = [(g * cos_p - pltpu.roll(g, HALF, 1) * sin_p).astype(BF) for g in grad_k]
    s_part = jnp.zeros((PROMPT_PAD, HD), F32)
    for h in range(HEADS):
        for at, grad in ((at_q[h], grad_q[h]), (at_k[h], grad_k[h]), (at_v[h], grad_v[h])):
            gcat[:, at] = grad
            s_part = s_part + grad.astype(F32) * acc[0:PROMPT_PAD, at]

    def grad_block(j):
        rows = pl.ds(pl.multiple_of(j * COLS, COLS), COLS)
        return dot_t(gcat[0:PROMPT_SENT], w_all[rows, :])

    def rs_copy(way, step, t):
        return remote(
            rs_tx.at[way, step, t], rs_rx.at[way, step, t], rs_s.at[way, step, t], rs_r.at[way, step, t],
            {"tensor": mod8(z + SIGN[way])},
        )

    def rs_put(way, step, t, value):
        rs_tx[way, step, t] = value.astype(BF)
        rs_copy(way, step, t).start()

    for way in range(2):
        first, count = RS_LAST[way][0], len(RS_LAST[way])
        rows = pl.ds(pl.multiple_of(mod8(z + 4) * COLS + 128 * first, 128), 128 * count)
        part = dot_t(gcat[0:PROMPT_SENT], w_all[rows, :])
        for i in range(count):
            rs_put(way, 0, first + i, part[:, 128 * i : 128 * i + 128])
    blocks = (grad_block(mod8(z + 3)), grad_block(mod8(z - 3)))
    for way in range(2):
        for t in RS_LAST[1 - way]:
            rs_put(way, 1, t, blocks[way][:, 128 * t : 128 * t + 128])
    for way in range(2):
        for t in RS_LAST[way]:
            rs_own[way, t] = blocks[way][:, 128 * t : 128 * t + 128]
    sx_all[z] = lane_sums(s_part, PROMPT_PAD)
    send_small(sx_all, 2)

    blocks = (grad_block(mod8(z + 2)), grad_block(mod8(z - 2)))
    for t in (0, 1, 2):
        for way in range(2):
            if t < len(RS_LAST[way]):
                tile = RS_LAST[way][t]
                rs_copy(way, 0, tile).wait_recv()
                rs_put(way, 1, tile, rs_own[way, tile] + rs_rx[way, 0, tile].astype(F32))
    for h in range(HEADS):
        lanes = slice(HD * h, HD * h + HD)
        x = o_full[:, lanes]
        outer = jnp.where(row < PROMPT, x, pltpu.roll(x, ROWS_PAD - (PROMPT_PAD - PROMPT), 0))
        outer = outer.astype(BF)
        for g in range(R_HIGH):
            ot_src[h * R_HIGH + g] = outer[R_ROWS * g : R_ROWS * g + R_ROWS]
    scatter_rows(ot_src, ot_mid, OT)

    for step in (2, 3):
        if step == 3:
            blocks = (grad_block(mod8(z + 1)), grad_block(mod8(z - 1)))
        for i in range(TILES):
            for way in range(2):
                t = RS_ORDER[way][i]
                rs_copy(way, step - 1, t).wait_recv()
                value = blocks[way][:, 128 * t : 128 * t + 128] + rs_rx[way, step - 1, t].astype(F32)
                rs_put(way, step, t, value)
    @pl.when(there_r)
    def _():
        await_middle(ot_mid, OT)
        relay(lambda s: ot_mid[inverse_slot[s]], ot_send, ot_dst, OT, mine_r)

    own = grad_block(z)
    await_bytes(sx_all, sm_r.at[2], NZ - 1)
    s_col[...] = jnp.broadcast_to(total_of(sx_all) * (1.0 / (NZ * COLS)), (128, PROMPT_PAD)).T
    inv = inv_p[0:PROMPT_SENT]
    second = inv * inv * s_col[0:PROMPT_SENT]
    ends = [None] * TILES
    for t in FINAL_ORDER:
        lanes = slice(128 * t, 128 * t + 128)
        value = own[:, lanes]
        for way in range(2):
            rs_copy(way, 3, t).wait_recv()
            value = value + rs_rx[way, 3, t].astype(F32)
        value = inv * (value * gain[z, :, lanes]) - prm_all[z, 0:PROMPT_SENT, lanes].astype(F32) * second
        low = value.astype(BF)
        for g in range(G_HIGH):
            p = t * G_HIGH + g
            gr_src[p] = low[G_ROWS * g : G_ROWS * g + G_ROWS]
            scatter_grad(p)
        ends[t] = value[96:100]
    first, second = tail_rows(ends)
    for p, value in ((30, first), (31, second)):
        gr_src[p] = value.astype(BF)
        scatter_grad(p)
    gr_mid[d] = gr_src[d]
    await_middle(gr_mid, GR)
    before = jnp.zeros((G_ROWS, 128), F32)
    for e in range(ND):
        now = gr_mid[e].astype(F32)
        if e > 0:
            now = now + jnp.where(task_of[e] == task_of[e - 1], before, 0.0)
        gr_run[e] = now
        before = now

    def task_sum(t):
        at = jnp.maximum(last_of[t], 0)
        return jnp.where(task_of[at] == t, gr_run[at], 0.0).astype(BF)

    relay(task_sum, gr_send, gr_dst, GR, d)
    await_rows(ot_dst, a2_r.at[OT, 1])
    await_bytes(gr_dst, a2_r.at[GR, 1], ND - 1)
    await_bytes(spt_all, a2_s.at[SP, 0], ND - 1)
    await_bytes(pp_src, a2_s.at[PP, 0], ND - 1)
    await_bytes(pp_send, a2_s.at[PP, 1], ND - 1)
    await_bytes(gr_src, a2_s.at[GR, 0], ND - 1)
    await_bytes(gr_send, a2_s.at[GR, 1], ND - 1)
    await_rows(ct_src, a2_s.at[CT, 0])
    await_rows(ot_src, a2_s.at[OT, 0])

    @pl.when(there_r)
    def _():
        await_bytes(ct_send, a2_s.at[CT, 1], ND - 1)
        await_bytes(ot_send, a2_s.at[OT, 1], ND - 1)

    for which, ref in enumerate((sst_all, ssp_all, sx_all)):
        await_bytes(ref, sm_s.at[which], NZ - 1)
    for way in range(2):
        for j in range(len(SUBS)):
            for k in range(1, 5):
                if k < 4 or j in LAST[way]:
                    ring_send(way, k, j).wait_send()
        for step in range(4):
            for t in range(TILES):
                if step > 0 or t in RS_LAST[way]:
                    rs_copy(way, step, t).wait_send()


def assemble(ot_ref, gr_ref, out_ref, pg_ref):
    for c in range(HEADS):
        lanes = slice(128 * c, 128 * c + 128)
        for g in range(R_HIGH - 1):
            out_ref[0, R_ROWS * g : R_ROWS * g + R_ROWS, lanes] = ot_ref[c * R_HIGH + g]
        out_ref[0, 320:356, lanes] = ot_ref[c * R_HIGH + 8, 0:36]
    for c in range(TILES):
        lanes = slice(128 * c, 128 * c + 128)
        for g in range(G_HIGH):
            pg_ref[G_ROWS * g : G_ROWS * g + G_ROWS, 0, lanes] = gr_ref[c * G_HIGH + g].astype(F32)
        pg_ref[96:100, 0, lanes] = gr_ref[30 + c // 4].astype(F32)[4 * (c % 4) : 4 * (c % 4) + 4]


def on_device(text, prompts, gain, w_query, w_key, w_value, cotangent, task_of, lengths, slot):
    cosine, sine = rope_constants()
    vmem, dma, smem = pltpu.VMEM, pltpu.SemaphoreType.DMA, pltpu.SMEM
    anywhere = pl.BlockSpec(memory_space=pl.ANY)
    whole = pl.BlockSpec(memory_space=pltpu.VMEM)
    g_piece, r_piece = (G_ROWS, 128), (R_ROWS, 128)
    out_pieces, grad_pieces = pl.pallas_call(
        kernel,
        out_shape=(
            pltpu.VMEM((R_PIECES, *r_piece), BF),
            pltpu.VMEM((ND, *g_piece), BF),
        ),
        in_specs=[anywhere] * 12,
        out_specs=(whole, whole),
        scratch_shapes=[
            *[smem((ND,), jnp.int32)] * 5, vmem((NZ, 1, COLS), F32),
            vmem((NZ, TEXT, COLS), BF), vmem((NZ, PROMPT_PAD, COLS), BF), vmem((PROMPT, COLS), BF),
            vmem((ROWS, WIDTH), BF), vmem((NZ * COLS, ALL), BF),
            vmem((ROWS_PAD, HD), F32), vmem((ROWS_PAD, HD), F32),
            vmem((ROWS_PAD, ALL), F32), vmem((ROWS_PAD, COLS), BF),
            vmem((TEXT, 128), F32), vmem((PROMPT_PAD, 128), F32), vmem((PROMPT_PAD, 128), F32),
            vmem((NZ, 1, TEXT), F32), vmem((NZ, 1, PROMPT_PAD), F32), vmem((ND, 1, PROMPT_PAD), F32),
            vmem((NZ, 1, PROMPT_PAD), F32),
            vmem((ND, *g_piece), BF), vmem((ND, *g_piece), BF), vmem((ND, *g_piece), BF), vmem((ND, *g_piece), BF),
            vmem((R_PIECES, *r_piece), BF), vmem((ND, *r_piece), BF), vmem((ND, *r_piece), BF), vmem((R_PIECES, *r_piece), BF),
            vmem((R_PIECES, *r_piece), BF), vmem((ND, *r_piece), BF), vmem((ND, *r_piece), BF),
            vmem((ND, *g_piece), BF), vmem((ND, *g_piece), BF), vmem((ND, *g_piece), BF), vmem((ND, *g_piece), F32),
            vmem((ROWS_PAD, WIDTH), F32), vmem((ROWS_PAD, WIDTH), BF),
            vmem((ROWS_PAD, WIDTH), F32), vmem((PROMPT_PAD, ALL), BF),
            vmem((2, TILES, PROMPT_SENT, 128), F32),
            vmem((2, 4, TILES, PROMPT_SENT, 128), BF), vmem((2, 4, TILES, PROMPT_SENT, 128), BF),
            dma((12,)), dma((2, 4, len(SUBS))), dma((2, 4, len(SUBS))), dma((2, 4, TILES)), dma((2, 4, TILES)),
            dma((3,)), dma((3,)), dma((5, 2)), dma((5, 2)),
        ],
        compiler_params=pltpu.CompilerParams(
            collective_id=0, has_side_effects=True, vmem_limit_bytes=56 * 1024 * 1024
        ),
    )(
        task_of, lengths, slot, text, prompts, gain.reshape(NZ, 1, COLS), w_query, w_key, w_value, cotangent,
        jnp.asarray(cosine), jnp.asarray(sine),
    )
    attn_out, prompt_grad = pl.pallas_call(
        assemble,
        out_shape=(
            jax.ShapeDtypeStruct((1, ROWS, WIDTH), BF),
            jax.ShapeDtypeStruct((PROMPT, 1, COLS), F32),
        ),
        in_specs=[whole, whole],
        out_specs=(whole, whole),
    )(*(pltpu.with_memory_space_constraint(x, pltpu.VMEM) for x in (out_pieces, grad_pieces)))
    return attn_out, prompt_grad.reshape(1, PROMPT, COLS)


def solution(mesh):
    in_specs = (
        P("dp", None, "tensor"),
        P("dp", None, "tensor"),
        P(),
        P(None, "tensor"),
        P(None, "tensor"),
        P(None, "tensor"),
        P("dp", None, "tensor"),
        P(),
        P(),
        P(),
    )
    out_specs = (P("dp", None, "tensor"), P("dp", None, "tensor"))
    return jax.shard_map(on_device, mesh=mesh, in_specs=in_specs, out_specs=out_specs, check_vma=False)
```

```python
import math

import jax
import jax.numpy as jnp
import numpy as np
from jax import lax
from jax.experimental import pallas as pl
from jax.experimental.pallas import tpu as pltpu
from jax.sharding import PartitionSpec as P

HD = 128
HALF = 64
EPS = 1e-05
MESH = pl.DeviceIdType.MESH
BF = jnp.bfloat16
F32 = jnp.float32

TEXT = 256
PROMPT = 100
PROMPT_PAD = 128
PROMPT_SENT = 104
ROWS = TEXT + PROMPT
ROWS_PAD = TEXT + PROMPT_PAD
COLS = 640
TILES = COLS // 128
HEADS = 3
WIDTH = HEADS * HD
ALL = 3 * WIDTH
NZ = 8
ND = 32
G_ROWS = 16
G_HIGH = 6
R_ROWS = 40
R_HIGH = 9
R_PIECES = HEADS * R_HIGH
TEXT_SUB = 4
SUBS = ((0, 64), (64, 64), (128, 64), (192, 64), (0, 56), (56, 48))
LAST = ((0, 1, 4), (2, 3, 5))
LATE = (1, 3)
TEXT_ORDER = ((0, 2), (1, 3), (2, 0), (3, 1))
PROMPT_ORDER = ((4, 5), (5, 4))
RS_LAST = ((0, 1, 2), (3, 4))
RS_ORDER = ((3, 4, 0, 1, 2), (0, 1, 2, 3, 4))
HALVES = ((0, 48), (48, 104))
FINAL_ORDER = (0, 1, 3, 4, 2)


def rope_constants():
    frequency = (np.float32(10000.0) ** (-np.arange(HALF, dtype=np.float32) / np.float32(HALF))).astype(np.float32)
    position = np.concatenate([np.arange(PROMPT_PAD), np.arange(TEXT) + PROMPT]).astype(np.float32)
    angle = (position[:, None] * frequency[None, :]).astype(np.float32)
    cosine = np.cos(angle.astype(np.float64)).astype(np.float32)
    sine = np.sin(angle.astype(np.float64)).astype(np.float32)
    return np.concatenate([cosine, cosine], axis=1), np.concatenate([-sine, sine], axis=1)


def dot(a, b):
    return lax.dot_general(a, b, (((1,), (0,)), ((), ())), preferred_element_type=F32)


def dot_t(a, b):
    return lax.dot_general(a, b, (((1,), (1,)), ((), ())), preferred_element_type=F32)


def tail_rows(tiles):
    last = jnp.concatenate(tiles + [jnp.zeros((12, 128), F32)], axis=0)
    return last[0:16], last[16:32]


def kernel(
    task_hbm, lengths_hbm, slot_hbm, text_hbm, prompts_hbm, gain_hbm, wq_hbm, wk_hbm, wv_hbm, cot_hbm, cos_hbm, sin_hbm,
    ot_dst, gr_dst,
    task_of, lengths, slot, inverse_slot, last_of, gain,
    text_all, prm_all, pr_loc, ct_loc, w_all, cos_t, sin_t, acc, nb, inv_t, inv_p, s_col,
    sst_all, ssp_all, spt_all, sx_all,
    pp_src, pp_mid, pp_send, pp_dst,
    ct_src, ct_mid, ct_send, ct_dst,
    ot_src, ot_mid, ot_send,
    gr_src, gr_mid, gr_send, gr_run,
    u_ext, u_all, o_full, gcat, rs_own, rs_tx, rs_rx,
    local_sem, ag_s, ag_r, rs_s, rs_r, sm_s, sm_r, a2_s, a2_r,
):
    d = lax.axis_index("dp")
    z = lax.axis_index("tensor")

    def mod8(v):
        return lax.rem(v + 16, NZ)

    loads = [
        pltpu.make_async_copy(prompts_hbm.at[0], pr_loc, local_sem.at[0]),
        pltpu.make_async_copy(text_hbm.at[0], text_all.at[z], local_sem.at[1]),
        pltpu.make_async_copy(cot_hbm.at[0], ct_loc, local_sem.at[2]),
        pltpu.make_async_copy(wq_hbm, w_all.at[:, pl.ds(0, WIDTH)], local_sem.at[3]),
        pltpu.make_async_copy(wk_hbm, w_all.at[:, pl.ds(WIDTH, WIDTH)], local_sem.at[4]),
        pltpu.make_async_copy(wv_hbm, w_all.at[:, pl.ds(2 * WIDTH, WIDTH)], local_sem.at[5]),
        pltpu.make_async_copy(cos_hbm, cos_t, local_sem.at[6]),
        pltpu.make_async_copy(sin_hbm, sin_t, local_sem.at[7]),
        pltpu.make_async_copy(gain_hbm, gain, local_sem.at[8]),
        pltpu.make_async_copy(task_hbm, task_of, local_sem.at[9]),
        pltpu.make_async_copy(lengths_hbm, lengths, local_sem.at[10]),
        pltpu.make_async_copy(slot_hbm, slot, local_sem.at[11]),
    ]
    barrier = pltpu.get_barrier_semaphore()

    def greet_dp(i, carry):
        pl.semaphore_signal(barrier, inc=1, device_id={"dp": lax.rem(d + i, ND)}, device_id_type=MESH)
        return carry

    def greet_z(i, carry):
        pl.semaphore_signal(barrier, inc=1, device_id={"tensor": lax.rem(z + i, NZ)}, device_id_type=MESH)
        return carry

    lax.fori_loop(1, NZ, greet_z, 0)
    lax.fori_loop(1, ND, greet_dp, 0)
    for load in loads:
        load.start()

    def remote(src, dst, s_sem, r_sem, where):
        return pltpu.make_async_remote_copy(
            src_ref=src, dst_ref=dst, send_sem=s_sem, recv_sem=r_sem, device_id=where, device_id_type=MESH
        )

    mine_r = lax.div(d * R_PIECES + ND - 1, ND)
    there_r = jnp.logical_and(mine_r < R_PIECES, lax.div(mine_r * ND, R_PIECES) == d)
    PP, CT, OT, GR, SP = range(5)

    def scatter_grad(p):
        @pl.when(d != p)
        def _():
            remote(gr_src.at[p], gr_mid.at[d], a2_s.at[GR, 0], a2_r.at[GR, 0], {"dp": p}).start()

    def scatter_rows(src, mid, which):
        first = jnp.minimum(mine_r, R_PIECES - 1)

        def send_piece(p):
            m = lax.div(p * ND, R_PIECES)
            remote(src.at[p], mid.at[d], a2_s.at[which, 0], a2_r.at[which, 0], {"dp": m}).start()

        def body(i, carry):
            send_piece(lax.rem(first + i, R_PIECES))
            return carry

        lax.fori_loop(1, R_PIECES, body, 0)

        @pl.when(there_r)
        def _():
            mid[d] = src[first]

        @pl.when(jnp.logical_not(there_r))
        def _():
            send_piece(first)

    def scatter_all(src, mid, which):
        def body(i, carry):
            m = lax.rem(d + i, ND)
            remote(src.at[m], mid.at[d], a2_s.at[which, 0], a2_r.at[which, 0], {"dp": m}).start()
            return carry

        lax.fori_loop(1, ND, body, 0)
        mid[d] = src[d]

    def await_bytes(ref, sem, count):
        part = ref.at[pl.ds(0, count)]
        pltpu.make_async_copy(part, part, sem).wait()

    def await_middle(mid, which):
        await_bytes(mid, a2_r.at[which, 0], ND - 1)

    def relay(value, send, dst, which, mine):
        def body(i, carry):
            e = lax.rem(d + i, ND)
            send[e] = value(e)
            remote(send.at[e], dst.at[mine], a2_s.at[which, 1], a2_r.at[which, 1], {"dp": e}).start()
            return carry

        lax.fori_loop(1, ND, body, 0)
        dst[mine] = value(d)

    def await_rows(ref, sem):
        @pl.when(there_r)
        def _():
            await_bytes(ref, sem, R_PIECES - 1)

        @pl.when(jnp.logical_not(there_r))
        def _():
            await_bytes(ref, sem, R_PIECES)

    def send_small(ref, which):
        def body(i, carry):
            remote(ref.at[z], ref.at[z], sm_s.at[which], sm_r.at[which], {"tensor": lax.rem(z + i, NZ)}).start()
            return carry

        lax.fori_loop(1, NZ, body, 0)

    def await_small(ref, sem):
        part = ref.at[pl.ds(0, NZ - 1)]
        pltpu.make_async_copy(part, part, sem).wait()

    SIGN = (1, -1)

    def ring_rows(c, j):
        first, count = SUBS[j]
        return (text_all if j < TEXT_SUB else prm_all).at[c, pl.ds(first, count), :]

    def ring_send(way, k, j):
        rows = ring_rows(mod8(z - SIGN[way] * (k - 1)), j)
        return remote(rows, rows, ag_s.at[way, k - 1, j], ag_r.at[way, k - 1, j], {"tensor": mod8(z + SIGN[way])})

    def ring_recv(way, k, j):
        rows = ring_rows(mod8(z - SIGN[way] * k), j)
        return remote(rows, rows, ag_s.at[way, k - 1, j], ag_r.at[way, k - 1, j], {"tensor": mod8(z + SIGN[way])})

    def ring_step(k, pairs):
        for pair in pairs:
            for way, j in enumerate(pair):
                if k < 4 or j in LAST[way]:
                    ring_recv(way, k, j).wait_recv()
                    if k < 3 or (k == 3 and j in LAST[way] and j not in LATE):
                        ring_send(way, k + 1, j).start()

    def ring_begin(pairs):
        for pair in pairs:
            for way, j in enumerate(pair):
                ring_send(way, 1, j).start()

    def lane_sums(squares, rows):
        return jnp.broadcast_to(jnp.sum(squares, axis=1, keepdims=True), (rows, 128)).T[0:1]

    def total_of(ref):
        total = ref[0]
        for i in range(1, NZ):
            total = total + ref[i]
        return total

    def inverse(squares, rows):
        inv = lax.rsqrt(squares * (1.0 / (NZ * COLS)) + EPS)
        return jnp.broadcast_to(inv, (128, rows)).T

    def normed_text(c):
        for t in range(TILES):
            lanes = slice(128 * t, 128 * t + 128)
            nb[PROMPT_PAD:, lanes] = (text_all[c, :, lanes].astype(F32) * inv_t[...] * gain[c, :, lanes]).astype(BF)

    def normed_prompts(c):
        for t in range(TILES):
            lanes = slice(128 * t, 128 * t + 128)
            nb[0:PROMPT_PAD, lanes] = (prm_all[c, :, lanes].astype(F32) * inv_p[...] * gain[c, :, lanes]).astype(BF)

    def multiply(c, which=slice(0, ROWS_PAD)):
        rows = pl.ds(pl.multiple_of(c * COLS, COLS), COLS)
        for n in range(3):
            wide = slice(WIDTH * n, WIDTH * n + WIDTH)
            acc[which, wide] += dot(nb[which], w_all[rows, wide])

    def project(c):
        normed_text(c)
        normed_prompts(c)
        multiply(c)

    def project_each(k, count):
        def body(i, carry):
            project(mod8(z + k * (i - 1) if count == 3 else z + k * (2 * i - 1)))
            return carry

        lax.fori_loop(0, count, body, 0)

    loads[0].wait()
    for c in range(TILES):
        for g in range(G_HIGH):
            pp_src[c * G_HIGH + g] = pr_loc[G_ROWS * g : G_ROWS * g + G_ROWS, 128 * c : 128 * c + 128]
    first, second = tail_rows([pr_loc[96:100, 128 * c : 128 * c + 128].astype(F32) for c in range(TILES)])
    pp_src[30] = first.astype(BF)
    pp_src[31] = second.astype(BF)
    total = jnp.zeros((PROMPT, 128), F32)
    for c in range(TILES):
        x = pr_loc[:, 128 * c : 128 * c + 128].astype(F32)
        total = total + x * x
    total = jnp.concatenate([total, jnp.zeros((PROMPT_PAD - PROMPT, 128), F32)], axis=0)
    ssp_all[z] = lane_sums(total, PROMPT_PAD)
    loads[1].wait()
    total = jnp.zeros((TEXT, 128), F32)
    for c in range(TILES):
        x = text_all[z, :, 128 * c : 128 * c + 128].astype(F32)
        total = total + x * x
    sst_all[z] = lane_sums(total, TEXT)
    pl.semaphore_wait(barrier, ND - 1 + NZ - 1)
    send_small(ssp_all, 1)
    send_small(sst_all, 0)
    ring_begin(TEXT_ORDER)
    scatter_all(pp_src, pp_mid, PP)
    loads[2].wait()
    for c in range(HEADS):
        lanes = slice(128 * c, 128 * c + 128)
        for g in range(R_HIGH - 1):
            ct_src[c * R_HIGH + g] = ct_loc[R_ROWS * g : R_ROWS * g + R_ROWS, lanes]
        ct_src[c * R_HIGH + 8] = jnp.zeros((R_ROWS, 128), BF)
        ct_src[c * R_HIGH + 8, 0:36] = ct_loc[320:356, lanes]
    prm_all[:, PROMPT_SENT:, :] = jnp.zeros((NZ, PROMPT_PAD - PROMPT_SENT, COLS), BF)
    acc[...] = jnp.zeros_like(acc)
    for load in loads[9:]:
        load.wait()
    def look_up(s, carry):
        found, upto = jnp.int32(0), jnp.int32(0)
        for e in range(ND):
            found = jnp.where(slot[e] == s, e, found)
            upto = upto + jnp.where(task_of[e] <= s, 1, 0)
        inverse_slot[s] = found
        last_of[s] = upto - 1
        return carry

    lax.fori_loop(0, ND, look_up, 0)
    await_bytes(ssp_all, sm_r.at[1], NZ - 1)
    spt_all[d] = total_of(ssp_all)

    def tell_dp(i, carry):
        m = lax.rem(d + i, ND)
        remote(spt_all.at[d], spt_all.at[d], a2_s.at[SP, 0], a2_r.at[SP, 0], {"dp": m}).start()
        return carry

    lax.fori_loop(1, ND, tell_dp, 0)
    ring_step(1, TEXT_ORDER[:1])
    await_middle(pp_mid, PP)
    relay(lambda e: pp_mid[task_of[e]], pp_send, pp_dst, PP, d)
    ring_step(1, TEXT_ORDER[1:3])
    await_bytes(sst_all, sm_r.at[0], NZ - 1)
    inv_t[...] = inverse(total_of(sst_all), TEXT)
    ring_step(1, TEXT_ORDER[3:])
    await_bytes(pp_dst, a2_r.at[PP, 1], ND - 1)
    for c in range(TILES):
        lanes = slice(128 * c, 128 * c + 128)
        for g in range(G_HIGH):
            prm_all[z, G_ROWS * g : G_ROWS * g + G_ROWS, lanes] = pp_dst[c * G_HIGH + g]
        end = pp_dst[30 + c // 4].astype(F32)[4 * (c % 4) : 4 * (c % 4) + 4]
        prm_all[z, 96:104, lanes] = jnp.concatenate([end, jnp.zeros((4, 128), F32)], axis=0).astype(BF)
    ring_begin(PROMPT_ORDER)
    scatter_rows(ct_src, ct_mid, CT)
    ring_step(2, TEXT_ORDER)
    await_bytes(spt_all, a2_r.at[SP, 0], ND - 1)
    inv_p[...] = inverse(spt_all[task_of[d]], PROMPT_PAD)
    ring_step(1, PROMPT_ORDER)
    for load in loads[3:6] + loads[8:9]:
        load.wait()
    project_each(1, 3)
    ring_step(3, TEXT_ORDER)
    @pl.when(there_r)
    def _():
        await_middle(ct_mid, CT)
        relay(lambda e: ct_mid[slot[e]], ct_send, ct_dst, CT, mine_r)

    ring_step(2, PROMPT_ORDER)
    for way in range(2):
        ring_send(way, 4, LATE[way]).start()
    project_each(2, 2)
    ring_step(3, PROMPT_ORDER)
    project_each(3, 2)
    length = lengths[d]
    await_rows(ct_dst, a2_r.at[CT, 1])
    for c in range(HEADS):
        for g in range(R_HIGH):
            u_ext[R_ROWS * g : R_ROWS * g + R_ROWS, 128 * c : 128 * c + 128] = ct_dst[c * R_HIGH + g].astype(F32)
    u_ext[R_ROWS * R_HIGH :] = jnp.zeros((ROWS_PAD - R_ROWS * R_HIGH, WIDTH), F32)
    row = lax.broadcasted_iota(jnp.int32, (ROWS_PAD, HD), 0)
    live = (row < PROMPT) | ((row >= PROMPT_PAD) & (row < length + PROMPT_PAD))
    for h in range(HEADS):
        lanes = slice(HD * h, HD * h + HD)
        x = u_ext[:, lanes]
        x = jnp.where(row < PROMPT_PAD, x, pltpu.roll(x, PROMPT_PAD - PROMPT, 0))
        u_all[:, lanes] = jnp.where(live, x, 0.0).astype(BF)
    loads[6].wait()
    loads[7].wait()

    ring_step(4, TEXT_ORDER)
    normed_text(mod8(z + 4))
    multiply(mod8(z + 4), slice(PROMPT_PAD, ROWS_PAD))
    ring_step(4, PROMPT_ORDER)
    normed_prompts(mod8(z + 4))
    multiply(mod8(z + 4), slice(0, PROMPT_PAD))

    score_scale = 1.0 / math.sqrt(HD)
    cos_all, sin_all = cos_t[...], sin_t[...]
    cos_p, sin_p = cos_all[:PROMPT_PAD], sin_all[:PROMPT_PAD]
    block_rows = [slice(128 * b, 128 * b + 128) for b in range(3)]
    allowed = []
    for b in range(3):
        shape = (128, 128 * b + 128)
        r = lax.broadcasted_iota(jnp.int32, shape, 0) + 128 * b
        c = lax.broadcasted_iota(jnp.int32, shape, 1)
        allowed.append((c <= r) & ((c < PROMPT) | ((c >= PROMPT_PAD) & (c < length + PROMPT_PAD))))
    at_q = [slice(HD * h, HD * h + HD) for h in range(HEADS)]
    at_k = [slice(WIDTH + HD * h, WIDTH + HD * h + HD) for h in range(HEADS)]
    at_v = [slice(2 * WIDTH + HD * h, 2 * WIDTH + HD * h + HD) for h in range(HEADS)]
    every = [(h, b) for h in range(HEADS) for b in range(3)]

    def turned(pre):
        return (pre * cos_all + pltpu.roll(pre, HALF, 1) * sin_all).astype(BF)

    def keys(b):
        return slice(0, 128 * b + 128)

    q = [turned(acc[:, at_q[h]]) for h in range(HEADS)]
    k = [turned(acc[:, at_k[h]]) for h in range(HEADS)]
    v = [acc[:, at_v[h]].astype(BF) for h in range(HEADS)]
    u = [u_all[:, at_q[h]] for h in range(HEADS)]
    scores = {
        (h, b): jnp.where(allowed[b], dot_t(q[h][block_rows[b]], k[h][keys(b)]) * score_scale, -1e30) for h, b in every
    }
    grad_prob = {(h, b): dot_t(u[h][block_rows[b]], v[h][keys(b)]) for h, b in every}
    peak = {at: jnp.max(scores[at], axis=1, keepdims=True) for at in every}
    weights = {at: jnp.exp(scores[at] - peak[at]) for at in every}
    norm = {at: 1.0 / jnp.sum(weights[at], axis=1, keepdims=True) for at in every}
    prob = {at: weights[at] * norm[at] for at in every}
    delta = {at: jnp.sum(prob[at] * grad_prob[at], axis=1, keepdims=True) for at in every}
    grads = {
        at: prob[at][:, :PROMPT_PAD] * (grad_prob[at][:, :PROMPT_PAD] - delta[at]) for at in every
    }
    for h, b in every:
        mixed = dot(prob[h, b].astype(BF), v[h][keys(b)])
        o_full[block_rows[b], at_q[h]] = mixed if b == 0 else jnp.where(live[block_rows[b]], mixed, 0.0)
    grad_t = [jnp.concatenate([grads[h, b].T for b in range(3)], axis=1).astype(BF) for h in range(HEADS)]
    prob_t = [jnp.concatenate([prob[h, b][:, :PROMPT_PAD].T for b in range(3)], axis=1).astype(BF) for h in range(HEADS)]
    grad_q = [dot(grads[h, 0].astype(BF), k[h][:PROMPT_PAD]) * score_scale for h in range(HEADS)]
    grad_k = [dot(grad_t[h], q[h]) * score_scale for h in range(HEADS)]
    grad_v = [dot(prob_t[h], u[h]).astype(BF) for h in range(HEADS)]
    grad_q = [(g * cos_p - pltpu.roll(g, HALF, 1) * sin_p).astype(BF) for g in grad_q]
    grad_k = [(g * cos_p - pltpu.roll(g, HALF, 1) * sin_p).astype(BF) for g in grad_k]
    s_part = jnp.zeros((PROMPT_PAD, HD), F32)
    for h in range(HEADS):
        for at, grad in ((at_q[h], grad_q[h]), (at_k[h], grad_k[h]), (at_v[h], grad_v[h])):
            gcat[:, at] = grad
            s_part = s_part + grad.astype(F32) * acc[0:PROMPT_PAD, at]

    def grad_block(j):
        rows = pl.ds(pl.multiple_of(j * COLS, COLS), COLS)
        return dot_t(gcat[0:PROMPT_SENT], w_all[rows, :])

    def rs_copy(way, step, t, half):
        rows = slice(*HALVES[half])
        return remote(
            rs_tx.at[way, step, t, rows], rs_rx.at[way, step, t, rows],
            rs_s.at[way, step, t, half], rs_r.at[way, step, t, half],
            {"tensor": mod8(z + SIGN[way])},
        )

    def rs_put(way, step, t, value, add=False):
        for half in range(2):
            rows = slice(*HALVES[half])
            now = value[rows]
            if add:
                rs_copy(way, step - 1, t, half).wait_recv()
                now = now + rs_rx[way, step - 1, t, rows].astype(F32)
            rs_tx[way, step, t, rows] = now.astype(BF)
            rs_copy(way, step, t, half).start()

    for way in range(2):
        first, count = RS_LAST[way][0], len(RS_LAST[way])
        rows = pl.ds(pl.multiple_of(mod8(z + 4) * COLS + 128 * first, 128), 128 * count)
        part = dot_t(gcat[0:PROMPT_SENT], w_all[rows, :])
        for i in range(count):
            rs_put(way, 0, first + i, part[:, 128 * i : 128 * i + 128])
    blocks = (grad_block(mod8(z + 3)), grad_block(mod8(z - 3)))
    for way in range(2):
        for t in RS_LAST[1 - way]:
            rs_put(way, 1, t, blocks[way][:, 128 * t : 128 * t + 128])
    for way in range(2):
        for t in RS_LAST[way]:
            rs_own[way, t] = blocks[way][:, 128 * t : 128 * t + 128]
    sx_all[z] = lane_sums(s_part, PROMPT_PAD)
    send_small(sx_all, 2)

    blocks = (grad_block(mod8(z + 2)), grad_block(mod8(z - 2)))
    for t in (0, 1, 2):
        for way in range(2):
            if t < len(RS_LAST[way]):
                tile = RS_LAST[way][t]
                rs_put(way, 1, tile, rs_own[way, tile], add=True)
    for h in range(HEADS):
        lanes = slice(HD * h, HD * h + HD)
        x = o_full[:, lanes]
        outer = jnp.where(row < PROMPT, x, pltpu.roll(x, ROWS_PAD - (PROMPT_PAD - PROMPT), 0))
        outer = outer.astype(BF)
        for g in range(R_HIGH):
            ot_src[h * R_HIGH + g] = outer[R_ROWS * g : R_ROWS * g + R_ROWS]
    scatter_rows(ot_src, ot_mid, OT)

    for step in (2, 3):
        if step == 3:
            blocks = (grad_block(mod8(z + 1)), grad_block(mod8(z - 1)))
        for i in range(TILES):
            for way in range(2):
                t = RS_ORDER[way][i]
                rs_put(way, step, t, blocks[way][:, 128 * t : 128 * t + 128], add=True)
    @pl.when(there_r)
    def _():
        await_middle(ot_mid, OT)
        relay(lambda s: ot_mid[inverse_slot[s]], ot_send, ot_dst, OT, mine_r)

    own = grad_block(z)
    await_bytes(sx_all, sm_r.at[2], NZ - 1)
    s_col[...] = jnp.broadcast_to(total_of(sx_all) * (1.0 / (NZ * COLS)), (128, PROMPT_PAD)).T
    inv = inv_p[0:PROMPT_SENT]
    second = inv * inv * s_col[0:PROMPT_SENT]
    ends = [None] * TILES
    for t in FINAL_ORDER:
        lanes = slice(128 * t, 128 * t + 128)
        value = own[:, lanes]
        for way in range(2):
            for half in range(2):
                rs_copy(way, 3, t, half).wait_recv()
            value = value + rs_rx[way, 3, t].astype(F32)
        value = inv * (value * gain[z, :, lanes]) - prm_all[z, 0:PROMPT_SENT, lanes].astype(F32) * second
        low = value.astype(BF)
        for g in range(G_HIGH):
            p = t * G_HIGH + g
            gr_src[p] = low[G_ROWS * g : G_ROWS * g + G_ROWS]
            scatter_grad(p)
        ends[t] = value[96:100]
    first, second = tail_rows(ends)
    for p, value in ((30, first), (31, second)):
        gr_src[p] = value.astype(BF)
        scatter_grad(p)
    gr_mid[d] = gr_src[d]
    await_middle(gr_mid, GR)
    before = jnp.zeros((G_ROWS, 128), F32)
    for e in range(ND):
        now = gr_mid[e].astype(F32)
        if e > 0:
            now = now + jnp.where(task_of[e] == task_of[e - 1], before, 0.0)
        gr_run[e] = now
        before = now

    def task_sum(t):
        at = jnp.maximum(last_of[t], 0)
        return jnp.where(task_of[at] == t, gr_run[at], 0.0).astype(BF)

    relay(task_sum, gr_send, gr_dst, GR, d)
    await_rows(ot_dst, a2_r.at[OT, 1])
    await_bytes(gr_dst, a2_r.at[GR, 1], ND - 1)
    await_bytes(spt_all, a2_s.at[SP, 0], ND - 1)
    await_bytes(pp_src, a2_s.at[PP, 0], ND - 1)
    await_bytes(pp_send, a2_s.at[PP, 1], ND - 1)
    await_bytes(gr_src, a2_s.at[GR, 0], ND - 1)
    await_bytes(gr_send, a2_s.at[GR, 1], ND - 1)
    await_rows(ct_src, a2_s.at[CT, 0])
    await_rows(ot_src, a2_s.at[OT, 0])

    @pl.when(there_r)
    def _():
        await_bytes(ct_send, a2_s.at[CT, 1], ND - 1)
        await_bytes(ot_send, a2_s.at[OT, 1], ND - 1)

    for which, ref in enumerate((sst_all, ssp_all, sx_all)):
        await_bytes(ref, sm_s.at[which], NZ - 1)
    for way in range(2):
        for j in range(len(SUBS)):
            for k in range(1, 5):
                if k < 4 or j in LAST[way]:
                    ring_send(way, k, j).wait_send()
        for step in range(4):
            for t in range(TILES):
                if step > 0 or t in RS_LAST[way]:
                    for half in range(2):
                        rs_copy(way, step, t, half).wait_send()


def assemble(ot_ref, gr_ref, out_ref, pg_ref):
    for c in range(HEADS):
        lanes = slice(128 * c, 128 * c + 128)
        for g in range(R_HIGH - 1):
            out_ref[0, R_ROWS * g : R_ROWS * g + R_ROWS, lanes] = ot_ref[c * R_HIGH + g]
        out_ref[0, 320:356, lanes] = ot_ref[c * R_HIGH + 8, 0:36]
    for c in range(TILES):
        lanes = slice(128 * c, 128 * c + 128)
        for g in range(G_HIGH):
            pg_ref[G_ROWS * g : G_ROWS * g + G_ROWS, 0, lanes] = gr_ref[c * G_HIGH + g].astype(F32)
        pg_ref[96:100, 0, lanes] = gr_ref[30 + c // 4].astype(F32)[4 * (c % 4) : 4 * (c % 4) + 4]


def on_device(text, prompts, gain, w_query, w_key, w_value, cotangent, task_of, lengths, slot):
    cosine, sine = rope_constants()
    vmem, dma, smem = pltpu.VMEM, pltpu.SemaphoreType.DMA, pltpu.SMEM
    anywhere = pl.BlockSpec(memory_space=pl.ANY)
    whole = pl.BlockSpec(memory_space=pltpu.VMEM)
    g_piece, r_piece = (G_ROWS, 128), (R_ROWS, 128)
    out_pieces, grad_pieces = pl.pallas_call(
        kernel,
        out_shape=(
            pltpu.VMEM((R_PIECES, *r_piece), BF),
            pltpu.VMEM((ND, *g_piece), BF),
        ),
        in_specs=[anywhere] * 12,
        out_specs=(whole, whole),
        scratch_shapes=[
            *[smem((ND,), jnp.int32)] * 5, vmem((NZ, 1, COLS), F32),
            vmem((NZ, TEXT, COLS), BF), vmem((NZ, PROMPT_PAD, COLS), BF), vmem((PROMPT, COLS), BF),
            vmem((ROWS, WIDTH), BF), vmem((NZ * COLS, ALL), BF),
            vmem((ROWS_PAD, HD), F32), vmem((ROWS_PAD, HD), F32),
            vmem((ROWS_PAD, ALL), F32), vmem((ROWS_PAD, COLS), BF),
            vmem((TEXT, 128), F32), vmem((PROMPT_PAD, 128), F32), vmem((PROMPT_PAD, 128), F32),
            vmem((NZ, 1, TEXT), F32), vmem((NZ, 1, PROMPT_PAD), F32), vmem((ND, 1, PROMPT_PAD), F32),
            vmem((NZ, 1, PROMPT_PAD), F32),
            vmem((ND, *g_piece), BF), vmem((ND, *g_piece), BF), vmem((ND, *g_piece), BF), vmem((ND, *g_piece), BF),
            vmem((R_PIECES, *r_piece), BF), vmem((ND, *r_piece), BF), vmem((ND, *r_piece), BF), vmem((R_PIECES, *r_piece), BF),
            vmem((R_PIECES, *r_piece), BF), vmem((ND, *r_piece), BF), vmem((ND, *r_piece), BF),
            vmem((ND, *g_piece), BF), vmem((ND, *g_piece), BF), vmem((ND, *g_piece), BF), vmem((ND, *g_piece), F32),
            vmem((ROWS_PAD, WIDTH), F32), vmem((ROWS_PAD, WIDTH), BF),
            vmem((ROWS_PAD, WIDTH), F32), vmem((PROMPT_PAD, ALL), BF),
            vmem((2, TILES, PROMPT_SENT, 128), F32),
            vmem((2, 4, TILES, PROMPT_SENT, 128), BF), vmem((2, 4, TILES, PROMPT_SENT, 128), BF),
            dma((12,)), dma((2, 4, len(SUBS))), dma((2, 4, len(SUBS))), dma((2, 4, TILES, 2)), dma((2, 4, TILES, 2)),
            dma((3,)), dma((3,)), dma((5, 2)), dma((5, 2)),
        ],
        compiler_params=pltpu.CompilerParams(
            collective_id=0, has_side_effects=True, vmem_limit_bytes=56 * 1024 * 1024
        ),
    )(
        task_of, lengths, slot, text, prompts, gain.reshape(NZ, 1, COLS), w_query, w_key, w_value, cotangent,
        jnp.asarray(cosine), jnp.asarray(sine),
    )
    attn_out, prompt_grad = pl.pallas_call(
        assemble,
        out_shape=(
            jax.ShapeDtypeStruct((1, ROWS, WIDTH), BF),
            jax.ShapeDtypeStruct((PROMPT, 1, COLS), F32),
        ),
        in_specs=[whole, whole],
        out_specs=(whole, whole),
    )(*(pltpu.with_memory_space_constraint(x, pltpu.VMEM) for x in (out_pieces, grad_pieces)))
    return attn_out, prompt_grad.reshape(1, PROMPT, COLS)


def solution(mesh):
    in_specs = (
        P("dp", None, "tensor"),
        P("dp", None, "tensor"),
        P(),
        P(None, "tensor"),
        P(None, "tensor"),
        P(None, "tensor"),
        P("dp", None, "tensor"),
        P(),
        P(),
        P(),
    )
    out_specs = (P("dp", None, "tensor"), P("dp", None, "tensor"))
    return jax.shard_map(on_device, mesh=mesh, in_specs=in_specs, out_specs=out_specs, check_vma=False)
```
